16 devices in a mesh: tp: 4 (over z, y), dp: 4 (over x, core).
Axes of the slice: x: 2, y: 2, z: 2, core: 2. Of those that a mesh axis runs over, the one named last changes fastest.
Arguments:
- hidden: bfloat16 [4, 1024, 768], P('dp')
- ln_gamma: float32 [768], replicated
- ln_beta: float32 [768], replicated
- embed_table: bfloat16 [50304, 768], P('tp')
- labels: int32 [4, 1024], P('dp')
- loss_mask: int32 [4, 1024], P('dp')
Outputs:
- output 1: float32 [], replicated
- output 2: bfloat16 [4, 1024, 768], P('dp')
- output 3: float32 [50304, 768], P('tp')
- output 4: float32 [768], replicated
- output 5: float32 [768], replicated
All inputs are finite; a program needn't handle non-finite values.
Results may differ from the reference program's by a relative error of at most 0.001.
Values sent between devices are 32-bit elements.
A program may use at most 1 GiB of HBM per device.

```python
import jax
import jax.numpy as jnp
from jax import lax

HIDDEN = 768
VOCAB_SIZE = 50304
NUM_SEQS = 4
SEQ_LEN = 1024
TOKEN_BLOCK = min(SEQ_LEN, 128)
LAYER_EPS = 1e-5
SCORE_SCALE = 3.5


def setup_inputs(seed: int = 0) -> dict:
    rand_keys = jax.random.split(jax.random.key(seed), 6)
    hidden = (1.5 * jax.random.normal(rand_keys[0], (NUM_SEQS, SEQ_LEN, HIDDEN), jnp.float32)).astype(jnp.bfloat16)
    ln_gamma = 1.0 + 0.3 * jax.random.normal(rand_keys[1], (HIDDEN,), jnp.float32)
    ln_beta = 0.3 * jax.random.normal(rand_keys[2], (HIDDEN,), jnp.float32)
    embed_table = (SCORE_SCALE * HIDDEN ** -0.5 * jax.random.normal(rand_keys[3], (VOCAB_SIZE, HIDDEN), jnp.float32)).astype(jnp.bfloat16)
    labels = jax.random.randint(rand_keys[4], (NUM_SEQS, SEQ_LEN), 0, VOCAB_SIZE, jnp.int32)
    lengths = jax.random.randint(rand_keys[5], (NUM_SEQS, 1), 1, SEQ_LEN + 1, jnp.int32)
    positions = jnp.arange(SEQ_LEN, dtype=jnp.int32)[None, :]
    loss_mask = (positions < lengths).astype(jnp.int32)
    return {'hidden': hidden, 'ln_gamma': ln_gamma, 'ln_beta': ln_beta, 'embed_table': embed_table, 'labels': labels, 'loss_mask': loss_mask}


def reference(hidden, ln_gamma, ln_beta, embed_table, labels, loss_mask):
    mask_float = loss_mask.astype(jnp.float32)
    token_count = jnp.sum(mask_float)
    vocab_ids = jnp.arange(VOCAB_SIZE, dtype=jnp.int32)[None, :]
    block_hidden = hidden.reshape(-1, TOKEN_BLOCK, HIDDEN)
    block_labels = labels.reshape(-1, TOKEN_BLOCK)
    block_mask = mask_float.reshape(-1, TOKEN_BLOCK, 1)

    def block_step(scan_carry, block_data):
        d_embed, d_gamma, d_beta, loss_sum = scan_carry
        block_rows, row_labels, row_mask = block_data
        x_float = block_rows.astype(jnp.float32)
        row_mean = jnp.mean(x_float, axis=-1, keepdims=True)
        centered = x_float - row_mean
        inv_std = lax.rsqrt(jnp.mean(centered * centered, axis=-1, keepdims=True) + LAYER_EPS)
        x_hat = centered * inv_std
        normed = (x_hat * ln_gamma + ln_beta).astype(jnp.bfloat16)
        logits = jnp.dot(normed, embed_table.T, preferred_element_type=jnp.float32)
        row_max = jnp.max(logits, axis=-1, keepdims=True)
        log_norm = row_max + jnp.log(jnp.sum(jnp.exp(logits - row_max), axis=-1, keepdims=True))
        is_target = vocab_ids == row_labels[:, None]
        target_logit = jnp.sum(jnp.where(is_target, logits, 0.0), axis=-1, keepdims=True)
        loss_sum = loss_sum + jnp.sum(row_mask * (log_norm - target_logit))
        soft_probs = jnp.exp(logits - log_norm)
        grad_logits = (jnp.where(is_target, soft_probs - 1.0, soft_probs) * (row_mask / token_count)).astype(jnp.bfloat16)
        grad_normed = jnp.dot(grad_logits, embed_table, preferred_element_type=jnp.float32)
        d_embed = d_embed + jnp.dot(grad_logits.T, normed, preferred_element_type=jnp.float32)
        d_gamma = d_gamma + jnp.sum(grad_normed * x_hat, axis=0)
        d_beta = d_beta + jnp.sum(grad_normed, axis=0)
        grad_scaled = grad_normed * ln_gamma
        grad_x = (grad_scaled - jnp.mean(grad_scaled, axis=-1, keepdims=True) - x_hat * jnp.mean(grad_scaled * x_hat, axis=-1, keepdims=True)) * inv_std
        return (d_embed, d_gamma, d_beta, loss_sum), grad_x.astype(jnp.bfloat16)

    zero_carry = (jnp.zeros((VOCAB_SIZE, HIDDEN), jnp.float32), jnp.zeros((HIDDEN,), jnp.float32), jnp.zeros((HIDDEN,), jnp.float32), jnp.zeros((), jnp.float32))
    final_carry, grad_blocks = lax.scan(block_step, zero_carry, (block_hidden, block_labels, block_mask))
    d_embed, d_gamma, d_beta, loss_sum = final_carry
    d_hidden = grad_blocks.reshape(NUM_SEQS, SEQ_LEN, HIDDEN)
    return loss_sum / token_count, d_hidden, d_embed, d_gamma, d_beta
```

```python
import functools

import jax
import jax.numpy as jnp
from jax import lax
from jax.experimental import pallas as pl
from jax.experimental.pallas import tpu as pltpu
from jax.sharding import PartitionSpec as P

LAYER_EPS = 1e-5
BLOCK = 256
PAIR = 2 * BLOCK
BIG = 1e30
VMEM_LIMIT = 62 * 1024 * 1024


def chunk_list(total, size):
    return [(start, min(size, total - start)) for start in range(0, total, size)]


def logits_kernel(idx_ref, e_ref, za_ref, zb_ref, *rest):
    l_ref, zc_ref, st_ref = rest[-3:]
    pl.when(pl.program_id(0) < idx_ref[1])(lambda: logits_step(e_ref, za_ref, zb_ref, l_ref, zc_ref, st_ref))


def logits_step(e_ref, za_ref, zb_ref, l_ref, zc_ref, st_ref):
    zc_ref[0, :BLOCK, :] = za_ref[0]
    zc_ref[0, BLOCK:, :] = zb_ref[0]
    rows = e_ref.shape[0]
    size = 528
    full = rows // size

    def step(start, n, carry):
        top, total = carry
        tile = lax.dot_general(e_ref[pl.ds(start, n), :], zc_ref[0], (((1,), (1,)), ((), ())), preferred_element_type=jnp.float32)
        l_ref[0, pl.ds(start, n), :] = tile
        new_top = jnp.maximum(top, jnp.max(tile, axis=0, keepdims=True))
        total = total * jnp.exp(top - new_top) + jnp.sum(jnp.exp(tile - new_top), axis=0, keepdims=True)
        return new_top, total

    carry = (jnp.full((1, PAIR), -BIG, jnp.float32), jnp.zeros((1, PAIR), jnp.float32))
    carry = lax.fori_loop(0, full, lambda i, c: step(pl.multiple_of(i * size, 16), size, c), carry)
    if rows > full * size:
        carry = step(full * size, rows - full * size, carry)
    st_ref[0, 0:1, :] = carry[0]
    st_ref[0, 1:2, :] = carry[1]


def grad_tile(tile, lse, weight, is_target):
    probs = jnp.exp(tile - lse)
    return (jnp.where(is_target, probs - 1.0, probs) * weight).astype(jnp.bfloat16)


def dz_kernel(idx_ref, *refs):
    pl.when(pl.program_id(0) < idx_ref[1])(lambda: dz_step(idx_ref, *refs))


def dz_step(idx_ref, e_ref, l_ref, tok_ref, lab_ref, dz_ref, tl_ref, acc_ref, sem):
    i = pl.program_id(0)
    rows = e_ref.shape[0]
    size = 512
    full = rows // size
    lse = tok_ref[0, 0:1, :]
    weight = tok_ref[0, 1:2, :]
    label = lab_ref[0]
    acc_ref[...] = jnp.zeros_like(acc_ref)

    def step(start, n, target):
        tile = l_ref[0, pl.ds(start, n), :]
        is_target = lax.broadcasted_iota(jnp.int32, (n, PAIR), 0) == label - start
        target = target + jnp.sum(jnp.where(is_target, tile, 0.0), axis=0, keepdims=True)
        grad = grad_tile(tile, lse, weight, is_target)
        acc_ref[...] += lax.dot_general(grad, e_ref[pl.ds(start, n), :], (((0,), (0,)), ((), ())), preferred_element_type=jnp.float32)
        return target

    target = lax.fori_loop(0, full, lambda k, c: step(pl.multiple_of(k * size, 16), size, c), jnp.zeros((1, PAIR), jnp.float32))
    if rows > full * size:
        target = step(full * size, rows - full * size, target)
    tl_ref[0] = target
    copies = [pltpu.make_async_copy(acc_ref.at[pl.ds(h * BLOCK, BLOCK), :], dz_ref.at[idx_ref[2 + 2 * i + h]], sem.at[h]) for h in range(2)]
    for copy in copies:
        copy.start()
    for copy in copies:
        copy.wait()


def de_kernel(idx_ref, l_ref, z_ref, tok_ref, lab_ref, de_ref):
    j, i = pl.program_id(0), pl.program_id(1)
    rows = de_ref.shape[0]
    lse = tok_ref[0, 0:1, :]
    weight = tok_ref[0, 1:2, :]
    label = lab_ref[0] - j * rows

    def fill(first):
        for start, n in chunk_list(rows, 528):
            is_target = lax.broadcasted_iota(jnp.int32, (n, PAIR), 0) == label - start
            grad = grad_tile(l_ref[0, start:start + n, :], lse, weight, is_target)
            part = jnp.dot(grad, z_ref[0], preferred_element_type=jnp.float32)
            if first:
                de_ref[start:start + n, :] = part
            else:
                de_ref[start:start + n, :] += part

    pl.when(i == 0)(lambda: fill(True))
    pl.when((i > 0) & (i < idx_ref[1]))(lambda: fill(False))


def order_blocks(active):
    n = active.shape[0]
    act = active.astype(jnp.int32)
    ids = jnp.arange(n, dtype=jnp.int32)
    before = (ids[None, :] < ids[:, None]).astype(jnp.int32)
    ahead = jnp.sum(before * act[None, :], axis=1)
    count = jnp.sum(act)
    place = jnp.where(act > 0, ahead, count + ids - ahead)
    order = jnp.sum(jnp.where(place[None, :] == ids[:, None], ids[None, :], 0), axis=1)
    return order, count


def last(i, s):
    return jnp.minimum(i, s[1] - 1)


def call_logits(idx, e, z, previous, rows):
    pairs = 8
    base = 0 if previous is None else pairs // 2
    width = e.shape[1]
    extra = [] if previous is None else list(previous)
    spec = pltpu.PrefetchScalarGridSpec(
        num_scalar_prefetch=1,
        grid=(4,),
        in_specs=[
            pl.BlockSpec((rows, width), lambda i, s: (s[0], 0), pipeline_mode=pl.Buffered(1)),
            pl.BlockSpec((1, BLOCK, width), lambda i, s: (s[2 + 2 * last(i, s)], 0, 0)),
            pl.BlockSpec((1, BLOCK, width), lambda i, s: (s[3 + 2 * last(i, s)], 0, 0)),
        ] + [pl.BlockSpec(memory_space=pl.ANY)] * len(extra),
        out_specs=[
            pl.BlockSpec((1, rows, PAIR), lambda i, s: (base + last(i, s), 0, 0)),
            pl.BlockSpec((1, PAIR, width), lambda i, s: (base + last(i, s), 0, 0)),
            pl.BlockSpec((1, 2, PAIR), lambda i, s: (base + last(i, s), 0, 0)),
        ],
    )
    return pl.pallas_call(
        logits_kernel,
        grid_spec=spec,
        out_shape=[
            jax.ShapeDtypeStruct((pairs, rows, PAIR), jnp.float32),
            jax.ShapeDtypeStruct((pairs, PAIR, width), jnp.bfloat16),
            jax.ShapeDtypeStruct((pairs, 2, PAIR), jnp.float32),
        ],
        input_output_aliases={} if previous is None else {4: 0, 5: 1, 6: 2},
        compiler_params=pltpu.CompilerParams(vmem_limit_bytes=VMEM_LIMIT, dimension_semantics=("arbitrary",)),
        cost_estimate=pl.CostEstimate(flops=2 * 1200 * rows * width, bytes_accessed=4 * 1200 * rows, transcendentals=1200 * rows),
        name="logits_near" if previous is None else "logits_far",
    )(idx, e, z, z, *extra)


def call_dz(idx, e, l, tok, lab, rows):
    width = e.shape[1]
    spec = pltpu.PrefetchScalarGridSpec(
        num_scalar_prefetch=1,
        grid=(4,),
        in_specs=[
            pl.BlockSpec((rows, width), lambda i, s: (s[0], 0), pipeline_mode=pl.Buffered(1)),
            pl.BlockSpec((1, rows, PAIR), lambda i, s: (last(i, s), 0, 0)),
            pl.BlockSpec((1, 2, PAIR), lambda i, s: (last(i, s), 0, 0)),
            pl.BlockSpec((1, 1, PAIR), lambda i, s: (last(i, s), 0, 0)),
        ],
        out_specs=[
            pl.BlockSpec(memory_space=pl.ANY),
            pl.BlockSpec((1, 1, PAIR), lambda i, s: (last(i, s), 0, 0)),
        ],
        scratch_shapes=[pltpu.VMEM((PAIR, width), jnp.float32), pltpu.SemaphoreType.DMA((2,))],
    )
    return pl.pallas_call(
        dz_kernel,
        grid_spec=spec,
        out_shape=[jax.ShapeDtypeStruct((8, BLOCK, width), jnp.float32), jax.ShapeDtypeStruct((4, 1, PAIR), jnp.float32)],
        compiler_params=pltpu.CompilerParams(vmem_limit_bytes=VMEM_LIMIT, dimension_semantics=("arbitrary",)),
        cost_estimate=pl.CostEstimate(flops=2 * 1200 * rows * width, bytes_accessed=4 * 1200 * rows, transcendentals=1200 * rows),
        name="dz_part",
    )(idx, e, l, tok, lab)


def call_de(idx, l, zc, tok, lab):
    rows, width = l.shape[1], zc.shape[2]
    splits = 3
    part = rows // splits
    spec = pltpu.PrefetchScalarGridSpec(
        num_scalar_prefetch=1,
        grid=(splits, 8),
        in_specs=[
            pl.BlockSpec((1, part, PAIR), lambda j, i, s: (s[2 + last(i, s)], j, 0)),
            pl.BlockSpec((1, PAIR, width), lambda j, i, s: (s[2 + last(i, s)], 0, 0)),
            pl.BlockSpec((1, 2, PAIR), lambda j, i, s: (s[2 + last(i, s)], 0, 0)),
            pl.BlockSpec((1, 1, PAIR), lambda j, i, s: (s[2 + last(i, s)], 0, 0)),
        ],
        out_specs=pl.BlockSpec((part, width), lambda j, i, s: (j, 0)),
    )
    return pl.pallas_call(
        de_kernel,
        grid_spec=spec,
        out_shape=jax.ShapeDtypeStruct((rows, width), jnp.float32),
        compiler_params=pltpu.CompilerParams(vmem_limit_bytes=VMEM_LIMIT, dimension_semantics=("arbitrary", "arbitrary")),
        cost_estimate=pl.CostEstimate(flops=2 * 2400 * rows * width, bytes_accessed=4 * 2400 * rows, transcendentals=2400 * rows),
        name="de_part",
    )(idx, l, zc, tok, lab)


def solution(mesh):
    n_tp, n_dp = mesh.shape['tp'], mesh.shape['dp']

    def flip(x, axis, bits):
        n = n_tp if axis == 'tp' else n_dp
        return lax.ppermute(x, axis, [(k, k ^ bits) for k in range(n)])

    def pick(x, index):
        return lax.dynamic_index_in_dim(x, index, 0, keepdims=False)

    def local_step(hidden, ln_gamma, ln_beta, embed_shard, labels, loss_mask):
        tp, dp = lax.axis_index('tp'), lax.axis_index('dp')
        core, side = dp % 2, dp // 2
        seq, width = hidden.shape[1:]
        quarters = seq // BLOCK
        rows = embed_shard.shape[0] // 2
        row_start = tp * (2 * rows) + core * rows

        x_float = hidden[0].astype(jnp.float32)
        centered = x_float - jnp.mean(x_float, axis=-1, keepdims=True)
        inv_std = lax.rsqrt(jnp.mean(centered * centered, axis=-1, keepdims=True) + LAYER_EPS)
        x_hat = centered * inv_std

        def to_z(values):
            return (values * ln_gamma + ln_beta).astype(jnp.bfloat16)

        marked = jnp.where(loss_mask[0] > 0, labels[0], -1)
        marked = lax.all_gather(marked, 'dp').reshape(n_dp, quarters, BLOCK)
        token_count = jnp.sum((marked >= 0).astype(jnp.float32))
        near = lax.dynamic_slice_in_dim(marked, side * 2, 2, 0).reshape(2 * quarters, BLOCK)
        far = lax.dynamic_slice_in_dim(marked, (1 - side) * 2, 2, 0).reshape(2 * quarters, BLOCK)
        near_order, near_n = order_blocks(jnp.any(near >= 0, axis=1))
        far_order, far_n = order_blocks(jnp.any(far >= 0, axis=1))
        near_pairs, far_pairs = (near_n + 1) // 2, (far_n + 1) // 2
        lab = jnp.concatenate([near[near_order], far[far_order]]).reshape(8, 1, PAIR)
        core_id = core.astype(jnp.int32)[None]
        near_idx = jnp.concatenate([core_id, near_pairs[None], near_order])
        far_idx = jnp.concatenate([core_id, far_pairs[None], (far_order // quarters) * quarters + ((far_order % quarters) ^ tp)])
        pair_ids = jnp.arange(8, dtype=jnp.int32)
        pair_idx = jnp.where(pair_ids < near_pairs, pair_ids, jnp.minimum(4 + pair_ids - near_pairs, 7))
        pair_idx = jnp.concatenate([core_id, (near_pairs + far_pairs)[None], pair_idx])

        own_quarter = pick(x_hat.reshape(quarters, BLOCK, width), tp)
        mate = flip(x_hat, 'dp', 1)
        first_piece = flip(own_quarter, 'dp', 2)
        pieces = [first_piece] + [flip(first_piece, 'tp', k) for k in (1, 2, 3)]
        mate_pieces = [flip(piece, 'dp', 1) for piece in pieces]

        def by_core(mine, other):
            return jnp.stack([jnp.where(core == 0, mine, other), jnp.where(core == 0, other, mine)])

        near_z = to_z(by_core(x_hat, mate)).reshape(2 * quarters, BLOCK, width)
        previous = call_logits(near_idx, embed_shard, near_z, None, rows)
        far_z = to_z(by_core(jnp.stack(pieces), jnp.stack(mate_pieces))).reshape(2 * quarters, BLOCK, width)
        logits, z_pairs, stats = call_logits(far_idx, embed_shard, far_z, previous, rows)

        every = lax.all_gather(stats, ('tp', 'dp')).reshape(n_tp, 2, 2, 8, 2, PAIR)
        every = lax.dynamic_index_in_dim(every, side, 1, keepdims=False).reshape(2 * n_tp, 8, 2, PAIR)
        top = jnp.max(every[:, :, 0], axis=0)
        total = jnp.sum(every[:, :, 1] * jnp.exp(every[:, :, 0] - top), axis=0)
        live = lab[:, 0] >= 0
        lse = jnp.where(live, top + jnp.log(total), BIG)
        tok = jnp.stack([lse, jnp.where(live, 1.0 / token_count, 0.0)], axis=1)
        local_lab = lab - row_start

        dz, target = call_dz(near_idx, embed_shard, logits, tok, local_lab, rows)
        d_rows = call_de(pair_idx, logits, z_pairs, tok, local_lab)
        d_mate = flip(d_rows, 'dp', 1)
        d_embed = by_core(d_rows, d_mate).reshape(2 * rows, width)

        dz = jnp.where((near >= 0)[..., None], dz, 0.0).reshape(2, quarters, BLOCK, width)
        part = pick(dz, core) + flip(pick(dz, 1 - core), 'dp', 1)
        grad = pick(part, tp)
        for k in (1, 2, 3):
            grad = grad + flip(pick(part, tp ^ k), 'tp', k)
        hat = own_quarter
        d_gamma = jnp.sum(grad * hat, axis=0)
        d_beta = jnp.sum(grad, axis=0)
        scaled = grad * ln_gamma
        inner = scaled - jnp.mean(scaled, axis=-1, keepdims=True) - hat * jnp.mean(scaled * hat, axis=-1, keepdims=True)
        inner = jnp.stack([inner] + [flip(inner, 'tp', k) for k in (1, 2, 3)])
        inner = jnp.stack([pick(inner, tp ^ q) for q in range(quarters)]).reshape(seq, width)
        d_hidden = (inner * inv_std).astype(jnp.bfloat16)[None]

        near_live = live[:4]
        lead = ((tp == 0) & (core == 0)).astype(jnp.float32)
        loss = jnp.sum(jnp.where(near_live, lead * lse[:4] - target[:, 0], 0.0)) / token_count
        sums = lax.psum(jnp.concatenate([d_gamma, d_beta, jnp.broadcast_to(loss, (128,))]), ('tp', 'dp'))
        return sums[2 * width], d_hidden, d_embed, sums[:width], sums[width:2 * width]

    return jax.shard_map(local_step, mesh=mesh, in_specs=(P('dp', None, None), P(None), P(None), P('tp', None), P('dp', None), P('dp', None)), out_specs=(P(), P('dp', None, None), P('tp', None), P(None), P(None)), check_vma=False)
```

```python
import functools

import jax
import jax.numpy as jnp
from jax import lax
from jax.experimental import pallas as pl
from jax.experimental.pallas import tpu as pltpu
from jax.sharding import PartitionSpec as P

LAYER_EPS = 1e-5
BLOCK = 256
PAIR = 2 * BLOCK
BIG = 1e30
VMEM_LIMIT = 62 * 1024 * 1024


CORE, NEAR_PAIRS, FAR_PAIRS, ALL_PAIRS, ROW_START = 0, 1, 2, 3, 4
NEAR_ORDER, FAR_PIECES, PAIR_IDS = 8, 16, 24


def chunk_list(total, size):
    return [(start, min(size, total - start)) for start in range(0, total, size)]


def last(i, count):
    return jnp.minimum(i, count - 1)


def logits_kernel(count, idx_ref, e_ref, za_ref, zb_ref, *rest):
    l_ref, zc_ref, st_ref = rest[-3:]
    pl.when(pl.program_id(0) < idx_ref[count])(lambda: logits_step(e_ref, za_ref, zb_ref, l_ref, zc_ref, st_ref))


def logits_step(e_ref, za_ref, zb_ref, l_ref, zc_ref, st_ref):
    zc_ref[0, :BLOCK, :] = za_ref[0]
    zc_ref[0, BLOCK:, :] = zb_ref[0]
    rows = e_ref.shape[0]
    size = 528
    full = rows // size
    tail = rows - full * size

    def product(start, n):
        tile = lax.dot_general(e_ref[pl.ds(start, n), :], zc_ref[0], (((1,), (1,)), ((), ())), preferred_element_type=jnp.float32)
        l_ref[0, pl.ds(start, n), :] = tile
        return jnp.max(tile, axis=0, keepdims=True)

    def add(start, n, old_top, top, total):
        tile = l_ref[0, pl.ds(start, n), :]
        return total * jnp.exp(old_top - top) + jnp.sum(jnp.exp(tile - top), axis=0, keepdims=True)

    def step(i, carry):
        old_top, top, total = carry
        start = pl.multiple_of(i * size, 16)
        peak = product(start, size)
        total = add(pl.multiple_of(start - size, 16), size, old_top, top, total)
        return top, jnp.maximum(top, peak), total

    low = jnp.full((1, PAIR), -BIG, jnp.float32)
    peak = product(0, size)
    old_top, top, total = lax.fori_loop(1, full, step, (low, peak, jnp.zeros((1, PAIR), jnp.float32)))
    if tail:
        peak = product(full * size, tail)
        total = add((full - 1) * size, size, old_top, top, total)
        old_top, top = top, jnp.maximum(top, peak)
        total = add(full * size, tail, old_top, top, total)
    else:
        total = add((full - 1) * size, size, old_top, top, total)
    st_ref[0, 0:1, :] = top
    st_ref[0, 1:2, :] = total


def grad_tile(tile, lse, weight, is_target):
    probs = jnp.exp(tile - lse)
    return (jnp.where(is_target, probs - 1.0, probs) * weight).astype(jnp.bfloat16)


def dz_kernel(idx_ref, et_ref, l_ref, tok_ref, lab_ref, own_ref, mate_ref, tl_ref, l_out_ref, acc_ref, grad_ref, out_ref, sem):
    i = pl.program_id(0)
    live = i < idx_ref[NEAR_PAIRS]
    pl.when(live)(lambda: dz_step(idx_ref, et_ref, l_ref, tok_ref, lab_ref, tl_ref, acc_ref, grad_ref))

    @pl.when(live)
    def _():
        out_ref[...] = acc_ref[...].T

    @pl.when(jnp.logical_not(live))
    def _():
        out_ref[...] = jnp.zeros_like(out_ref)

    for h in range(2):
        block = idx_ref[NEAR_ORDER + 2 * i + h]
        for seq in range(2):
            target = own_ref if seq == 0 else mate_ref
            copy = pltpu.make_async_copy(out_ref.at[pl.ds(h * BLOCK, BLOCK), :], target.at[block % 4], sem.at[h])
            pl.when(block // 4 == (idx_ref[CORE] + seq) % 2)(copy.start)
    for h in range(2):
        pltpu.make_async_copy(out_ref.at[pl.ds(h * BLOCK, BLOCK), :], own_ref.at[0], sem.at[h]).wait()


def dz_step(idx_ref, et_ref, l_ref, tok_ref, lab_ref, tl_ref, acc_ref, grad_ref):
    rows = et_ref.shape[1]
    size = grad_ref.shape[1]
    full = rows // size
    tail = rows - full * size
    lse = tok_ref[0, 0:1, :]
    weight = tok_ref[0, 1:2, :]
    label = lab_ref[0] - idx_ref[ROW_START]

    def grad(start, n, slot, target):
        tile = l_ref[0, pl.ds(start, n), :]
        is_target = lax.broadcasted_iota(jnp.int32, (n, PAIR), 0) == label - start
        grad_ref[slot, :n, :] = grad_tile(tile, lse, weight, is_target)
        return target + jnp.sum(jnp.where(is_target, tile, 0.0), axis=0, keepdims=True)

    def product(start, n, slot):
        return jnp.dot(et_ref[:, pl.ds(start, n)], grad_ref[slot, :n, :], preferred_element_type=jnp.float32)

    def step(k, target):
        start = pl.multiple_of(k * size, size)
        target = grad(start, size, k % 2, target)
        acc_ref[...] += product(pl.multiple_of(start - size, size), size, (k + 1) % 2)
        return target

    target = grad(0, size, 0, jnp.zeros((1, PAIR), jnp.float32))
    acc_ref[...] = jnp.zeros_like(acc_ref)
    target = lax.fori_loop(1, full, step, target)
    if tail:
        target = grad(full * size, tail, full % 2, target)
    acc_ref[...] += product((full - 1) * size, size, (full - 1) % 2)
    if tail:
        acc_ref[...] += product(full * size, tail, full % 2)
    tl_ref[0] = target


def de_kernel(offset, rows, got_offset, idx_ref, l_ref, z_ref, tok_ref, lab_ref, *rest):
    if got_offset is None:
        part_ref, out_ref, sem = rest[-3:]
        got_ref = None
    else:
        got_ref, part_ref, out_ref, sem = rest[0], rest[-3], rest[-2], rest[-1]
    i = pl.program_id(0)
    core = idx_ref[CORE]
    half = out_ref.shape[0] // 2
    count = idx_ref[ALL_PAIRS]
    lse = tok_ref[0, 0:1, :]
    weight = tok_ref[0, 1:2, :]
    label = lab_ref[0] - idx_ref[ROW_START] - offset

    def rows_at(side, start, n):
        return out_ref.at[pl.ds(pl.multiple_of(side * half + start, 8), n), :]

    own = pltpu.make_async_copy(part_ref, rows_at(core, offset, rows), sem.at[0])
    got = None
    if got_ref is not None:
        got = pltpu.make_async_copy(got_ref, rows_at(1 - core, got_offset, got_ref.shape[0]), sem.at[1])
        pl.when(i == 0)(got.start)

    def fill(first):
        for start, n in chunk_list(rows, 528):
            is_target = lax.broadcasted_iota(jnp.int32, (n, PAIR), 0) == label - start
            grad = grad_tile(l_ref[0, start:start + n, :], lse, weight, is_target)
            part = jnp.dot(grad, z_ref[0], preferred_element_type=jnp.float32)
            if first:
                part_ref[start:start + n, :] = part
            else:
                part_ref[start:start + n, :] += part

    pl.when(i == 0)(lambda: fill(True))
    pl.when((i > 0) & (i < count))(lambda: fill(False))
    pl.when(i == count - 1)(own.start)

    @pl.when(i == pl.num_programs(0) - 1)
    def _():
        own.wait()
        if got is not None:
            got.wait()


def place_kernel(got_offset, idx_ref, got_ref, de_ref, out_ref, sem):
    half = out_ref.shape[0] // 2
    start = pl.multiple_of((1 - idx_ref[CORE]) * half + got_offset, 8)
    copy = pltpu.make_async_copy(got_ref, out_ref.at[pl.ds(start, got_ref.shape[0]), :], sem)
    copy.start()
    copy.wait()


def params(n_dims=1):
    return pltpu.CompilerParams(vmem_limit_bytes=VMEM_LIMIT, dimension_semantics=("arbitrary",) * n_dims)


def cost(pairs, rows, width):
    n = PAIR * pairs * rows
    return pl.CostEstimate(flops=2 * n * width, bytes_accessed=4 * n, transcendentals=n)


ANY = pl.BlockSpec(memory_space=pl.ANY)


def call_logits(idx, e, z, previous, rows):
    pairs = 8
    base, count, order = (0, NEAR_PAIRS, NEAR_ORDER) if previous is None else (4, FAR_PAIRS, FAR_PIECES)
    width = e.shape[1]
    extra = [] if previous is None else list(previous)
    spec = pltpu.PrefetchScalarGridSpec(
        num_scalar_prefetch=1,
        grid=(4,),
        in_specs=[
            pl.BlockSpec((rows, width), lambda i, s: (s[CORE], 0), pipeline_mode=pl.Buffered(1)),
            pl.BlockSpec((1, BLOCK, width), lambda i, s: (s[order + 2 * last(i, s[count])], 0, 0)),
            pl.BlockSpec((1, BLOCK, width), lambda i, s: (s[order + 1 + 2 * last(i, s[count])], 0, 0)),
        ] + [ANY] * len(extra),
        out_specs=[
            pl.BlockSpec((1, rows, PAIR), lambda i, s: (base + last(i, s[count]), 0, 0)),
            pl.BlockSpec((1, PAIR, width), lambda i, s: (base + last(i, s[count]), 0, 0)),
            pl.BlockSpec((1, 2, PAIR), lambda i, s: (last(i, s[count]), 0, 0)),
        ],
    )
    return pl.pallas_call(
        functools.partial(logits_kernel, count),
        grid_spec=spec,
        out_shape=[
            jax.ShapeDtypeStruct((pairs, rows, PAIR), jnp.float32),
            jax.ShapeDtypeStruct((pairs, PAIR, width), jnp.bfloat16),
            jax.ShapeDtypeStruct((4, 2, PAIR), jnp.float32),
        ],
        input_output_aliases={} if previous is None else {4: 0, 5: 1},
        compiler_params=params(),
        cost_estimate=cost(3, rows, width),
        name="logits_near" if previous is None else "logits_far",
    )(idx, e, z, z, *extra)


def call_dz(idx, et, l, tok, lab):
    width, rows = et.shape
    pick_row = lambda i, s: (last(i, s[NEAR_PAIRS]), 0, 0)
    spec = pltpu.PrefetchScalarGridSpec(
        num_scalar_prefetch=1,
        grid=(4,),
        in_specs=[
            pl.BlockSpec((width, rows), lambda i, s: (0, 0), pipeline_mode=pl.Buffered(1)),
            pl.BlockSpec((1, rows, PAIR), pick_row),
            pl.BlockSpec((1, 2, PAIR), pick_row),
            pl.BlockSpec((1, 1, PAIR), pick_row),
        ],
        out_specs=[ANY, ANY, pl.BlockSpec((1, 1, PAIR), pick_row), ANY],
        scratch_shapes=[
            pltpu.VMEM((width, PAIR), jnp.float32),
            pltpu.VMEM((2, 512, PAIR), jnp.bfloat16),
            pltpu.VMEM((PAIR, width), jnp.float32),
            pltpu.SemaphoreType.DMA((2,)),
        ],
    )
    half = jax.ShapeDtypeStruct((4, BLOCK, width), jnp.float32)
    return pl.pallas_call(
        dz_kernel,
        grid_spec=spec,
        out_shape=[half, half, jax.ShapeDtypeStruct((4, 1, PAIR), jnp.float32), jax.ShapeDtypeStruct(l.shape, l.dtype)],
        input_output_aliases={2: 3},
        compiler_params=params(),
        cost_estimate=cost(3, rows, width),
        name="dz_part",
    )(idx, et, l, tok, lab)


def call_de(idx, l, zc, tok, lab, de, offset, rows, got, got_offset):
    total, width = l.shape[1], zc.shape[2]
    j = offset // rows
    pick_row = lambda i, s: (last(i, s[ALL_PAIRS]), 0, 0)
    extra = [] if de is None else [de]
    extra_specs = [ANY] * len(extra)
    if got is not None:
        extra = [got] + extra
        extra_specs = [pl.BlockSpec(got.shape, lambda i, s: (0, 0), pipeline_mode=pl.Buffered(1))] + extra_specs
    spec = pltpu.PrefetchScalarGridSpec(
        num_scalar_prefetch=1,
        grid=(8,),
        in_specs=[
            pl.BlockSpec((1, rows, PAIR), lambda i, s: (s[PAIR_IDS + last(i, s[ALL_PAIRS])], j, 0)),
            pl.BlockSpec((1, PAIR, width), lambda i, s: (s[PAIR_IDS + last(i, s[ALL_PAIRS])], 0, 0)),
            pl.BlockSpec((1, 2, PAIR), lambda i, s: (s[PAIR_IDS + last(i, s[ALL_PAIRS])], 0, 0)),
            pl.BlockSpec((1, 1, PAIR), lambda i, s: (s[PAIR_IDS + last(i, s[ALL_PAIRS])], 0, 0)),
        ] + extra_specs,
        out_specs=[pl.BlockSpec((rows, width), lambda i, s: (0, 0)), ANY],
        scratch_shapes=[pltpu.SemaphoreType.DMA((2,))],
    )
    return pl.pallas_call(
        functools.partial(de_kernel, offset, rows, got_offset if got is not None else None),
        grid_spec=spec,
        out_shape=[jax.ShapeDtypeStruct((rows, width), jnp.float32), jax.ShapeDtypeStruct((2 * total, width), jnp.float32)],
        input_output_aliases={} if de is None else {4 + len(extra): 1},
        compiler_params=params(),
        cost_estimate=cost(5, rows, width),
        name=f"de_{offset}",
    )(idx, l, zc, tok, lab, *extra)


def call_place(idx, got, de, got_offset):
    spec = pltpu.PrefetchScalarGridSpec(
        num_scalar_prefetch=1,
        grid=(1,),
        in_specs=[pl.BlockSpec(got.shape, lambda i, s: (0, 0), pipeline_mode=pl.Buffered(1)), ANY],
        out_specs=ANY,
        scratch_shapes=[pltpu.SemaphoreType.DMA],
    )
    return pl.pallas_call(
        functools.partial(place_kernel, got_offset),
        grid_spec=spec,
        out_shape=jax.ShapeDtypeStruct(de.shape, de.dtype),
        input_output_aliases={2: 0},
        compiler_params=params(),
        name="place",
    )(idx, got, de)


def order_blocks(active):
    n = active.shape[1]
    act = active.astype(jnp.int32)
    ids = jnp.arange(n, dtype=jnp.int32)
    before = (ids[None, :] < ids[:, None]).astype(jnp.int32)
    ahead = jnp.sum(before[None] * act[:, None, :], axis=2)
    count = jnp.sum(act, axis=1, keepdims=True)
    place = jnp.where(act > 0, ahead, count + ids - ahead)
    hit = place[:, None, :] == ids[None, :, None]
    return jnp.sum(jnp.where(hit, ids, 0), axis=2), count[:, 0], hit


def solution(mesh):
    n_tp, n_dp = mesh.shape['tp'], mesh.shape['dp']

    def flip(x, axis, bits):
        n = n_tp if axis == 'tp' else n_dp
        return lax.ppermute(x, axis, [(k, k ^ bits) for k in range(n)])

    def flip_both(x, tp_bits, dp_bits):
        return lax.ppermute(x, ('tp', 'dp'), [(k, ((k // n_dp) ^ tp_bits) * n_dp + ((k % n_dp) ^ dp_bits)) for k in range(n_tp * n_dp)])

    def from_group(x):
        return jnp.stack([x] + [flip_both(x, t, d) for t in range(4) for d in range(2) if (t, d) != (0, 0)])

    def pick(x, index):
        return lax.dynamic_index_in_dim(x, index, 0, keepdims=False)

    def local_step(hidden, ln_gamma, ln_beta, embed_shard, labels, loss_mask):
        tp, dp = lax.axis_index('tp'), lax.axis_index('dp')
        core = dp & 1
        y, z = tp & 1, tp >> 1
        seq, width = hidden.shape[1:]
        quarters, piece = seq // BLOCK, BLOCK // 2
        rows = embed_shard.shape[0] // 2
        row_start = tp * (2 * rows) + core * rows

        def by_core(mine, other):
            return jnp.stack([jnp.where(core == 0, mine, other), jnp.where(core == 0, other, mine)])

        x_float = hidden[0].astype(jnp.float32)
        centered = x_float - jnp.mean(x_float, axis=-1, keepdims=True)
        inv_std = lax.rsqrt(jnp.mean(centered * centered, axis=-1, keepdims=True) + LAYER_EPS)
        x_hat = centered * inv_std

        def to_z(values):
            return (values * ln_gamma + ln_beta).astype(jnp.bfloat16)

        marked = jnp.where(loss_mask[0] > 0, labels[0], -1)
        far_marks = [flip(marked, 'dp', 2), flip(marked, 'dp', 3)]
        marks = jnp.concatenate([by_core(marked, flip(marked, 'dp', 1)), by_core(*far_marks)]).reshape(2, 8, BLOCK)
        mate = flip(x_hat, 'dp', 1)
        own_quarter = pick(x_hat.reshape(quarters, BLOCK, width), tp)
        first = [flip(own_quarter[:piece], 'dp', 2), flip(own_quarter[piece:], 'dp', 2)]

        token_count = jnp.sum((marks >= 0).astype(jnp.float32))
        order, active, hit = order_blocks(jnp.any(marks >= 0, axis=2))
        lab = jnp.sum(jnp.where(hit[..., None], marks[:, None], 0), axis=2).reshape(8, 1, PAIR)
        pairs = (active + 1) // 2
        pair_ids = jnp.arange(8, dtype=jnp.int32)
        pair_idx = jnp.where(pair_ids < pairs[0], pair_ids, jnp.minimum(4 + pair_ids - pairs[0], 7))
        far_pieces = (order[1] & ~3) | ((order[1] & 3) ^ tp)
        zero = jnp.zeros((), jnp.int32)
        scalars = jnp.stack([core, pairs[0], pairs[1], pairs[0] + pairs[1], row_start, zero, zero, zero])
        idx = jnp.concatenate([scalars, order[0], far_pieces, pair_idx])
        embed_t = lax.dynamic_slice_in_dim(embed_shard, core * rows, rows, 0).T

        a0, b0 = first
        a1, b2 = flip(a0, 'tp', 1), flip(b0, 'tp', 2)
        a2, a3 = flip(a0, 'tp', 2), flip(a1, 'tp', 2)
        b1, b3 = flip(b0, 'tp', 1), flip(b2, 'tp', 1)
        far_x = [a0, b0, a1, b1, a2, b2, a3, b3]
        far_mate = [flip(v, 'dp', 1) for v in far_x]

        near_z = to_z(by_core(x_hat, mate)).reshape(2 * quarters, BLOCK, width)
        logits, z_pairs, near_stats = call_logits(idx, embed_shard, near_z, None, rows)

        def combine(every, labels_here):
            top = jnp.max(every[:, :, 0], axis=0)
            total = jnp.sum(every[:, :, 1] * jnp.exp(every[:, :, 0] - top), axis=0)
            live = labels_here[:, 0] >= 0
            lse = jnp.where(live, top + jnp.log(total), BIG)
            return jnp.stack([lse, jnp.where(live, 1.0 / token_count, 0.0)], axis=1), lse, live

        near_tok, near_lse, near_live = combine(from_group(near_stats), lab[:4])
        dz_own, dz_mate, target, logits = call_dz(idx, embed_t, logits, near_tok, lab[:4])

        part = dz_own + flip(dz_mate, 'dp', 1)
        part_gamma = jnp.sum(part * x_hat.reshape(quarters, BLOCK, width), axis=(0, 1))
        part_beta = jnp.sum(part, axis=(0, 1))
        lead = (tp == 0).astype(jnp.float32)
        loss = jnp.sum(jnp.where(near_live, jnp.where(core == 0, lead, 0.0) * near_lse - target[:, 0], 0.0)) / token_count
        sums = jnp.concatenate([part_gamma, part_beta, jnp.broadcast_to(loss, (512,))])

        grid_part = part.reshape(2, 2, BLOCK, width)
        a_part, b_part = grid_part[:, :, :piece], grid_part[:, :, piece:]
        a_keep = lax.dynamic_index_in_dim(a_part, y, 1, keepdims=False) + flip(lax.dynamic_index_in_dim(a_part, 1 - y, 1, keepdims=False), 'tp', 1)
        b_keep = pick(b_part, z) + flip(pick(b_part, 1 - z), 'tp', 2)
        a_grad = pick(a_keep, z) + flip(pick(a_keep, 1 - z), 'tp', 2)
        b_grad = pick(b_keep, y) + flip(pick(b_keep, 1 - y), 'tp', 1)
        grad = jnp.concatenate([a_grad, b_grad])

        far_z = to_z(by_core(jnp.concatenate(far_x), jnp.concatenate(far_mate))).reshape(2 * quarters, BLOCK, width)
        far_z, logits = lax.optimization_barrier((far_z, logits))
        logits, z_pairs, far_stats = call_logits(idx, embed_shard, far_z, (logits, z_pairs), rows)
        mixed = from_group(jnp.concatenate([far_stats.reshape(8, 512), sums.reshape(4, 512)]))
        far_tok, _, _ = combine(mixed[:, :8].reshape(8, 4, 2, PAIR), lab[4:])
        side_sums = jnp.sum(mixed[:, 8:], axis=0).reshape(-1)
        sums = side_sums + flip(side_sums, 'dp', 2)
        tok = jnp.concatenate([near_tok, far_tok])

        chunks = [(0, rows // 3), (rows // 3, rows // 3), (4 * (rows // 6), rows // 6), (5 * (rows // 6), rows // 6)]
        d_embed, got, got_offset = None, [], []
        for n, (offset, size) in enumerate(chunks):
            arrived = got[n - 2] if n >= 2 else None
            d_chunk, d_embed = call_de(idx, logits, z_pairs, tok, lab, d_embed, offset, size, arrived, chunks[n - 2][0] if n >= 2 else None)
            got.append(flip(d_chunk, 'dp', 1))
        for n in (2, 3):
            d_embed = call_place(idx, got[n], d_embed, chunks[n][0])

        hat = own_quarter
        scaled = grad * ln_gamma
        inner = scaled - jnp.mean(scaled, axis=-1, keepdims=True) - hat * jnp.mean(scaled * hat, axis=-1, keepdims=True)
        a0, b0 = inner[:piece], inner[piece:]
        a1, b2 = flip(a0, 'tp', 1), flip(b0, 'tp', 2)
        a2, a3 = flip(a0, 'tp', 2), flip(a1, 'tp', 2)
        b1, b3 = flip(b0, 'tp', 1), flip(b2, 'tp', 1)
        inner = jnp.stack([jnp.concatenate(v) for v in ((a0, b0), (a1, b1), (a2, b2), (a3, b3))])
        inner = jnp.stack([pick(inner, tp ^ q) for q in range(quarters)]).reshape(seq, width)
        d_hidden = (inner * inv_std).astype(jnp.bfloat16)[None]

        return sums[2 * width], d_hidden, d_embed, sums[:width], sums[width:2 * width]

    return jax.shard_map(local_step, mesh=mesh, in_specs=(P('dp', None, None), P(None), P(None), P('tp', None), P('dp', None), P('dp', None)), out_specs=(P(), P('dp', None, None), P('tp', None), P(None), P(None)), check_vma=False)
```

```python
import functools

import jax
import jax.numpy as jnp
from jax import lax
from jax.experimental import pallas as pl
from jax.experimental.pallas import tpu as pltpu
from jax.sharding import PartitionSpec as P


LAYER_EPS = 1e-5
BLOCK = 256
PAIR = 2 * BLOCK
BIG = 1e30
VMEM_LIMIT = 62 * 1024 * 1024


CORE, NEAR_PAIRS, FAR_PAIRS, ALL_PAIRS, ROW_START = 0, 1, 2, 3, 4
NEAR_ORDER, NEAR_PIECES, FAR_PIECES, PAIR_IDS = 8, 16, 24, 32


def chunk_list(total, size):
    return [(start, min(size, total - start)) for start in range(0, total, size)]


def last(i, count):
    return jnp.minimum(i, count - 1)


def logits_kernel(count, idx_ref, e_ref, za_ref, zb_ref, *rest):
    l_ref, zc_ref, st_ref = rest[-3:]
    pl.when(pl.program_id(0) < idx_ref[count])(lambda: logits_step(e_ref, za_ref, zb_ref, l_ref, zc_ref, st_ref))


def logits_step(e_ref, za_ref, zb_ref, l_ref, zc_ref, st_ref):
    zc_ref[0, :BLOCK, :] = za_ref[0]
    zc_ref[0, BLOCK:, :] = zb_ref[0]
    rows = e_ref.shape[0]
    size = 528

    top = jnp.full((1, PAIR), -BIG, jnp.float32)
    total = jnp.zeros((1, PAIR), jnp.float32)

    def add(start, n, old_top, top, total):
        return total * jnp.exp(old_top - top) + jnp.sum(jnp.exp(l_ref[0, start:start + n, :] - top), axis=0, keepdims=True)

    waiting = None
    for start, n in chunk_list(rows, size):
        tile = lax.dot_general(e_ref[start:start + n, :], zc_ref[0], (((1,), (1,)), ((), ())), preferred_element_type=jnp.float32)
        l_ref[0, start:start + n, :] = tile
        new_top = jnp.maximum(top, jnp.max(tile, axis=0, keepdims=True))
        if waiting is not None:
            total = add(*waiting, total)
        waiting = (start, n, top, new_top)
        top = new_top
    total = add(*waiting, total)
    st_ref[0, 0:1, :] = top
    st_ref[0, 1:2, :] = total


def grad_tile(tile, lse, weight, is_target):
    probs = jnp.exp(tile - lse)
    return (jnp.where(is_target, probs - 1.0, probs) * weight).astype(jnp.bfloat16)


def dz_kernel(idx_ref, e_ref, l_ref, tok_ref, lab_ref, own_ref, mate_ref, tl_ref, l_out_ref, acc_ref, out_ref, et_ref, sem):
    i = pl.program_id(0)
    rows = e_ref.shape[0]
    size = 512
    full = rows // size

    @pl.when(i == 0)
    def _():
        def turn(k, carry):
            start = pl.multiple_of(k * size, size)
            et_ref[:, pl.ds(start, size)] = e_ref[pl.ds(start, size), :].T
            return carry

        lax.fori_loop(0, full, turn, 0)
        if rows > full * size:
            et_ref[:, full * size:] = e_ref[full * size:, :].T

    live = i < idx_ref[NEAR_PAIRS]
    pl.when(live)(lambda: dz_step(idx_ref, et_ref, l_ref, tok_ref, lab_ref, tl_ref, acc_ref))

    @pl.when(live)
    def _():
        out_ref[...] = acc_ref[...].T

    @pl.when(jnp.logical_not(live))
    def _():
        out_ref[...] = jnp.zeros_like(out_ref)

    for h in range(2):
        block = idx_ref[NEAR_ORDER + 2 * i + h]
        for seq in range(2):
            target = own_ref if seq == 0 else mate_ref
            copy = pltpu.make_async_copy(out_ref.at[pl.ds(h * BLOCK, BLOCK), :], target.at[block % 4], sem.at[h])
            pl.when(block // 4 == (idx_ref[CORE] + seq) % 2)(copy.start)
    for h in range(2):
        pltpu.make_async_copy(out_ref.at[pl.ds(h * BLOCK, BLOCK), :], own_ref.at[0], sem.at[h]).wait()


def dz_step(idx_ref, et_ref, l_ref, tok_ref, lab_ref, tl_ref, acc_ref):
    lse = tok_ref[0, 0:1, :]
    weight = tok_ref[0, 1:2, :]
    label = lab_ref[0] - idx_ref[ROW_START]
    target = jnp.zeros((1, PAIR), jnp.float32)
    for start, n in chunk_list(et_ref.shape[1], 1024):
        tile = l_ref[0, start:start + n, :]
        is_target = lax.broadcasted_iota(jnp.int32, (n, PAIR), 0) == label - start
        grad = grad_tile(tile, lse, weight, is_target)
        target = target + jnp.sum(jnp.where(is_target, tile, 0.0), axis=0, keepdims=True)
        part = jnp.dot(et_ref[:, start:start + n], grad, preferred_element_type=jnp.float32)
        if start == 0:
            acc_ref[...] = part
        else:
            acc_ref[...] += part
    tl_ref[0] = target


def de_kernel(offset, rows, got_offset, idx_ref, l_ref, z_ref, tok_ref, lab_ref, *rest):
    if got_offset is None:
        part_ref, out_ref, sem = rest[-3:]
        got_ref = None
    else:
        got_ref, part_ref, out_ref, sem = rest[0], rest[-3], rest[-2], rest[-1]
    i = pl.program_id(0)
    core = idx_ref[CORE]
    half = out_ref.shape[0] // 2
    count = idx_ref[ALL_PAIRS]
    lse = tok_ref[0, 0:1, :]
    weight = tok_ref[0, 1:2, :]
    label = lab_ref[0] - idx_ref[ROW_START] - offset

    def rows_at(side, start, n):
        return out_ref.at[pl.ds(pl.multiple_of(side * half + start, 8), n), :]

    own = pltpu.make_async_copy(part_ref, rows_at(core, offset, rows), sem.at[0])
    got = None
    if got_ref is not None:
        got = pltpu.make_async_copy(got_ref, rows_at(1 - core, got_offset, got_ref.shape[0]), sem.at[1])
        pl.when(i == 0)(got.start)

    @pl.when(i == 0)
    def _():
        part_ref[...] = jnp.zeros_like(part_ref)

    @pl.when(i < count)
    def _():
        for start, n in chunk_list(rows, 528):
            is_target = lax.broadcasted_iota(jnp.int32, (n, PAIR), 0) == label - start
            grad = grad_tile(l_ref[0, start:start + n, :], lse, weight, is_target)
            part_ref[start:start + n, :] += jnp.dot(grad, z_ref[0], preferred_element_type=jnp.float32)

    pl.when(i == count - 1)(own.start)

    @pl.when(i == pl.num_programs(0) - 1)
    def _():
        own.wait()
        if got is not None:
            got.wait()


def place_kernel(got_offset, idx_ref, got_ref, de_ref, out_ref, sem):
    half = out_ref.shape[0] // 2
    start = pl.multiple_of((1 - idx_ref[CORE]) * half + got_offset, 8)
    copy = pltpu.make_async_copy(got_ref, out_ref.at[pl.ds(start, got_ref.shape[0]), :], sem)
    copy.start()
    copy.wait()


def params(limit=VMEM_LIMIT):
    return pltpu.CompilerParams(vmem_limit_bytes=limit, dimension_semantics=("arbitrary",))


def cost(pairs, rows, width):
    n = PAIR * pairs * rows
    return pl.CostEstimate(flops=2 * n * width, bytes_accessed=4 * n, transcendentals=n)


ANY = pl.BlockSpec(memory_space=pl.ANY)


def call_logits(idx, e, z, previous, rows):
    pairs = 8
    base, count, order = (0, NEAR_PAIRS, NEAR_PIECES) if previous is None else (4, FAR_PAIRS, FAR_PIECES)
    width = e.shape[1]
    extra = [] if previous is None else list(previous)
    spec = pltpu.PrefetchScalarGridSpec(
        num_scalar_prefetch=1,
        grid=(4,),
        in_specs=[
            pl.BlockSpec((rows, width), lambda i, s: (s[CORE], 0), pipeline_mode=pl.Buffered(1)),
            pl.BlockSpec((1, BLOCK, width), lambda i, s: (s[order + 2 * last(i, s[count])], 0, 0)),
            pl.BlockSpec((1, BLOCK, width), lambda i, s: (s[order + 1 + 2 * last(i, s[count])], 0, 0)),
        ] + [ANY] * len(extra),
        out_specs=[
            pl.BlockSpec((1, rows, PAIR), lambda i, s: (base + last(i, s[count]), 0, 0)),
            pl.BlockSpec((1, PAIR, width), lambda i, s: (base + last(i, s[count]), 0, 0)),
            pl.BlockSpec((1, 2, PAIR), lambda i, s: (last(i, s[count]), 0, 0)),
        ],
    )
    return pl.pallas_call(
        functools.partial(logits_kernel, count),
        grid_spec=spec,
        out_shape=[
            jax.ShapeDtypeStruct((pairs, rows, PAIR), jnp.float32),
            jax.ShapeDtypeStruct((pairs, PAIR, width), jnp.bfloat16),
            jax.ShapeDtypeStruct((4, 2, PAIR), jnp.float32),
        ],
        input_output_aliases={} if previous is None else {4: 0, 5: 1},
        compiler_params=params(),
        cost_estimate=cost(3, rows, width),
        name="logits_near" if previous is None else "logits_far",
    )(idx, e, z, z, *extra)


def call_dz(idx, e, l, tok, lab):
    width, rows = e.shape[1], l.shape[1]
    pick_row = lambda i, s: (last(i, s[NEAR_PAIRS]), 0, 0)
    spec = pltpu.PrefetchScalarGridSpec(
        num_scalar_prefetch=1,
        grid=(4,),
        in_specs=[
            pl.BlockSpec((rows, width), lambda i, s: (s[CORE], 0), pipeline_mode=pl.Buffered(1)),
            pl.BlockSpec((1, rows, PAIR), pick_row),
            pl.BlockSpec((1, 2, PAIR), pick_row),
            pl.BlockSpec((1, 1, PAIR), pick_row),
        ],
        out_specs=[ANY, ANY, pl.BlockSpec((1, 1, PAIR), pick_row), ANY],
        scratch_shapes=[
            pltpu.VMEM((width, PAIR), jnp.float32),
            pltpu.VMEM((PAIR, width), jnp.float32),
            pltpu.VMEM((width, rows), jnp.bfloat16),
            pltpu.SemaphoreType.DMA((2,)),
        ],
    )
    half = jax.ShapeDtypeStruct((4, BLOCK, width), jnp.float32)
    return pl.pallas_call(
        dz_kernel,
        grid_spec=spec,
        out_shape=[half, half, jax.ShapeDtypeStruct((4, 1, PAIR), jnp.float32), jax.ShapeDtypeStruct(l.shape, l.dtype)],
        input_output_aliases={2: 3},
        compiler_params=params(),
        cost_estimate=cost(3, rows, width),
        name="dz_part",
    )(idx, e, l, tok, lab)


def call_de(idx, l, zc, tok, lab, de, offset, rows, got, got_offset):
    total, width = l.shape[1], zc.shape[2]
    j = offset // rows
    extra = [] if de is None else [de]
    extra_specs = [ANY] * len(extra)
    if got is not None:
        extra = [got] + extra
        extra_specs = [pl.BlockSpec(got.shape, lambda i, s: (0, 0), pipeline_mode=pl.Buffered(1))] + extra_specs
    spec = pltpu.PrefetchScalarGridSpec(
        num_scalar_prefetch=1,
        grid=(8,),
        in_specs=[
            pl.BlockSpec((1, rows, PAIR), lambda i, s: (s[PAIR_IDS + last(i, s[ALL_PAIRS])], j, 0)),
            pl.BlockSpec((1, PAIR, width), lambda i, s: (s[PAIR_IDS + last(i, s[ALL_PAIRS])], 0, 0)),
            pl.BlockSpec((1, 2, PAIR), lambda i, s: (s[PAIR_IDS + last(i, s[ALL_PAIRS])], 0, 0)),
            pl.BlockSpec((1, 1, PAIR), lambda i, s: (s[PAIR_IDS + last(i, s[ALL_PAIRS])], 0, 0)),
        ] + extra_specs,
        out_specs=[pl.BlockSpec((rows, width), lambda i, s: (0, 0)), ANY],
        scratch_shapes=[pltpu.SemaphoreType.DMA((2,))],
    )
    return pl.pallas_call(
        functools.partial(de_kernel, offset, rows, got_offset if got is not None else None),
        grid_spec=spec,
        out_shape=[jax.ShapeDtypeStruct((rows, width), jnp.float32), jax.ShapeDtypeStruct((2 * total, width), jnp.float32)],
        input_output_aliases={} if de is None else {4 + len(extra): 1},
        compiler_params=params(),
        cost_estimate=cost(5, rows, width),
    )(idx, l, zc, tok, lab, *extra)


def call_place(idx, got, de, got_offset):
    spec = pltpu.PrefetchScalarGridSpec(
        num_scalar_prefetch=1,
        grid=(1,),
        in_specs=[pl.BlockSpec(got.shape, lambda i, s: (0, 0), pipeline_mode=pl.Buffered(1)), ANY],
        out_specs=ANY,
        scratch_shapes=[pltpu.SemaphoreType.DMA],
    )
    return pl.pallas_call(
        functools.partial(place_kernel, got_offset),
        grid_spec=spec,
        out_shape=jax.ShapeDtypeStruct(de.shape, de.dtype),
        input_output_aliases={2: 0},
        compiler_params=params(),
        name="place",
    )(idx, got, de)


def order_blocks(active):
    n = active.shape[1]
    act = active.astype(jnp.int32)
    ids = jnp.arange(n, dtype=jnp.int32)
    before = (ids[None, :] < ids[:, None]).astype(jnp.int32)
    ahead = jnp.sum(before[None] * act[:, None, :], axis=2)
    count = jnp.sum(act, axis=1, keepdims=True)
    place = jnp.where(act > 0, ahead, count + ids - ahead)
    hit = place[:, None, :] == ids[None, :, None]
    return jnp.sum(jnp.where(hit, ids, 0), axis=2), count[:, 0], hit


def solution(mesh):
    n_tp, n_dp = mesh.shape['tp'], mesh.shape['dp']

    def flip(x, axis, bits):
        n = n_tp if axis == 'tp' else n_dp
        return lax.ppermute(x, axis, [(k, k ^ bits) for k in range(n)])

    def flip_both(x, tp_bits, dp_bits):
        return lax.ppermute(x, ('tp', 'dp'), [(k, ((k // n_dp) ^ tp_bits) * n_dp + ((k % n_dp) ^ dp_bits)) for k in range(n_tp * n_dp)])

    def from_group(x):
        return jnp.stack([x] + [flip_both(x, t, d) for t in range(4) for d in range(2) if (t, d) != (0, 0)])

    def pick(x, index):
        return lax.dynamic_index_in_dim(x, index, 0, keepdims=False)

    def local_step(hidden, ln_gamma, ln_beta, embed_shard, labels, loss_mask):
        tp, dp = lax.axis_index('tp'), lax.axis_index('dp')
        core = dp & 1
        y, z = tp & 1, tp >> 1
        seq, width = hidden.shape[1:]
        quarters, piece = seq // BLOCK, BLOCK // 2
        rows = embed_shard.shape[0] // 2
        row_start = tp * (2 * rows) + core * rows

        def by_core(mine, other):
            return jnp.stack([jnp.where(core == 0, mine, other), jnp.where(core == 0, other, mine)])

        marked = jnp.where(loss_mask[0] > 0, labels[0], -1)
        far_marks = [flip(marked, 'dp', 2), flip(marked, 'dp', 3)]
        mate_marks = flip(marked, 'dp', 1)

        x_float = hidden[0].astype(jnp.float32)
        centered = x_float - jnp.mean(x_float, axis=-1, keepdims=True)
        inv_std = lax.rsqrt(jnp.mean(centered * centered, axis=-1, keepdims=True) + LAYER_EPS)
        x_hat = (centered * inv_std).reshape(quarters, BLOCK, width)

        def to_z(values):
            return (values * ln_gamma + ln_beta).astype(jnp.bfloat16)

        mate = flip(x_hat, 'dp', 1)
        own_quarter, far_quarter = lax.optimization_barrier((pick(x_hat, tp), pick(x_hat, tp ^ 3)))
        far0, far3 = flip(own_quarter, 'dp', 2), flip(far_quarter, 'dp', 2)

        marks = jnp.concatenate([by_core(marked, mate_marks), by_core(*far_marks)]).reshape(2, 8, BLOCK)
        token_count = jnp.sum((marks >= 0).astype(jnp.float32))
        order, active, hit = order_blocks(jnp.any(marks >= 0, axis=2))
        lab = jnp.sum(jnp.where(hit[..., None], marks[:, None], 0), axis=2).reshape(8, 1, PAIR)
        pairs = (active + 1) // 2
        pair_ids = jnp.arange(8, dtype=jnp.int32)
        pair_idx = jnp.where(pair_ids < pairs[0], pair_ids, jnp.minimum(4 + pair_ids - pairs[0], 7))
        zero = jnp.zeros((), jnp.int32)
        scalars = jnp.stack([core, pairs[0], pairs[1], pairs[0] + pairs[1], row_start, zero, zero, zero])
        idx = jnp.concatenate([scalars, order[0], order[0] ^ (core * 4), order[1] ^ (core * 4 + tp), pair_idx])

        near_z = to_z(jnp.concatenate([x_hat, mate]))
        logits, z_pairs, near_stats = call_logits(idx, embed_shard, near_z, None, rows)

        def combine(every, labels_here):
            top = jnp.max(every[:, :, 0], axis=0)
            total = jnp.sum(every[:, :, 1] * jnp.exp(every[:, :, 0] - top), axis=0)
            live = labels_here[:, 0] >= 0
            lse = jnp.where(live, top + jnp.log(total), BIG)
            return jnp.stack([lse, jnp.where(live, 1.0 / token_count, 0.0)], axis=1), lse, live

        near_tok, near_lse, near_live = combine(from_group(near_stats), lab[:4])
        mate0, mate3 = flip(far0, 'dp', 1), flip(far3, 'dp', 1)
        far1, far2 = flip(far0, 'tp', 1), flip(far0, 'tp', 2)
        dz_own, dz_mate, target, logits = call_dz(idx, embed_shard, logits, near_tok, lab[:4])

        mate1, mate2 = flip(far1, 'dp', 1), flip(far2, 'dp', 1)
        part = dz_own + flip(dz_mate, 'dp', 1)
        grid_part = part.reshape(2, 2, BLOCK, width)
        a_part, b_part = grid_part[:, :, :piece], grid_part[:, :, piece:]
        a_got = flip(lax.dynamic_index_in_dim(a_part, 1 - y, 1, keepdims=False), 'tp', 1)
        b_got = flip(pick(b_part, 1 - z), 'tp', 2)
        a_keep = lax.dynamic_index_in_dim(a_part, y, 1, keepdims=False) + a_got
        b_keep = pick(b_part, z) + b_got

        pieces, logits = lax.optimization_barrier(([far0, far1, far2, far3, mate0, mate1, mate2, mate3], logits))
        far_z = to_z(jnp.stack(pieces))
        logits, z_pairs, far_stats = call_logits(idx, embed_shard, far_z, (logits, z_pairs), rows)
        far_tok, _, _ = combine(from_group(far_stats), lab[4:])
        a_grad = flip(pick(a_keep, 1 - z), 'tp', 2)
        b_grad = flip(pick(b_keep, 1 - y), 'tp', 1)
        grad = jnp.concatenate([pick(a_keep, z) + a_grad, pick(b_keep, y) + b_grad])
        tok = jnp.concatenate([near_tok, far_tok])

        hat = own_quarter
        scaled = grad * ln_gamma
        inner = scaled - jnp.mean(scaled, axis=-1, keepdims=True) - hat * jnp.mean(scaled * hat, axis=-1, keepdims=True)
        a0, b0 = inner[:piece], inner[piece:]
        a1, b2 = flip(a0, 'tp', 1), flip(b0, 'tp', 2)
        a2, a3 = flip(a0, 'tp', 2), flip(a1, 'tp', 2)
        b1, b3 = flip(b0, 'tp', 1), flip(b2, 'tp', 1)
        gathered = jnp.stack([jnp.concatenate(v) for v in ((a0, b0), (a1, b1), (a2, b2), (a3, b3))])
        gathered = jnp.stack([pick(gathered, tp ^ q) for q in range(quarters)]).reshape(seq, width)
        d_hidden = (gathered * inv_std).astype(jnp.bfloat16)[None]

        lead = ((tp == 0) & (core == 0)).astype(jnp.float32)
        loss = jnp.sum(jnp.where(near_live, lead * near_lse - target[:, 0], 0.0)) / token_count
        sums = jnp.concatenate([jnp.sum(grad * hat, axis=0), jnp.sum(grad, axis=0), jnp.broadcast_to(loss, (512,))]).reshape(4, 512)
        for bits in (1, 2):
            got_sums = flip(sums, 'dp', bits)
            sums = sums + got_sums
        got_sums = [flip(sums, 'tp', k) for k in (1, 2, 3)]
        sums = (sums + got_sums[0] + (got_sums[1] + got_sums[2])).reshape(-1)

        chunks = [(0, rows // 3), (rows // 3, rows // 3), (4 * (rows // 6), rows // 6), (5 * (rows // 6), rows // 6)]
        d_embed, got = None, []
        for n, (offset, size) in enumerate(chunks):
            arrived = got[n - 2] if n >= 2 else None
            d_chunk, d_embed = call_de(idx, logits, z_pairs, tok, lab, d_embed, offset, size, arrived, chunks[n - 2][0] if n >= 2 else None)
            got.append(flip(d_chunk, 'dp', 1))
        for n in (2, 3):
            d_embed = call_place(idx, got[n], d_embed, chunks[n][0])

        return sums[2 * width], d_hidden, d_embed, sums[:width], sums[width:2 * width]


    return jax.shard_map(local_step, mesh=mesh, in_specs=(P('dp', None, None), P(None), P(None), P('tp', None), P('dp', None), P('dp', None)), out_specs=(P(), P('dp', None, None), P('tp', None), P(None), P(None)), check_vma=False)
```

```python
import functools

import jax
import jax.numpy as jnp
from jax import lax
from jax.experimental import pallas as pl
from jax.experimental.pallas import tpu as pltpu
from jax.sharding import PartitionSpec as P


LAYER_EPS = 1e-5
BLOCK = 256
PAIR = 2 * BLOCK
BIG = 1e30
VMEM_LIMIT = 62 * 1024 * 1024
DE_VMEM = 28 * 1024 * 1024


CORE, NEAR_PAIRS, FAR_PAIRS, ALL_PAIRS, ROW_START = 0, 1, 2, 3, 4
NEAR_ORDER, NEAR_PIECES, FAR_PIECES, PAIR_IDS = 8, 16, 24, 32


def chunk_list(total, size):
    return [(start, min(size, total - start)) for start in range(0, total, size)]


def last(i, count):
    return jnp.minimum(i, count - 1)


def logits_kernel(count, order, n_pieces, idx_ref, e_ref, gamma_ref, beta_ref, *rest):
    pieces = rest[:n_pieces]
    l_ref, zc_ref, st_ref, x_ref, sem = rest[-5:]
    i = pl.program_id(0)

    def copies(block, slot, h):
        target = x_ref.at[slot, pl.ds(h * BLOCK, BLOCK), :]
        if len(pieces[0].shape) == 3:
            return [(block >> 2 == k, pltpu.make_async_copy(ref.at[block & 3], target, sem.at[slot, h])) for k, ref in enumerate(pieces)]
        return [(block == k, pltpu.make_async_copy(ref, target, sem.at[slot, h])) for k, ref in enumerate(pieces)]

    def fetch(pair):
        for h in range(2):
            for chosen, copy in copies(idx_ref[order + 2 * pair + h], pair % 2, h):
                pl.when(chosen)(copy.start)

    pl.when(i == 0)(lambda: fetch(0))
    pl.when(i + 1 < idx_ref[count])(lambda: fetch(i + 1))

    @pl.when(i < idx_ref[count])
    def _():
        for h in range(2):
            copies(0, i % 2, h)[0][1].wait()
        zc_ref[0] = (x_ref[i % 2] * gamma_ref[...] + beta_ref[...]).astype(jnp.bfloat16)
        logits_step(e_ref, l_ref, zc_ref, st_ref)


def logits_step(e_ref, l_ref, zc_ref, st_ref):
    rows = e_ref.shape[0]
    size = 528

    top = jnp.full((1, PAIR), -BIG, jnp.float32)
    total = jnp.zeros((1, PAIR), jnp.float32)

    def add(start, n, old_top, top, total):
        return total * jnp.exp(old_top - top) + jnp.sum(jnp.exp(l_ref[0, start:start + n, :] - top), axis=0, keepdims=True)

    waiting = None
    for start, n in chunk_list(rows, size):
        tile = lax.dot_general(e_ref[start:start + n, :], zc_ref[0], (((1,), (1,)), ((), ())), preferred_element_type=jnp.float32)
        l_ref[0, start:start + n, :] = tile
        new_top = jnp.maximum(top, jnp.max(tile, axis=0, keepdims=True))
        if waiting is not None:
            total = add(*waiting, total)
        waiting = (start, n, top, new_top)
        top = new_top
    total = add(*waiting, total)
    st_ref[0, 0:1, :] = top
    st_ref[0, 1:2, :] = total


def grad_tile(tile, lse, weight, is_target):
    probs = jnp.exp(tile - lse)
    return (jnp.where(is_target, probs - 1.0, probs) * weight).astype(jnp.bfloat16)


def dz_kernel(idx_ref, e_ref, l_ref, tok_ref, lab_ref, own_ref, mate_ref, tl_ref, l_out_ref, acc_ref, out_ref, et_ref, sem):
    i = pl.program_id(0)
    rows = e_ref.shape[0]
    size = 512
    full = rows // size

    @pl.when(i == 0)
    def _():
        def turn(k, carry):
            start = pl.multiple_of(k * size, size)
            et_ref[:, pl.ds(start, size)] = e_ref[pl.ds(start, size), :].T
            return carry

        lax.fori_loop(0, full, turn, 0)
        if rows > full * size:
            et_ref[:, full * size:] = e_ref[full * size:, :].T

    live = i < idx_ref[NEAR_PAIRS]
    pl.when(live)(lambda: dz_step(idx_ref, et_ref, l_ref, tok_ref, lab_ref, tl_ref, acc_ref))

    @pl.when(live)
    def _():
        out_ref[...] = acc_ref[...].T

    @pl.when(jnp.logical_not(live))
    def _():
        out_ref[...] = jnp.zeros_like(out_ref)

    for h in range(2):
        block = idx_ref[NEAR_ORDER + 2 * i + h]
        for seq in range(2):
            target = own_ref if seq == 0 else mate_ref
            copy = pltpu.make_async_copy(out_ref.at[pl.ds(h * BLOCK, BLOCK), :], target.at[block % 4], sem.at[h])
            pl.when(block // 4 == (idx_ref[CORE] + seq) % 2)(copy.start)
    for h in range(2):
        pltpu.make_async_copy(out_ref.at[pl.ds(h * BLOCK, BLOCK), :], own_ref.at[0], sem.at[h]).wait()


def dz_step(idx_ref, et_ref, l_ref, tok_ref, lab_ref, tl_ref, acc_ref):
    lse = tok_ref[0, 0:1, :]
    weight = tok_ref[0, 1:2, :]
    label = lab_ref[0] - idx_ref[ROW_START]
    target = jnp.zeros((1, PAIR), jnp.float32)
    for start, n in chunk_list(et_ref.shape[1], 1024):
        tile = l_ref[0, start:start + n, :]
        is_target = lax.broadcasted_iota(jnp.int32, (n, PAIR), 0) == label - start
        grad = grad_tile(tile, lse, weight, is_target)
        target = target + jnp.sum(jnp.where(is_target, tile, 0.0), axis=0, keepdims=True)
        part = jnp.dot(et_ref[:, start:start + n], grad, preferred_element_type=jnp.float32)
        if start == 0:
            acc_ref[...] = part
        else:
            acc_ref[...] += part
    tl_ref[0] = target


def de_kernel(offset, rows, got_offset, idx_ref, l_ref, z_ref, tok_ref, lab_ref, *rest):
    if got_offset is None:
        part_ref, out_ref, sem = rest[-3:]
        got_ref = None
    else:
        got_ref, part_ref, out_ref, sem = rest[0], rest[-3], rest[-2], rest[-1]
    i = pl.program_id(0)
    core = idx_ref[CORE]
    half = out_ref.shape[0] // 2
    count = idx_ref[ALL_PAIRS]
    lse = tok_ref[0, 0:1, :]
    weight = tok_ref[0, 1:2, :]
    label = lab_ref[0] - idx_ref[ROW_START] - offset

    def rows_at(side, start, n):
        return out_ref.at[pl.ds(pl.multiple_of(side * half + start, 8), n), :]

    own = pltpu.make_async_copy(part_ref, rows_at(core, offset, rows), sem.at[0])
    got = None
    if got_ref is not None:
        got = pltpu.make_async_copy(got_ref, rows_at(1 - core, got_offset, got_ref.shape[0]), sem.at[1])
        pl.when(i == 0)(got.start)

    @pl.when(i == 0)
    def _():
        part_ref[...] = jnp.zeros_like(part_ref)

    @pl.when(i < count)
    def _():
        for start, n in chunk_list(rows, 528):
            is_target = lax.broadcasted_iota(jnp.int32, (n, PAIR), 0) == label - start
            grad = grad_tile(l_ref[0, start:start + n, :], lse, weight, is_target)
            part_ref[start:start + n, :] += jnp.dot(grad, z_ref[0], preferred_element_type=jnp.float32)

    pl.when(i == count - 1)(own.start)

    @pl.when(i == pl.num_programs(0) - 1)
    def _():
        own.wait()
        if got is not None:
            got.wait()


def place_kernel(got_offset, idx_ref, got_ref, de_ref, out_ref, sem):
    half = out_ref.shape[0] // 2
    start = pl.multiple_of((1 - idx_ref[CORE]) * half + got_offset, 8)
    copy = pltpu.make_async_copy(got_ref, out_ref.at[pl.ds(start, got_ref.shape[0]), :], sem)
    copy.start()
    copy.wait()


def params(limit=VMEM_LIMIT):
    return pltpu.CompilerParams(vmem_limit_bytes=limit, dimension_semantics=("arbitrary",))


def cost(pairs, rows, width):
    n = PAIR * pairs * rows
    return pl.CostEstimate(flops=2 * n * width, bytes_accessed=4 * n, transcendentals=n)


ANY = pl.BlockSpec(memory_space=pl.ANY)


def call_logits(idx, e, gamma, beta, pieces, previous, rows):
    pairs = 8
    base, count, order = (0, NEAR_PAIRS, NEAR_PIECES) if previous is None else (4, FAR_PAIRS, FAR_PIECES)
    width = e.shape[1]
    extra = [] if previous is None else list(previous)
    spec = pltpu.PrefetchScalarGridSpec(
        num_scalar_prefetch=1,
        grid=(4,),
        in_specs=[pl.BlockSpec((rows, width), lambda i, s: (s[CORE], 0), pipeline_mode=pl.Buffered(1))]
        + [pl.BlockSpec((1, width), lambda i, s: (0, 0))] * 2 + [ANY] * (len(pieces) + len(extra)),
        out_specs=[
            pl.BlockSpec((1, rows, PAIR), lambda i, s: (base + last(i, s[count]), 0, 0)),
            pl.BlockSpec((1, PAIR, width), lambda i, s: (base + last(i, s[count]), 0, 0)),
            pl.BlockSpec((1, 2, PAIR), lambda i, s: (last(i, s[count]), 0, 0)),
        ],
        scratch_shapes=[pltpu.VMEM((2, PAIR, width), jnp.float32), pltpu.SemaphoreType.DMA((2, 2))],
    )
    first = 4 + len(pieces)
    return pl.pallas_call(
        functools.partial(logits_kernel, count, order, len(pieces)),
        grid_spec=spec,
        out_shape=[
            jax.ShapeDtypeStruct((pairs, rows, PAIR), jnp.float32),
            jax.ShapeDtypeStruct((pairs, PAIR, width), jnp.bfloat16),
            jax.ShapeDtypeStruct((4, 2, PAIR), jnp.float32),
        ],
        input_output_aliases={} if previous is None else {first: 0, first + 1: 1},
        compiler_params=params(),
        cost_estimate=cost(3, rows, width),
        name="logits_near" if previous is None else "logits_far",
    )(idx, e, gamma[None], beta[None], *pieces, *extra)


def call_dz(idx, e, l, tok, lab):
    width, rows = e.shape[1], l.shape[1]
    pick_row = lambda i, s: (last(i, s[NEAR_PAIRS]), 0, 0)
    spec = pltpu.PrefetchScalarGridSpec(
        num_scalar_prefetch=1,
        grid=(4,),
        in_specs=[
            pl.BlockSpec((rows, width), lambda i, s: (s[CORE], 0), pipeline_mode=pl.Buffered(1)),
            pl.BlockSpec((1, rows, PAIR), pick_row),
            pl.BlockSpec((1, 2, PAIR), pick_row),
            pl.BlockSpec((1, 1, PAIR), pick_row),
        ],
        out_specs=[ANY, ANY, pl.BlockSpec((1, 1, PAIR), pick_row), ANY],
        scratch_shapes=[
            pltpu.VMEM((width, PAIR), jnp.float32),
            pltpu.VMEM((PAIR, width), jnp.float32),
            pltpu.VMEM((width, rows), jnp.bfloat16),
            pltpu.SemaphoreType.DMA((2,)),
        ],
    )
    half = jax.ShapeDtypeStruct((4, BLOCK, width), jnp.float32)
    return pl.pallas_call(
        dz_kernel,
        grid_spec=spec,
        out_shape=[half, half, jax.ShapeDtypeStruct((4, 1, PAIR), jnp.float32), jax.ShapeDtypeStruct(l.shape, l.dtype)],
        input_output_aliases={2: 3},
        compiler_params=params(),
        cost_estimate=cost(3, rows, width),
        name="dz_part",
    )(idx, e, l, tok, lab)


def call_de(idx, l, zc, tok, lab, de, offset, rows, got, got_offset):
    total, width = l.shape[1], zc.shape[2]
    j = offset // rows
    extra = [] if de is None else [de]
    extra_specs = [ANY] * len(extra)
    if got is not None:
        extra = [got] + extra
        extra_specs = [pl.BlockSpec(got.shape, lambda i, s: (0, 0), pipeline_mode=pl.Buffered(1))] + extra_specs
    spec = pltpu.PrefetchScalarGridSpec(
        num_scalar_prefetch=1,
        grid=(8,),
        in_specs=[
            pl.BlockSpec((1, rows, PAIR), lambda i, s: (s[PAIR_IDS + last(i, s[ALL_PAIRS])], j, 0)),
            pl.BlockSpec((1, PAIR, width), lambda i, s: (s[PAIR_IDS + last(i, s[ALL_PAIRS])], 0, 0)),
            pl.BlockSpec((1, 2, PAIR), lambda i, s: (s[PAIR_IDS + last(i, s[ALL_PAIRS])], 0, 0)),
            pl.BlockSpec((1, 1, PAIR), lambda i, s: (s[PAIR_IDS + last(i, s[ALL_PAIRS])], 0, 0)),
        ] + extra_specs,
        out_specs=[pl.BlockSpec((rows, width), lambda i, s: (0, 0)), ANY],
        scratch_shapes=[pltpu.SemaphoreType.DMA((2,))],
    )
    return pl.pallas_call(
        functools.partial(de_kernel, offset, rows, got_offset if got is not None else None),
        grid_spec=spec,
        out_shape=[jax.ShapeDtypeStruct((rows, width), jnp.float32), jax.ShapeDtypeStruct((2 * total, width), jnp.float32)],
        input_output_aliases={} if de is None else {4 + len(extra): 1},
        compiler_params=params(DE_VMEM),
        cost_estimate=cost(5, rows, width),
    )(idx, l, zc, tok, lab, *extra)


def call_place(idx, got, de, got_offset):
    spec = pltpu.PrefetchScalarGridSpec(
        num_scalar_prefetch=1,
        grid=(1,),
        in_specs=[pl.BlockSpec(got.shape, lambda i, s: (0, 0), pipeline_mode=pl.Buffered(1)), ANY],
        out_specs=ANY,
        scratch_shapes=[pltpu.SemaphoreType.DMA],
    )
    return pl.pallas_call(
        functools.partial(place_kernel, got_offset),
        grid_spec=spec,
        out_shape=jax.ShapeDtypeStruct(de.shape, de.dtype),
        input_output_aliases={2: 0},
        compiler_params=params(DE_VMEM),
        name="place",
    )(idx, got, de)


def order_blocks(active):
    n = active.shape[1]
    act = active.astype(jnp.int32)
    ids = jnp.arange(n, dtype=jnp.int32)
    before = (ids[None, :] < ids[:, None]).astype(jnp.int32)
    ahead = jnp.sum(before[None] * act[:, None, :], axis=2)
    count = jnp.sum(act, axis=1, keepdims=True)
    place = jnp.where(act > 0, ahead, count + ids - ahead)
    hit = place[:, None, :] == ids[None, :, None]
    return jnp.sum(jnp.where(hit, ids, 0), axis=2), count[:, 0], hit


def solution(mesh):
    n_tp, n_dp = mesh.shape['tp'], mesh.shape['dp']

    def flip(x, axis, bits):
        n = n_tp if axis == 'tp' else n_dp
        return lax.ppermute(x, axis, [(k, k ^ bits) for k in range(n)])

    def flip_both(x, tp_bits, dp_bits):
        return lax.ppermute(x, ('tp', 'dp'), [(k, ((k // n_dp) ^ tp_bits) * n_dp + ((k % n_dp) ^ dp_bits)) for k in range(n_tp * n_dp)])

    def from_group(x):
        return jnp.stack([x] + [flip_both(x, t, d) for t in range(4) for d in range(2) if (t, d) != (0, 0)])

    def pick(x, index):
        return lax.dynamic_index_in_dim(x, index, 0, keepdims=False)

    def local_step(hidden, ln_gamma, ln_beta, embed_shard, labels, loss_mask):
        tp, dp = lax.axis_index('tp'), lax.axis_index('dp')
        core = dp & 1
        y, z = tp & 1, tp >> 1
        seq, width = hidden.shape[1:]
        quarters, piece = seq // BLOCK, BLOCK // 2
        rows = embed_shard.shape[0] // 2
        row_start = tp * (2 * rows) + core * rows

        def by_core(mine, other):
            return jnp.stack([jnp.where(core == 0, mine, other), jnp.where(core == 0, other, mine)])

        marked = jnp.where(loss_mask[0] > 0, labels[0], -1)
        far_marks = [flip(marked, 'dp', 2), flip(marked, 'dp', 3)]
        mate_marks = flip(marked, 'dp', 1)

        x_float = hidden[0].astype(jnp.float32)
        centered = x_float - jnp.mean(x_float, axis=-1, keepdims=True)
        inv_std = lax.rsqrt(jnp.mean(centered * centered, axis=-1, keepdims=True) + LAYER_EPS)
        x_hat = (centered * inv_std).reshape(quarters, BLOCK, width)

        mate = flip(x_hat, 'dp', 1)
        own_quarter, far_quarter = lax.optimization_barrier((pick(x_hat, tp), pick(x_hat, tp ^ 3)))
        far0, far3 = flip(own_quarter, 'dp', 2), flip(far_quarter, 'dp', 2)

        marks = jnp.concatenate([by_core(marked, mate_marks), by_core(*far_marks)]).reshape(2, 8, BLOCK)
        token_count = jnp.sum((marks >= 0).astype(jnp.float32))
        order, active, hit = order_blocks(jnp.any(marks >= 0, axis=2))
        lab = jnp.sum(jnp.where(hit[..., None], marks[:, None], 0), axis=2).reshape(8, 1, PAIR)
        pairs = (active + 1) // 2
        pair_ids = jnp.arange(8, dtype=jnp.int32)
        pair_idx = jnp.where(pair_ids < pairs[0], pair_ids, jnp.minimum(4 + pair_ids - pairs[0], 7))
        zero = jnp.zeros((), jnp.int32)
        scalars = jnp.stack([core, pairs[0], pairs[1], pairs[0] + pairs[1], row_start, zero, zero, zero])
        idx = jnp.concatenate([scalars, order[0], order[0] ^ (core * 4), order[1] ^ (core * 4 + tp), pair_idx])

        logits, z_pairs, near_stats = call_logits(idx, embed_shard, ln_gamma, ln_beta, [x_hat, mate], None, rows)

        def combine(every, labels_here):
            top = jnp.max(every[:, :, 0], axis=0)
            total = jnp.sum(every[:, :, 1] * jnp.exp(every[:, :, 0] - top), axis=0)
            live = labels_here[:, 0] >= 0
            lse = jnp.where(live, top + jnp.log(total), BIG)
            return jnp.stack([lse, jnp.where(live, 1.0 / token_count, 0.0)], axis=1), lse, live

        near_tok, near_lse, near_live = combine(from_group(near_stats), lab[:4])
        mate0, mate3 = flip(far0, 'dp', 1), flip(far3, 'dp', 1)
        far1, far2 = flip(far0, 'tp', 1), flip(far0, 'tp', 2)
        dz_own, dz_mate, target, logits = call_dz(idx, embed_shard, logits, near_tok, lab[:4])

        mate1, mate2 = flip(far1, 'dp', 1), flip(far2, 'dp', 1)
        part = dz_own + flip(dz_mate, 'dp', 1)
        grid_part = part.reshape(2, 2, BLOCK, width)
        a_part, b_part = grid_part[:, :, :piece], grid_part[:, :, piece:]
        a_got = flip(lax.dynamic_index_in_dim(a_part, 1 - y, 1, keepdims=False), 'tp', 1)
        b_got = flip(pick(b_part, 1 - z), 'tp', 2)
        a_keep = lax.dynamic_index_in_dim(a_part, y, 1, keepdims=False) + a_got
        b_keep = pick(b_part, z) + b_got

        pieces = [far0, far1, far2, far3, mate0, mate1, mate2, mate3]
        logits, z_pairs, far_stats = call_logits(idx, embed_shard, ln_gamma, ln_beta, pieces, (logits, z_pairs), rows)
        far_tok, _, _ = combine(from_group(far_stats), lab[4:])
        a_grad = flip(pick(a_keep, 1 - z), 'tp', 2)
        b_grad = flip(pick(b_keep, 1 - y), 'tp', 1)
        grad = jnp.concatenate([pick(a_keep, z) + a_grad, pick(b_keep, y) + b_grad])
        tok = jnp.concatenate([near_tok, far_tok])

        hat = own_quarter
        scaled = grad * ln_gamma
        inner = scaled - jnp.mean(scaled, axis=-1, keepdims=True) - hat * jnp.mean(scaled * hat, axis=-1, keepdims=True)
        a0, b0 = inner[:piece], inner[piece:]
        a1, b2 = flip(a0, 'tp', 1), flip(b0, 'tp', 2)
        a2, a3 = flip(a0, 'tp', 2), flip(a1, 'tp', 2)
        b1, b3 = flip(b0, 'tp', 1), flip(b2, 'tp', 1)
        gathered = jnp.stack([jnp.concatenate(v) for v in ((a0, b0), (a1, b1), (a2, b2), (a3, b3))])
        gathered = jnp.stack([pick(gathered, tp ^ q) for q in range(quarters)]).reshape(seq, width)
        d_hidden = (gathered * inv_std).astype(jnp.bfloat16)[None]

        lead = ((tp == 0) & (core == 0)).astype(jnp.float32)
        loss = jnp.sum(jnp.where(near_live, lead * near_lse - target[:, 0], 0.0)) / token_count
        sums = jnp.concatenate([jnp.sum(grad * hat, axis=0), jnp.sum(grad, axis=0), jnp.broadcast_to(loss, (512,))]).reshape(4, 512)
        for bits in (1, 2):
            got_sums = flip(sums, 'dp', bits)
            sums = sums + got_sums
        got_sums = [flip(sums, 'tp', k) for k in (1, 2, 3)]
        sums = (sums + got_sums[0] + (got_sums[1] + got_sums[2])).reshape(-1)

        chunks = [(k * (rows // 6), rows // 6) for k in range(6)]
        d_embed, got = None, []
        for n, (offset, size) in enumerate(chunks):
            arrived = got[n - 2] if n >= 2 else None
            d_chunk, d_embed = call_de(idx, logits, z_pairs, tok, lab, d_embed, offset, size, arrived, chunks[n - 2][0] if n >= 2 else None)
            got.append(flip(d_chunk, 'dp', 1))
        for n in (4, 5):
            d_embed = call_place(idx, got[n], d_embed, chunks[n][0])

        return sums[2 * width], d_hidden, d_embed, sums[:width], sums[width:2 * width]


    return jax.shard_map(local_step, mesh=mesh, in_specs=(P('dp', None, None), P(None), P(None), P('tp', None), P('dp', None), P('dp', None)), out_specs=(P(), P('dp', None, None), P('tp', None), P(None), P(None)), check_vma=False)
```

```python
import functools

import jax
import jax.numpy as jnp
from jax import lax
from jax.experimental import pallas as pl
from jax.experimental.pallas import tpu as pltpu
from jax.sharding import PartitionSpec as P


LAYER_EPS = 1e-5
BLOCK = 256
PAIR = 2 * BLOCK
BIG = 1e30
VMEM_LIMIT = 62 * 1024 * 1024
DE_VMEM = 16 * 1024 * 1024


CORE, NEAR_PAIRS, FAR_PAIRS, ALL_PAIRS, ROW_START = 0, 1, 2, 3, 4
NEAR_ORDER, NEAR_PIECES, FAR_PIECES, PAIR_IDS = 8, 16, 24, 32


def chunk_list(total, size):
    return [(start, min(size, total - start)) for start in range(0, total, size)]


def last(i, count):
    return jnp.minimum(i, count - 1)


def logits_kernel(count, order, n_pieces, idx_ref, e_ref, gamma_ref, beta_ref, *rest):
    pieces = rest[:n_pieces]
    l_ref, zc_ref, st_ref, x_ref, sem = rest[-5:]
    i = pl.program_id(0)

    def copies(block, slot, h):
        target = x_ref.at[slot, pl.ds(h * BLOCK, BLOCK), :]
        if len(pieces[0].shape) == 3:
            return [(block >> 2 == k, pltpu.make_async_copy(ref.at[block & 3], target, sem.at[slot, h])) for k, ref in enumerate(pieces)]
        return [(block == k, pltpu.make_async_copy(ref, target, sem.at[slot, h])) for k, ref in enumerate(pieces)]

    def fetch(pair):
        for h in range(2):
            for chosen, copy in copies(idx_ref[order + 2 * pair + h], pair % 2, h):
                pl.when(chosen)(copy.start)

    pl.when(i == 0)(lambda: fetch(0))
    pl.when(i + 1 < idx_ref[count])(lambda: fetch(i + 1))

    @pl.when(i < idx_ref[count])
    def _():
        for h in range(2):
            copies(0, i % 2, h)[0][1].wait()
        zc_ref[0] = (x_ref[i % 2] * gamma_ref[...] + beta_ref[...]).astype(jnp.bfloat16)
        logits_step(e_ref, l_ref, zc_ref, st_ref)


def logits_step(e_ref, l_ref, zc_ref, st_ref):
    rows = e_ref.shape[0]
    size = 528

    top = jnp.full((1, PAIR), -BIG, jnp.float32)
    total = jnp.zeros((1, PAIR), jnp.float32)

    def add(start, n, old_top, top, total):
        return total * jnp.exp(old_top - top) + jnp.sum(jnp.exp(l_ref[0, start:start + n, :] - top), axis=0, keepdims=True)

    waiting = None
    for start, n in chunk_list(rows, size):
        tile = lax.dot_general(e_ref[start:start + n, :], zc_ref[0], (((1,), (1,)), ((), ())), preferred_element_type=jnp.float32)
        l_ref[0, start:start + n, :] = tile
        new_top = jnp.maximum(top, jnp.max(tile, axis=0, keepdims=True))
        if waiting is not None:
            total = add(*waiting, total)
        waiting = (start, n, top, new_top)
        top = new_top
    total = add(*waiting, total)
    st_ref[0, 0:1, :] = top
    st_ref[0, 1:2, :] = total


def grad_tile(tile, lse, weight, is_target):
    probs = jnp.exp(tile - lse)
    return (jnp.where(is_target, probs - 1.0, probs) * weight).astype(jnp.bfloat16)


def dz_kernel(idx_ref, e_ref, l_ref, tok_ref, lab_ref, own_ref, mate_ref, tl_ref, l_out_ref, acc_ref, out_ref, et_ref, sem):
    i = pl.program_id(0)
    rows = e_ref.shape[0]
    size = 512
    full = rows // size

    @pl.when(i == 0)
    def _():
        def turn(k, carry):
            start = pl.multiple_of(k * size, size)
            et_ref[:, pl.ds(start, size)] = e_ref[pl.ds(start, size), :].T
            return carry

        lax.fori_loop(0, full, turn, 0)
        if rows > full * size:
            et_ref[:, full * size:] = e_ref[full * size:, :].T

    live = i < idx_ref[NEAR_PAIRS]
    pl.when(live)(lambda: dz_step(idx_ref, et_ref, l_ref, tok_ref, lab_ref, tl_ref, acc_ref))

    @pl.when(live)
    def _():
        out_ref[...] = acc_ref[...].T

    @pl.when(jnp.logical_not(live))
    def _():
        out_ref[...] = jnp.zeros_like(out_ref)

    for h in range(2):
        block = idx_ref[NEAR_ORDER + 2 * i + h]
        for seq in range(2):
            target = own_ref if seq == 0 else mate_ref
            copy = pltpu.make_async_copy(out_ref.at[pl.ds(h * BLOCK, BLOCK), :], target.at[block % 4], sem.at[h])
            pl.when(block // 4 == (idx_ref[CORE] + seq) % 2)(copy.start)
    for h in range(2):
        pltpu.make_async_copy(out_ref.at[pl.ds(h * BLOCK, BLOCK), :], own_ref.at[0], sem.at[h]).wait()


def dz_step(idx_ref, et_ref, l_ref, tok_ref, lab_ref, tl_ref, acc_ref):
    lse = tok_ref[0, 0:1, :]
    weight = tok_ref[0, 1:2, :]
    label = lab_ref[0] - idx_ref[ROW_START]
    target = jnp.zeros((1, PAIR), jnp.float32)
    for start, n in chunk_list(et_ref.shape[1], 1024):
        tile = l_ref[0, start:start + n, :]
        is_target = lax.broadcasted_iota(jnp.int32, (n, PAIR), 0) == label - start
        grad = grad_tile(tile, lse, weight, is_target)
        target = target + jnp.sum(jnp.where(is_target, tile, 0.0), axis=0, keepdims=True)
        part = jnp.dot(et_ref[:, start:start + n], grad, preferred_element_type=jnp.float32)
        if start == 0:
            acc_ref[...] = part
        else:
            acc_ref[...] += part
    tl_ref[0] = target


def de_kernel(offset, rows, got_offset, idx_ref, l_ref, z_ref, tok_ref, lab_ref, *rest):
    got_ref = None if got_offset is None else rest[0]
    part_ref, out_ref, buf_ref, sem = rest[-4:]
    core = idx_ref[CORE]
    half = out_ref.shape[0] // 2
    count = idx_ref[ALL_PAIRS]

    def rows_at(side, start, n):
        return out_ref.at[pl.ds(pl.multiple_of(side * half + start, 8), n), :]

    def fetch(i):
        return pltpu.make_async_copy(l_ref.at[idx_ref[PAIR_IDS + i], pl.ds(offset, rows), :], buf_ref.at[i % 2], sem.at[i % 2])

    fetch(0).start()
    got = None
    if got_ref is not None:
        got = pltpu.make_async_copy(got_ref, rows_at(1 - core, got_offset, got_ref.shape[0]), sem.at[2])
        got.start()
    part_ref[...] = jnp.zeros_like(part_ref)

    def step(i, carry):
        fetch(i).wait()
        pl.when(i + 1 < count)(lambda: fetch(i + 1).start())
        pair = idx_ref[PAIR_IDS + i]
        lse = tok_ref[pair, 0:1, :]
        weight = tok_ref[pair, 1:2, :]
        label = lab_ref[pair] - idx_ref[ROW_START] - offset
        for start, n in chunk_list(rows, 528):
            is_target = lax.broadcasted_iota(jnp.int32, (n, PAIR), 0) == label - start
            grad = grad_tile(buf_ref[i % 2, start:start + n, :], lse, weight, is_target)
            part_ref[start:start + n, :] += jnp.dot(grad, z_ref[pair], preferred_element_type=jnp.float32)
        return carry

    lax.fori_loop(0, count, step, 0)
    own = pltpu.make_async_copy(part_ref, rows_at(core, offset, rows), sem.at[3])
    own.start()
    own.wait()
    if got is not None:
        got.wait()


def place_kernel(got_offset, idx_ref, got_ref, de_ref, out_ref, sem):
    half = out_ref.shape[0] // 2
    start = pl.multiple_of((1 - idx_ref[CORE]) * half + got_offset, 8)
    copy = pltpu.make_async_copy(got_ref, out_ref.at[pl.ds(start, got_ref.shape[0]), :], sem)
    copy.start()
    copy.wait()


def lse_kernel(st_ref, lab_ref, scale_ref, tok_ref, got_ref, send_sem, recv_sem):
    tp, dp = lax.axis_index('tp'), lax.axis_index('dp')
    peers = []
    for k in range(1, 8):
        z, y, c = k // 4, k // 2 % 2, k % 2
        peer_tp = (tp // 2 + z) % 2 * 2 + (tp % 2 + y) % 2
        peers.append({'tp': peer_tp, 'dp': dp // 2 * 2 + (dp % 2 + c) % 2})
    barrier = pltpu.get_barrier_semaphore()
    for peer in peers:
        pl.semaphore_signal(barrier, inc=1, device_id=peer, device_id_type=pl.DeviceIdType.MESH)
    pl.semaphore_wait(barrier, 7)
    copies = [
        pltpu.make_async_remote_copy(st_ref, got_ref.at[k], send_sem.at[k], recv_sem.at[k], device_id=peer, device_id_type=pl.DeviceIdType.MESH)
        for k, peer in enumerate(peers)
    ]
    for copy in copies:
        copy.start()
    for copy in copies:
        copy.wait()
    top = st_ref[:, 0, :]
    for k in range(7):
        top = jnp.maximum(top, got_ref[k, :, 0, :])
    total = st_ref[:, 1, :] * jnp.exp(st_ref[:, 0, :] - top)
    for k in range(7):
        total = total + got_ref[k, :, 1, :] * jnp.exp(got_ref[k, :, 0, :] - top)
    live = lab_ref[:, 0, :] >= 0
    tok_ref[:, 0, :] = jnp.where(live, top + jnp.log(total), BIG)
    tok_ref[:, 1, :] = jnp.where(live, scale_ref[...], 0.0)


def call_lse(stats, lab, scale, collective_id):
    vmem = pl.BlockSpec(memory_space=pltpu.VMEM)
    return pl.pallas_call(
        lse_kernel,
        in_specs=[vmem, vmem, vmem],
        out_specs=vmem,
        out_shape=jax.ShapeDtypeStruct(stats.shape, jnp.float32),
        scratch_shapes=[pltpu.VMEM((7,) + stats.shape, jnp.float32), pltpu.SemaphoreType.DMA((7,)), pltpu.SemaphoreType.DMA((7,))],
        compiler_params=pltpu.CompilerParams(collective_id=collective_id, has_side_effects=True, vmem_limit_bytes=4 * 1024 * 1024),
        cost_estimate=pl.CostEstimate(flops=10_000_000, bytes_accessed=1_000_000, transcendentals=20_000),
    )(stats, lab, scale)


def norm_kernel(pick_ref, h_ref, hat_ref, inv_ref, own_ref, far_ref):
    i = pl.program_id(0)
    x = h_ref[0].astype(jnp.float32)
    centered = x - jnp.mean(x, axis=-1, keepdims=True)
    inv = lax.rsqrt(jnp.mean(centered * centered, axis=-1, keepdims=True) + LAYER_EPS)
    hat = centered * inv
    hat_ref[0] = hat

    @pl.when(i == pick_ref[0])
    def _():
        own_ref[...] = hat
        inv_ref[...] = jnp.broadcast_to(inv, inv_ref.shape)

    @pl.when(i == pick_ref[1])
    def _():
        far_ref[...] = hat


def call_norm(picks, hidden):
    n, block, width = hidden.shape
    quarter = pl.BlockSpec((block, width), lambda i, s: (0, 0))
    each = pl.BlockSpec((1, block, width), lambda i, s: (i, 0, 0))
    one = jax.ShapeDtypeStruct((block, width), jnp.float32)
    return pl.pallas_call(
        norm_kernel,
        grid_spec=pltpu.PrefetchScalarGridSpec(
            num_scalar_prefetch=1, grid=(n,), in_specs=[each],
            out_specs=[each, pl.BlockSpec((block, 128), lambda i, s: (0, 0)), quarter, quarter],
        ),
        out_shape=[jax.ShapeDtypeStruct(hidden.shape, jnp.float32), jax.ShapeDtypeStruct((block, 128), jnp.float32), one, one],
        compiler_params=params(DE_VMEM),
        cost_estimate=pl.CostEstimate(flops=10_000_000, bytes_accessed=8_000_000, transcendentals=1024),
        name="norm",
    )(picks, hidden)


def norm_bwd_kernel(a_ref, b_ref, a_got_ref, b_got_ref, hat_ref, inv_ref, gamma_ref, loss_ref, a_out, b_out, sum_out):
    piece = a_ref.shape[0]
    grad = jnp.concatenate([a_ref[...] + a_got_ref[...], b_ref[...] + b_got_ref[...]])
    hat = hat_ref[...]
    scaled = grad * gamma_ref[...]
    inner = scaled - jnp.mean(scaled, axis=-1, keepdims=True) - hat * jnp.mean(scaled * hat, axis=-1, keepdims=True)
    inner = inner * inv_ref[:, 0:1]
    a_out[...] = inner[:piece]
    b_out[...] = inner[piece:]
    sum_out[...] = jnp.zeros_like(sum_out)
    sum_out[0:1, :] = jnp.sum(grad * hat, axis=0, keepdims=True)
    sum_out[1:2, :] = jnp.sum(grad, axis=0, keepdims=True)
    sum_out[2:3, 0:128] = loss_ref[...]


def call_norm_bwd(*args):
    piece, width = args[0].shape
    vmem = pl.BlockSpec(memory_space=pltpu.VMEM)
    half = jax.ShapeDtypeStruct((piece, width), jnp.float32)
    return pl.pallas_call(
        norm_bwd_kernel,
        in_specs=[vmem] * len(args),
        out_specs=[vmem] * 3,
        out_shape=[half, half, jax.ShapeDtypeStruct((8, width), jnp.float32)],
        compiler_params=pltpu.CompilerParams(vmem_limit_bytes=DE_VMEM),
        cost_estimate=pl.CostEstimate(flops=10_000_000, bytes_accessed=4_000_000, transcendentals=0),
        name="norm_bwd",
    )(*args)


def round_kernel(pick_ref, *refs):
    out_ref = refs[-1]
    piece = refs[0].shape[0]
    for p in range(4):
        start = pl.multiple_of(pick_ref[2 + p] * (2 * piece), 2 * piece)
        out_ref[0, pl.ds(start, piece), :] = refs[2 * p][...].astype(jnp.bfloat16)
        out_ref[0, pl.ds(start + piece, piece), :] = refs[2 * p + 1][...].astype(jnp.bfloat16)


def call_round(picks, pieces):
    piece, width = pieces[0].shape
    spec = pl.BlockSpec((piece, width), lambda i, s: (0, 0), pipeline_mode=pl.Buffered(1))
    out = (1, len(pieces) * piece, width)
    return pl.pallas_call(
        round_kernel,
        grid_spec=pltpu.PrefetchScalarGridSpec(
            num_scalar_prefetch=1, grid=(1,), in_specs=[spec] * len(pieces), out_specs=pl.BlockSpec(out, lambda i, s: (0, 0, 0)),
        ),
        out_shape=jax.ShapeDtypeStruct(out, jnp.bfloat16),
        compiler_params=params(DE_VMEM),
        cost_estimate=pl.CostEstimate(flops=1_000_000, bytes_accessed=5_000_000, transcendentals=0),
        name="round",
    )(picks, *pieces)


def params(limit=VMEM_LIMIT):
    return pltpu.CompilerParams(vmem_limit_bytes=limit, dimension_semantics=("arbitrary",))


def cost(pairs, rows, width):
    n = PAIR * pairs * rows
    return pl.CostEstimate(flops=2 * n * width, bytes_accessed=4 * n, transcendentals=n)


ANY = pl.BlockSpec(memory_space=pl.ANY)


def call_logits(idx, e, gamma, beta, pieces, previous, rows):
    pairs = 8
    base, count, order = (0, NEAR_PAIRS, NEAR_PIECES) if previous is None else (4, FAR_PAIRS, FAR_PIECES)
    width = e.shape[1]
    extra = [] if previous is None else list(previous)
    spec = pltpu.PrefetchScalarGridSpec(
        num_scalar_prefetch=1,
        grid=(4,),
        in_specs=[pl.BlockSpec((rows, width), lambda i, s: (s[CORE], 0), pipeline_mode=pl.Buffered(1))]
        + [pl.BlockSpec((1, width), lambda i, s: (0, 0))] * 2 + [ANY] * (len(pieces) + len(extra)),
        out_specs=[
            pl.BlockSpec((1, rows, PAIR), lambda i, s: (base + last(i, s[count]), 0, 0)),
            pl.BlockSpec((1, PAIR, width), lambda i, s: (base + last(i, s[count]), 0, 0)),
            pl.BlockSpec((1, 2, PAIR), lambda i, s: (last(i, s[count]), 0, 0)),
        ],
        scratch_shapes=[pltpu.VMEM((2, PAIR, width), jnp.float32), pltpu.SemaphoreType.DMA((2, 2))],
    )
    first = 4 + len(pieces)
    return pl.pallas_call(
        functools.partial(logits_kernel, count, order, len(pieces)),
        grid_spec=spec,
        out_shape=[
            jax.ShapeDtypeStruct((pairs, rows, PAIR), jnp.float32),
            jax.ShapeDtypeStruct((pairs, PAIR, width), jnp.bfloat16),
            jax.ShapeDtypeStruct((4, 2, PAIR), jnp.float32),
        ],
        input_output_aliases={} if previous is None else {first: 0, first + 1: 1},
        compiler_params=params(),
        cost_estimate=cost(3, rows, width),
        name="logits_near" if previous is None else "logits_far",
    )(idx, e, gamma[None], beta[None], *pieces, *extra)


def call_dz(idx, e, l, tok, lab):
    width, rows = e.shape[1], l.shape[1]
    pick_row = lambda i, s: (last(i, s[NEAR_PAIRS]), 0, 0)
    spec = pltpu.PrefetchScalarGridSpec(
        num_scalar_prefetch=1,
        grid=(4,),
        in_specs=[
            pl.BlockSpec((rows, width), lambda i, s: (s[CORE], 0), pipeline_mode=pl.Buffered(1)),
            pl.BlockSpec((1, rows, PAIR), pick_row),
            pl.BlockSpec((1, 2, PAIR), pick_row),
            pl.BlockSpec((1, 1, PAIR), pick_row),
        ],
        out_specs=[ANY, ANY, pl.BlockSpec((1, 1, PAIR), pick_row), ANY],
        scratch_shapes=[
            pltpu.VMEM((width, PAIR), jnp.float32),
            pltpu.VMEM((PAIR, width), jnp.float32),
            pltpu.VMEM((width, rows), jnp.bfloat16),
            pltpu.SemaphoreType.DMA((2,)),
        ],
    )
    half = jax.ShapeDtypeStruct((4, BLOCK, width), jnp.float32)
    return pl.pallas_call(
        dz_kernel,
        grid_spec=spec,
        out_shape=[half, half, jax.ShapeDtypeStruct((4, 1, PAIR), jnp.float32), jax.ShapeDtypeStruct(l.shape, l.dtype)],
        input_output_aliases={2: 3},
        compiler_params=params(),
        cost_estimate=cost(3, rows, width),
        name="dz_part",
    )(idx, e, l, tok, lab)


def call_de(idx, l, zc, tok, lab, de, offset, rows, got, got_offset):
    total, width = l.shape[1], zc.shape[2]

    def whole(x):
        return pl.BlockSpec(x.shape, lambda i, s: (0,) * x.ndim, pipeline_mode=pl.Buffered(1))

    extra = [] if de is None else [de]
    extra_specs = [ANY] * len(extra)
    if got is not None:
        extra = [got] + extra
        extra_specs = [whole(got)] + extra_specs
    spec = pltpu.PrefetchScalarGridSpec(
        num_scalar_prefetch=1,
        grid=(1,),
        in_specs=[ANY, whole(zc), whole(tok), whole(lab)] + extra_specs,
        out_specs=[pl.BlockSpec((rows, width), lambda i, s: (0, 0), pipeline_mode=pl.Buffered(1)), ANY],
        scratch_shapes=[pltpu.VMEM((2, rows, PAIR), jnp.float32), pltpu.SemaphoreType.DMA((4,))],
    )
    return pl.pallas_call(
        functools.partial(de_kernel, offset, rows, got_offset if got is not None else None),
        grid_spec=spec,
        out_shape=[jax.ShapeDtypeStruct((rows, width), jnp.float32), jax.ShapeDtypeStruct((2 * total, width), jnp.float32)],
        input_output_aliases={} if de is None else {4 + len(extra): 1},
        compiler_params=params(DE_VMEM),
        cost_estimate=cost(5, rows, width),
    )(idx, l, zc, tok, lab, *extra)


def call_place(idx, got, de, got_offset):
    spec = pltpu.PrefetchScalarGridSpec(
        num_scalar_prefetch=1,
        grid=(1,),
        in_specs=[pl.BlockSpec(got.shape, lambda i, s: (0, 0), pipeline_mode=pl.Buffered(1)), ANY],
        out_specs=ANY,
        scratch_shapes=[pltpu.SemaphoreType.DMA],
    )
    return pl.pallas_call(
        functools.partial(place_kernel, got_offset),
        grid_spec=spec,
        out_shape=jax.ShapeDtypeStruct(de.shape, de.dtype),
        input_output_aliases={2: 0},
        compiler_params=params(DE_VMEM),
        name="place",
    )(idx, got, de)


def idx_of(scalars, order, pair_idx, core, tp):
    return jnp.concatenate([scalars, order[0], order[0] ^ (core * 4), order[1] ^ (core * 4 + tp), pair_idx])


def order_blocks(active):
    n = active.shape[1]
    act = active.astype(jnp.int32)
    ids = jnp.arange(n, dtype=jnp.int32)
    before = (ids[None, :] < ids[:, None]).astype(jnp.int32)
    ahead = jnp.sum(before[None] * act[:, None, :], axis=2)
    count = jnp.sum(act, axis=1, keepdims=True)
    place = jnp.where(act > 0, ahead, count + ids - ahead)
    hit = place[:, None, :] == ids[None, :, None]
    return jnp.sum(jnp.where(hit, ids, 0), axis=2), count[:, 0], hit


def solution(mesh):
    n_tp, n_dp = mesh.shape['tp'], mesh.shape['dp']

    def flip(x, axis, bits):
        n = n_tp if axis == 'tp' else n_dp
        return lax.ppermute(x, axis, [(k, k ^ bits) for k in range(n)])

    def pick(x, index):
        return lax.dynamic_index_in_dim(x, index, 0, keepdims=False)

    def local_step(hidden, ln_gamma, ln_beta, embed_shard, labels, loss_mask):
        tp, dp = lax.axis_index('tp'), lax.axis_index('dp')
        core = dp & 1
        y, z = (tp & 1).astype(jnp.uint32), (tp >> 1).astype(jnp.uint32)
        not_y, not_z = 1 - y, 1 - z
        seq, width = hidden.shape[1:]
        quarters, piece = seq // BLOCK, BLOCK // 2
        rows = embed_shard.shape[0] // 2
        row_start = tp * (2 * rows) + core * rows

        def by_core(mine, other):
            return jnp.stack([jnp.where(core == 0, mine, other), jnp.where(core == 0, other, mine)])

        marked = jnp.where(loss_mask[0] > 0, labels[0], -1)
        far_marks = [flip(marked, 'dp', 2), flip(marked, 'dp', 3)]
        mate_marks = flip(marked, 'dp', 1)

        picks = jnp.stack([tp, tp ^ 3] + [tp ^ p for p in range(4)])
        x_hat, inv_std, own_quarter, far_quarter = call_norm(picks, hidden.reshape(quarters, BLOCK, width))
        mate = flip(x_hat, 'dp', 1)
        far0, far3 = flip(own_quarter, 'dp', 2), flip(far_quarter, 'dp', 2)

        marks = jnp.concatenate([by_core(marked, mate_marks), by_core(*far_marks)]).reshape(2, 8, BLOCK)
        token_count = jnp.sum((marks >= 0).astype(jnp.float32))
        order, active, hit = order_blocks(jnp.any(marks >= 0, axis=2))
        lab = jnp.sum(jnp.where(hit[..., None], marks[:, None], 0), axis=2).reshape(8, 1, PAIR)
        pairs = (active + 1) // 2
        pair_ids = jnp.arange(8, dtype=jnp.int32)
        pair_idx = jnp.where(pair_ids < pairs[0], pair_ids, jnp.minimum(4 + pair_ids - pairs[0], 7))
        zero = jnp.zeros((), jnp.int32)
        scalars = jnp.stack([core, pairs[0], pairs[1], pairs[0] + pairs[1], row_start, zero, zero, zero])
        idx, y, z, not_y, not_z = lax.optimization_barrier((idx_of(scalars, order, pair_idx, core, tp), y, z, not_y, not_z))

        logits, z_pairs, near_stats = call_logits(idx, embed_shard, ln_gamma, ln_beta, [x_hat, mate], None, rows)

        scale = jnp.broadcast_to(1.0 / token_count, (1, PAIR))
        near_tok = call_lse(near_stats, lab[:4], scale, 0)
        mate0, mate3 = flip(far0, 'dp', 1), flip(far3, 'dp', 1)
        far1, far2 = flip(far0, 'tp', 1), flip(far0, 'tp', 2)
        dz_own, dz_mate, target, logits = call_dz(idx, embed_shard, logits, near_tok, lab[:4])

        mate1, mate2 = flip(far1, 'dp', 1), flip(far2, 'dp', 1)
        lead = ((tp == 0) & (core == 0)).astype(jnp.float32)
        loss = jnp.sum(jnp.where(lab[:4, 0] >= 0, lead * near_tok[:, 0] - target[:, 0], 0.0)) / token_count
        loss, idx = lax.optimization_barrier((jnp.broadcast_to(loss, (1, 128)), idx))
        pieces = [far0, far1, far2, far3, mate0, mate1, mate2, mate3]
        logits, z_pairs, far_stats = call_logits(idx, embed_shard, ln_gamma, ln_beta, pieces, (logits, z_pairs), rows)
        far_tok = call_lse(far_stats, lab[4:], scale, 1)
        dz_got = flip(dz_mate, 'dp', 1)

        def part(column, half_z, half_y):
            def cut(x):
                x = x.reshape(2, 2, 2, piece, width)[:, :, column]
                return pick(x, half_z) if half_y is None else lax.dynamic_index_in_dim(x, half_y, 1, keepdims=False)

            return cut(dz_own) + cut(dz_got)

        a_got = flip(part(0, None, not_y), 'tp', 1)
        b_got = flip(part(1, not_z, None), 'tp', 2)
        a_keep = part(0, None, y) + a_got
        b_keep = part(1, z, None) + b_got
        a_grad = flip(pick(a_keep, not_z), 'tp', 2)
        b_grad = flip(pick(b_keep, not_y), 'tp', 1)
        tok = jnp.concatenate([near_tok, far_tok])

        a0, b0, sums = call_norm_bwd(pick(a_keep, z), pick(b_keep, y), a_grad, b_grad, own_quarter, inv_std, ln_gamma[None], loss)
        a1, b2 = flip(a0, 'tp', 1), flip(b0, 'tp', 2)
        a2, a3 = flip(a0, 'tp', 2), flip(a1, 'tp', 2)
        b1, b3 = flip(b0, 'tp', 1), flip(b2, 'tp', 1)
        d_hidden = call_round(picks, [a0, b0, a1, b1, a2, b2, a3, b3])

        for bits in (1, 2):
            got_sums = flip(sums, 'dp', bits)
            sums = sums + got_sums
        got_sums = [flip(sums, 'tp', k) for k in (1, 2, 3)]
        sums = sums + got_sums[0] + (got_sums[1] + got_sums[2])

        chunks = [(k * (rows // 6), rows // 6) for k in range(6)]
        d_embed, got = None, []
        for n, (offset, size) in enumerate(chunks):
            arrived = got[n - 2] if n >= 2 else None
            d_chunk, d_embed = call_de(idx, logits, z_pairs, tok, lab, d_embed, offset, size, arrived, chunks[n - 2][0] if n >= 2 else None)
            got.append(flip(d_chunk, 'dp', 1))
        for n in (4, 5):
            d_embed = call_place(idx, got[n], d_embed, chunks[n][0])

        return sums[2, 0], d_hidden, d_embed, sums[0], sums[1]


    return jax.shard_map(local_step, mesh=mesh, in_specs=(P('dp', None, None), P(None), P(None), P('tp', None), P('dp', None), P('dp', None)), out_specs=(P(), P('dp', None, None), P('tp', None), P(None), P(None)), check_vma=False)
```

```python
import functools

import jax
import jax.numpy as jnp
from jax import lax
from jax.experimental import pallas as pl
from jax.experimental.pallas import tpu as pltpu
from jax.sharding import PartitionSpec as P


LAYER_EPS = 1e-5
BLOCK = 256
PAIR = 2 * BLOCK
BIG = 1e30
VMEM_LIMIT = 62 * 1024 * 1024
DE_VMEM = 16 * 1024 * 1024
EARLY_OUT = True


CORE, NEAR_PAIRS, FAR_PAIRS, ALL_PAIRS, ROW_START = 0, 1, 2, 3, 4
NEAR_ORDER, NEAR_PIECES, FAR_PIECES, PAIR_IDS = 8, 16, 24, 32


def chunk_list(total, size):
    return [(start, min(size, total - start)) for start in range(0, total, size)]


def split_copy(source, target, sem, size):
    return [pltpu.make_async_copy(source.at[pl.ds(a, n), :], target.at[pl.ds(a, n), :], sem) for a, n in chunk_list(target.shape[0], size)]


def start(copies):
    for copy in copies:
        copy.start()


def last(i, count):
    return jnp.minimum(i, count - 1)


def logits_kernel(count, base, order, n_pieces, idx_ref, e_hbm, gamma_ref, beta_ref, *rest):
    pieces = rest[:n_pieces]
    l_hbm, zc_ref, st_ref, x_ref, e_ref, l_ref, sem, e_sem, l_sem = rest[-9:]
    i = pl.program_id(0)
    live = i < idx_ref[count]
    rows = e_ref.shape[0]
    slot = i % 2

    def copies(block, slot, h):
        target = x_ref.at[slot, pl.ds(h * BLOCK, BLOCK), :]
        if len(pieces[0].shape) == 3:
            return [(block >> 2 == k, pltpu.make_async_copy(ref.at[block & 3], target, sem.at[slot, h])) for k, ref in enumerate(pieces)]
        return [(block == k, pltpu.make_async_copy(ref, target, sem.at[slot, h])) for k, ref in enumerate(pieces)]

    def fetch(pair):
        for h in range(2):
            for chosen, copy in copies(idx_ref[order + 2 * pair + h], pair % 2, h):
                pl.when(chosen)(copy.start)

    def flush(k):
        pltpu.make_async_copy(l_ref.at[k], l_hbm.at[0], l_sem.at[k]).wait()

    @pl.when(i == 0)
    def _():
        fetch(0)
        table = e_hbm.at[pl.ds(pl.multiple_of(idx_ref[CORE] * rows, 16), rows), :]
        start(split_copy(table, e_ref, e_sem, 528))
        pltpu.make_async_copy(table, e_ref, e_sem).wait()

    pl.when(i + 1 < idx_ref[count])(lambda: fetch(i + 1))
    pl.when(live & (i >= 2))(lambda: flush(slot))

    @pl.when(live)
    def _():
        for h in range(2):
            copies(0, slot, h)[0][1].wait()
        zc_ref[0] = (x_ref[slot] * gamma_ref[...] + beta_ref[...]).astype(jnp.bfloat16)
        logits_step(e_ref, l_ref.at[slot], zc_ref, st_ref, split_copy(l_ref.at[slot], l_hbm.at[base + i], l_sem.at[slot], 528))

    @pl.when(i == idx_ref[count] - 1)
    def _():
        flush(slot)
        pl.when(i > 0)(lambda: flush(1 - slot))


def logits_step(e_ref, l_ref, zc_ref, st_ref, out):
    rows = e_ref.shape[0]
    size = 528
    top = jnp.full((1, PAIR), -BIG, jnp.float32)
    total = jnp.zeros((1, PAIR), jnp.float32)

    def add(start, n, old_top, top, total):
        return total * jnp.exp(old_top - top) + jnp.sum(jnp.exp(l_ref[start:start + n, :] - top), axis=0, keepdims=True)

    waiting = None
    for start, n in chunk_list(rows, size):
        tile = lax.dot_general(e_ref[start:start + n, :], zc_ref[0], (((1,), (1,)), ((), ())), preferred_element_type=jnp.float32)
        l_ref[start:start + n, :] = tile
        new_top = jnp.maximum(top, jnp.max(tile, axis=0, keepdims=True))
        if waiting is not None:
            total = add(*waiting, total)
            if EARLY_OUT:
                out[waiting[0] // size].start()
        waiting = (start, n, top, new_top)
        top = new_top
    total = add(*waiting, total)
    for copy in out[-1:] if EARLY_OUT else out:
        copy.start()
    st_ref[0, 0:1, :] = top
    st_ref[0, 1:2, :] = total


def grad_tile(tile, lse, weight, is_target):
    probs = jnp.exp(tile - lse)
    return (jnp.where(is_target, probs - 1.0, probs) * weight).astype(jnp.bfloat16)


def dz_kernel(idx_ref, e_hbm, l_hbm, tok_ref, lab_ref, own_ref, mate_ref, tl_ref, l_out_ref, acc_ref, out_ref, et_ref, e_ref, l_ref, sem, e_sem, l_sem):
    i = pl.program_id(0)
    rows = e_ref.shape[0]
    size = 512
    full = rows // size
    slot = i % 2

    def fetch(pair):
        start(split_copy(l_hbm.at[pair], l_ref.at[pair % 2], l_sem.at[pair % 2], size))

    @pl.when(i == 0)
    def _():
        table = e_hbm.at[pl.ds(pl.multiple_of(idx_ref[CORE] * rows, 16), rows), :]
        start(split_copy(table, e_ref, e_sem, size))
        fetch(0)
        pltpu.make_async_copy(table, e_ref, e_sem).wait()

        def turn(k, carry):
            at = pl.multiple_of(k * size, size)
            et_ref[:, pl.ds(at, size)] = e_ref[pl.ds(at, size), :].T
            return carry

        lax.fori_loop(0, full, turn, 0)
        if rows > full * size:
            et_ref[:, full * size:] = e_ref[full * size:, :].T

    live = i < idx_ref[NEAR_PAIRS]
    pl.when(i + 1 < idx_ref[NEAR_PAIRS])(lambda: fetch(i + 1))

    @pl.when(live)
    def _():
        pltpu.make_async_copy(l_hbm.at[0], l_ref.at[slot], l_sem.at[slot]).wait()
        dz_step(idx_ref, et_ref, l_ref.at[slot], tok_ref, lab_ref, tl_ref, acc_ref)

    @pl.when(live)
    def _():
        out_ref[...] = acc_ref[...].T

    @pl.when(jnp.logical_not(live))
    def _():
        out_ref[...] = jnp.zeros_like(out_ref)

    for h in range(2):
        block = idx_ref[NEAR_ORDER + 2 * i + h]
        for seq in range(2):
            target = own_ref if seq == 0 else mate_ref
            copy = pltpu.make_async_copy(out_ref.at[pl.ds(h * BLOCK, BLOCK), :], target.at[block % 4], sem.at[h])
            pl.when(block // 4 == (idx_ref[CORE] + seq) % 2)(copy.start)
    for h in range(2):
        pltpu.make_async_copy(out_ref.at[pl.ds(h * BLOCK, BLOCK), :], own_ref.at[0], sem.at[h]).wait()


def dz_step(idx_ref, et_ref, l_ref, tok_ref, lab_ref, tl_ref, acc_ref):
    lse = tok_ref[0, 0:1, :]
    weight = tok_ref[0, 1:2, :]
    label = lab_ref[0] - idx_ref[ROW_START]
    target = jnp.zeros((1, PAIR), jnp.float32)
    for start, n in chunk_list(et_ref.shape[1], 1024):
        tile = l_ref[start:start + n, :]
        is_target = lax.broadcasted_iota(jnp.int32, (n, PAIR), 0) == label - start
        grad = grad_tile(tile, lse, weight, is_target)
        target = target + jnp.sum(jnp.where(is_target, tile, 0.0), axis=0, keepdims=True)
        part = jnp.dot(et_ref[:, start:start + n], grad, preferred_element_type=jnp.float32)
        if start == 0:
            acc_ref[...] = part
        else:
            acc_ref[...] += part
    tl_ref[0] = target


def de_kernel(offset, rows, got_offset, idx_ref, l_ref, z_ref, tok_ref, lab_ref, *rest):
    got_ref = None if got_offset is None else rest[0]
    part_ref, out_ref, buf_ref, sem = rest[-4:]
    core = idx_ref[CORE]
    half = out_ref.shape[0] // 2
    count = idx_ref[ALL_PAIRS]

    def rows_at(side, start, n):
        return out_ref.at[pl.ds(pl.multiple_of(side * half + start, 8), n), :]

    def source(i):
        return l_ref.at[idx_ref[PAIR_IDS + i], pl.ds(offset, rows), :]

    def fetch(i):
        start(split_copy(source(i), buf_ref.at[i % 3], sem.at[i % 3], 264))

    fetch(0)
    pl.when(count > 1)(lambda: fetch(1))
    got = None
    if got_ref is not None:
        target = rows_at(1 - core, got_offset, got_ref.shape[0])
        start(split_copy(got_ref, target, sem.at[3], 264))
        got = pltpu.make_async_copy(got_ref, target, sem.at[3])
    part_ref[...] = jnp.zeros_like(part_ref)

    def step(i, carry):
        pltpu.make_async_copy(source(i), buf_ref.at[i % 3], sem.at[i % 3]).wait()
        pl.when(i + 2 < count)(lambda: fetch(i + 2))
        pair = idx_ref[PAIR_IDS + i]
        lse = tok_ref[pair, 0:1, :]
        weight = tok_ref[pair, 1:2, :]
        label = lab_ref[pair] - idx_ref[ROW_START] - offset
        for at, n in chunk_list(rows, 528):
            is_target = lax.broadcasted_iota(jnp.int32, (n, PAIR), 0) == label - at
            grad = grad_tile(buf_ref[i % 3, at:at + n, :], lse, weight, is_target)
            part_ref[at:at + n, :] += jnp.dot(grad, z_ref[pair], preferred_element_type=jnp.float32)
        return carry

    lax.fori_loop(0, count, step, 0)
    target = rows_at(core, offset, rows)
    start(split_copy(part_ref, target, sem.at[4], 264))
    pltpu.make_async_copy(part_ref, target, sem.at[4]).wait()
    if got is not None:
        got.wait()


def place_kernel(got_offset, idx_ref, got_ref, de_ref, out_ref, sem):
    half = out_ref.shape[0] // 2
    at = pl.multiple_of((1 - idx_ref[CORE]) * half + got_offset, 8)
    target = out_ref.at[pl.ds(at, got_ref.shape[0]), :]
    start(split_copy(got_ref, target, sem, 264))
    pltpu.make_async_copy(got_ref, target, sem).wait()


def lse_kernel(st_ref, lab_ref, scale_ref, tok_ref, got_ref, send_sem, recv_sem):
    tp, dp = lax.axis_index('tp'), lax.axis_index('dp')
    peers = []
    for k in range(1, 8):
        z, y, c = k // 4, k // 2 % 2, k % 2
        peer_tp = (tp // 2 + z) % 2 * 2 + (tp % 2 + y) % 2
        peers.append({'tp': peer_tp, 'dp': dp // 2 * 2 + (dp % 2 + c) % 2})
    barrier = pltpu.get_barrier_semaphore()
    for peer in peers:
        pl.semaphore_signal(barrier, inc=1, device_id=peer, device_id_type=pl.DeviceIdType.MESH)
    pl.semaphore_wait(barrier, 7)
    copies = [
        pltpu.make_async_remote_copy(st_ref, got_ref.at[k], send_sem.at[k], recv_sem.at[k], device_id=peer, device_id_type=pl.DeviceIdType.MESH)
        for k, peer in enumerate(peers)
    ]
    for copy in copies:
        copy.start()
    for copy in copies:
        copy.wait()
    top = st_ref[:, 0, :]
    for k in range(7):
        top = jnp.maximum(top, got_ref[k, :, 0, :])
    total = st_ref[:, 1, :] * jnp.exp(st_ref[:, 0, :] - top)
    for k in range(7):
        total = total + got_ref[k, :, 1, :] * jnp.exp(got_ref[k, :, 0, :] - top)
    live = lab_ref[:, 0, :] >= 0
    tok_ref[:, 0, :] = jnp.where(live, top + jnp.log(total), BIG)
    tok_ref[:, 1, :] = jnp.where(live, scale_ref[...], 0.0)


def call_lse(stats, lab, scale, collective_id):
    vmem = pl.BlockSpec(memory_space=pltpu.VMEM)
    return pl.pallas_call(
        lse_kernel,
        in_specs=[vmem, vmem, vmem],
        out_specs=vmem,
        out_shape=jax.ShapeDtypeStruct(stats.shape, jnp.float32),
        scratch_shapes=[pltpu.VMEM((7,) + stats.shape, jnp.float32), pltpu.SemaphoreType.DMA((7,)), pltpu.SemaphoreType.DMA((7,))],
        compiler_params=pltpu.CompilerParams(collective_id=collective_id, has_side_effects=True, vmem_limit_bytes=4 * 1024 * 1024),
        cost_estimate=pl.CostEstimate(flops=10_000_000, bytes_accessed=1_000_000, transcendentals=20_000),
    )(stats, lab, scale)


def norm_kernel(pick_ref, h_ref, hat_ref, inv_ref, own_ref, far_ref):
    i = pl.program_id(0)
    x = h_ref[0].astype(jnp.float32)
    centered = x - jnp.mean(x, axis=-1, keepdims=True)
    inv = lax.rsqrt(jnp.mean(centered * centered, axis=-1, keepdims=True) + LAYER_EPS)
    hat = centered * inv
    hat_ref[0] = hat

    @pl.when(i == pick_ref[0])
    def _():
        own_ref[...] = hat
        inv_ref[...] = jnp.broadcast_to(inv, inv_ref.shape)

    @pl.when(i == pick_ref[1])
    def _():
        far_ref[...] = hat


def call_norm(picks, hidden):
    n, block, width = hidden.shape
    quarter = pl.BlockSpec((block, width), lambda i, s: (0, 0))
    each = pl.BlockSpec((1, block, width), lambda i, s: (i, 0, 0))
    one = jax.ShapeDtypeStruct((block, width), jnp.float32)
    return pl.pallas_call(
        norm_kernel,
        grid_spec=pltpu.PrefetchScalarGridSpec(
            num_scalar_prefetch=1, grid=(n,), in_specs=[each],
            out_specs=[each, pl.BlockSpec((block, 128), lambda i, s: (0, 0)), quarter, quarter],
        ),
        out_shape=[jax.ShapeDtypeStruct(hidden.shape, jnp.float32), jax.ShapeDtypeStruct((block, 128), jnp.float32), one, one],
        compiler_params=params(DE_VMEM),
        cost_estimate=pl.CostEstimate(flops=10_000_000, bytes_accessed=8_000_000, transcendentals=1024),
        name="norm",
    )(picks, hidden)


def norm_bwd_kernel(a_ref, b_ref, a_got_ref, b_got_ref, hat_ref, inv_ref, gamma_ref, loss_ref, a_out, b_out, sum_out):
    piece = a_ref.shape[0]
    grad = jnp.concatenate([a_ref[...] + a_got_ref[...], b_ref[...] + b_got_ref[...]])
    hat = hat_ref[...]
    scaled = grad * gamma_ref[...]
    inner = scaled - jnp.mean(scaled, axis=-1, keepdims=True) - hat * jnp.mean(scaled * hat, axis=-1, keepdims=True)
    inner = inner * inv_ref[:, 0:1]
    a_out[...] = inner[:piece]
    b_out[...] = inner[piece:]
    sum_out[...] = jnp.zeros_like(sum_out)
    sum_out[0:1, :] = jnp.sum(grad * hat, axis=0, keepdims=True)
    sum_out[1:2, :] = jnp.sum(grad, axis=0, keepdims=True)
    sum_out[2:3, 0:128] = loss_ref[...]


def call_norm_bwd(*args):
    piece, width = args[0].shape
    vmem = pl.BlockSpec(memory_space=pltpu.VMEM)
    half = jax.ShapeDtypeStruct((piece, width), jnp.float32)
    return pl.pallas_call(
        norm_bwd_kernel,
        in_specs=[vmem] * len(args),
        out_specs=[vmem] * 3,
        out_shape=[half, half, jax.ShapeDtypeStruct((8, width), jnp.float32)],
        compiler_params=pltpu.CompilerParams(vmem_limit_bytes=DE_VMEM),
        cost_estimate=pl.CostEstimate(flops=10_000_000, bytes_accessed=4_000_000, transcendentals=0),
        name="norm_bwd",
    )(*args)


def round_kernel(pick_ref, *refs):
    out_ref = refs[-1]
    piece = refs[0].shape[0]
    for p in range(4):
        start = pl.multiple_of(pick_ref[2 + p] * (2 * piece), 2 * piece)
        out_ref[0, pl.ds(start, piece), :] = refs[2 * p][...].astype(jnp.bfloat16)
        out_ref[0, pl.ds(start + piece, piece), :] = refs[2 * p + 1][...].astype(jnp.bfloat16)


def call_round(picks, pieces):
    piece, width = pieces[0].shape
    spec = pl.BlockSpec((piece, width), lambda i, s: (0, 0), pipeline_mode=pl.Buffered(1))
    out = (1, len(pieces) * piece, width)
    return pl.pallas_call(
        round_kernel,
        grid_spec=pltpu.PrefetchScalarGridSpec(
            num_scalar_prefetch=1, grid=(1,), in_specs=[spec] * len(pieces), out_specs=pl.BlockSpec(out, lambda i, s: (0, 0, 0)),
        ),
        out_shape=jax.ShapeDtypeStruct(out, jnp.bfloat16),
        compiler_params=params(DE_VMEM),
        cost_estimate=pl.CostEstimate(flops=1_000_000, bytes_accessed=5_000_000, transcendentals=0),
        name="round",
    )(picks, *pieces)


def params(limit=VMEM_LIMIT):
    return pltpu.CompilerParams(vmem_limit_bytes=limit, dimension_semantics=("arbitrary",))


def cost(pairs, rows, width):
    n = PAIR * pairs * rows
    return pl.CostEstimate(flops=2 * n * width, bytes_accessed=4 * n, transcendentals=n)


ANY = pl.BlockSpec(memory_space=pl.ANY)


def call_logits(idx, e, gamma, beta, pieces, previous, rows):
    pairs = 8
    base, count, order = (0, NEAR_PAIRS, NEAR_PIECES) if previous is None else (4, FAR_PAIRS, FAR_PIECES)
    width = e.shape[1]
    extra = [] if previous is None else list(previous)
    spec = pltpu.PrefetchScalarGridSpec(
        num_scalar_prefetch=1,
        grid=(4,),
        in_specs=[ANY]
        + [pl.BlockSpec((1, width), lambda i, s: (0, 0))] * 2 + [ANY] * (len(pieces) + len(extra)),
        out_specs=[
            ANY,
            pl.BlockSpec((1, PAIR, width), lambda i, s: (base + last(i, s[count]), 0, 0)),
            pl.BlockSpec((1, 2, PAIR), lambda i, s: (last(i, s[count]), 0, 0)),
        ],
        scratch_shapes=[
            pltpu.VMEM((2, PAIR, width), jnp.float32),
            pltpu.VMEM((rows, width), jnp.bfloat16),
            pltpu.VMEM((2, rows, PAIR), jnp.float32),
            pltpu.SemaphoreType.DMA((2, 2)),
            pltpu.SemaphoreType.DMA,
            pltpu.SemaphoreType.DMA((2,)),
        ],
    )
    first = 4 + len(pieces)
    return pl.pallas_call(
        functools.partial(logits_kernel, count, base, order, len(pieces)),
        grid_spec=spec,
        out_shape=[
            jax.ShapeDtypeStruct((pairs, rows, PAIR), jnp.float32),
            jax.ShapeDtypeStruct((pairs, PAIR, width), jnp.bfloat16),
            jax.ShapeDtypeStruct((4, 2, PAIR), jnp.float32),
        ],
        input_output_aliases={} if previous is None else {first: 0, first + 1: 1},
        compiler_params=params(),
        cost_estimate=cost(3, rows, width),
        name="logits_near" if previous is None else "logits_far",
    )(idx, e, gamma[None], beta[None], *pieces, *extra)


def call_dz(idx, e, l, tok, lab):
    width, rows = e.shape[1], l.shape[1]
    pick_row = lambda i, s: (last(i, s[NEAR_PAIRS]), 0, 0)
    spec = pltpu.PrefetchScalarGridSpec(
        num_scalar_prefetch=1,
        grid=(4,),
        in_specs=[
            ANY,
            ANY,
            pl.BlockSpec((1, 2, PAIR), pick_row),
            pl.BlockSpec((1, 1, PAIR), pick_row),
        ],
        out_specs=[ANY, ANY, pl.BlockSpec((1, 1, PAIR), pick_row), ANY],
        scratch_shapes=[
            pltpu.VMEM((width, PAIR), jnp.float32),
            pltpu.VMEM((PAIR, width), jnp.float32),
            pltpu.VMEM((width, rows), jnp.bfloat16),
            pltpu.VMEM((rows, width), jnp.bfloat16),
            pltpu.VMEM((2, rows, PAIR), jnp.float32),
            pltpu.SemaphoreType.DMA((2,)),
            pltpu.SemaphoreType.DMA,
            pltpu.SemaphoreType.DMA((2,)),
        ],
    )
    half = jax.ShapeDtypeStruct((4, BLOCK, width), jnp.float32)
    return pl.pallas_call(
        dz_kernel,
        grid_spec=spec,
        out_shape=[half, half, jax.ShapeDtypeStruct((4, 1, PAIR), jnp.float32), jax.ShapeDtypeStruct(l.shape, l.dtype)],
        input_output_aliases={2: 3},
        compiler_params=params(),
        cost_estimate=cost(3, rows, width),
        name="dz_part",
    )(idx, e, l, tok, lab)


def call_de(idx, l, zc, tok, lab, de, offset, rows, got, got_offset):
    total, width = l.shape[1], zc.shape[2]

    def whole(x):
        return pl.BlockSpec(x.shape, lambda i, s: (0,) * x.ndim, pipeline_mode=pl.Buffered(1))

    extra = [] if de is None else [de]
    extra_specs = [ANY] * len(extra)
    if got is not None:
        extra = [got] + extra
        extra_specs = [whole(got)] + extra_specs
    spec = pltpu.PrefetchScalarGridSpec(
        num_scalar_prefetch=1,
        grid=(1,),
        in_specs=[ANY, whole(zc), whole(tok), whole(lab)] + extra_specs,
        out_specs=[pl.BlockSpec((rows, width), lambda i, s: (0, 0), pipeline_mode=pl.Buffered(1)), ANY],
        scratch_shapes=[pltpu.VMEM((3, rows, PAIR), jnp.float32), pltpu.SemaphoreType.DMA((5,))],
    )
    return pl.pallas_call(
        functools.partial(de_kernel, offset, rows, got_offset if got is not None else None),
        grid_spec=spec,
        out_shape=[jax.ShapeDtypeStruct((rows, width), jnp.float32), jax.ShapeDtypeStruct((2 * total, width), jnp.float32)],
        input_output_aliases={} if de is None else {4 + len(extra): 1},
        compiler_params=params(DE_VMEM),
        cost_estimate=cost(5, rows, width),
    )(idx, l, zc, tok, lab, *extra)


def call_place(idx, got, de, got_offset):
    spec = pltpu.PrefetchScalarGridSpec(
        num_scalar_prefetch=1,
        grid=(1,),
        in_specs=[pl.BlockSpec(got.shape, lambda i, s: (0, 0), pipeline_mode=pl.Buffered(1)), ANY],
        out_specs=ANY,
        scratch_shapes=[pltpu.SemaphoreType.DMA],
    )
    return pl.pallas_call(
        functools.partial(place_kernel, got_offset),
        grid_spec=spec,
        out_shape=jax.ShapeDtypeStruct(de.shape, de.dtype),
        input_output_aliases={2: 0},
        compiler_params=params(DE_VMEM),
        name="place",
    )(idx, got, de)


def idx_of(scalars, order, pair_idx, core, tp):
    return jnp.concatenate([scalars, order[0], order[0] ^ (core * 4), order[1] ^ (core * 4 + tp), pair_idx])


def order_blocks(active):
    n = active.shape[1]
    act = active.astype(jnp.int32)
    ids = jnp.arange(n, dtype=jnp.int32)
    before = (ids[None, :] < ids[:, None]).astype(jnp.int32)
    ahead = jnp.sum(before[None] * act[:, None, :], axis=2)
    count = jnp.sum(act, axis=1, keepdims=True)
    place = jnp.where(act > 0, ahead, count + ids - ahead)
    hit = place[:, None, :] == ids[None, :, None]
    return jnp.sum(jnp.where(hit, ids, 0), axis=2), count[:, 0], hit


def solution(mesh):
    n_tp, n_dp = mesh.shape['tp'], mesh.shape['dp']

    def flip(x, axis, bits):
        n = n_tp if axis == 'tp' else n_dp
        return lax.ppermute(x, axis, [(k, k ^ bits) for k in range(n)])

    def pick(x, index):
        return lax.dynamic_index_in_dim(x, index, 0, keepdims=False)

    def local_step(hidden, ln_gamma, ln_beta, embed_shard, labels, loss_mask):
        tp, dp = lax.axis_index('tp'), lax.axis_index('dp')
        core = dp & 1
        y, z = (tp & 1).astype(jnp.uint32), (tp >> 1).astype(jnp.uint32)
        not_y, not_z = 1 - y, 1 - z
        seq, width = hidden.shape[1:]
        quarters, piece = seq // BLOCK, BLOCK // 2
        rows = embed_shard.shape[0] // 2
        row_start = tp * (2 * rows) + core * rows

        def by_core(mine, other):
            return jnp.stack([jnp.where(core == 0, mine, other), jnp.where(core == 0, other, mine)])

        marked = jnp.where(loss_mask[0] > 0, labels[0], -1)
        far_marks = [flip(marked, 'dp', 2), flip(marked, 'dp', 3)]
        mate_marks = flip(marked, 'dp', 1)

        picks = jnp.stack([tp, tp ^ 3] + [tp ^ p for p in range(4)])
        x_hat, inv_std, own_quarter, far_quarter = call_norm(picks, hidden.reshape(quarters, BLOCK, width))
        mate = flip(x_hat, 'dp', 1)
        far0, far3 = flip(own_quarter, 'dp', 2), flip(far_quarter, 'dp', 2)

        marks = jnp.concatenate([by_core(marked, mate_marks), by_core(*far_marks)]).reshape(2, 8, BLOCK)
        token_count = jnp.sum((marks >= 0).astype(jnp.float32))
        order, active, hit = order_blocks(jnp.any(marks >= 0, axis=2))
        lab = jnp.sum(jnp.where(hit[..., None], marks[:, None], 0), axis=2).reshape(8, 1, PAIR)
        pairs = (active + 1) // 2
        pair_ids = jnp.arange(8, dtype=jnp.int32)
        pair_idx = jnp.where(pair_ids < pairs[0], pair_ids, jnp.minimum(4 + pair_ids - pairs[0], 7))
        zero = jnp.zeros((), jnp.int32)
        scalars = jnp.stack([core, pairs[0], pairs[1], pairs[0] + pairs[1], row_start, zero, zero, zero])
        idx, y, z, not_y, not_z = lax.optimization_barrier((idx_of(scalars, order, pair_idx, core, tp), y, z, not_y, not_z))

        logits, z_pairs, near_stats = call_logits(idx, embed_shard, ln_gamma, ln_beta, [x_hat, mate], None, rows)

        scale = jnp.broadcast_to(1.0 / token_count, (1, PAIR))
        near_tok = call_lse(near_stats, lab[:4], scale, 0)
        mate0, mate3 = flip(far0, 'dp', 1), flip(far3, 'dp', 1)
        far1, far2 = flip(far0, 'tp', 1), flip(far0, 'tp', 2)
        dz_own, dz_mate, target, logits = call_dz(idx, embed_shard, logits, near_tok, lab[:4])

        mate1, mate2 = flip(far1, 'dp', 1), flip(far2, 'dp', 1)
        lead = ((tp == 0) & (core == 0)).astype(jnp.float32)
        loss = jnp.sum(jnp.where(lab[:4, 0] >= 0, lead * near_tok[:, 0] - target[:, 0], 0.0)) / token_count
        loss, idx = lax.optimization_barrier((jnp.broadcast_to(loss, (1, 128)), idx))
        pieces = [far0, far1, far2, far3, mate0, mate1, mate2, mate3]
        logits, z_pairs, far_stats = call_logits(idx, embed_shard, ln_gamma, ln_beta, pieces, (logits, z_pairs), rows)
        far_tok = call_lse(far_stats, lab[4:], scale, 1)
        dz_got = flip(dz_mate, 'dp', 1)

        def part(column, half_z, half_y):
            def cut(x):
                x = x.reshape(2, 2, 2, piece, width)[:, :, column]
                return pick(x, half_z) if half_y is None else lax.dynamic_index_in_dim(x, half_y, 1, keepdims=False)

            return cut(dz_own) + cut(dz_got)

        a_got = flip(part(0, None, not_y), 'tp', 1)
        b_got = flip(part(1, not_z, None), 'tp', 2)
        a_keep = part(0, None, y) + a_got
        b_keep = part(1, z, None) + b_got
        a_grad = flip(pick(a_keep, not_z), 'tp', 2)
        b_grad = flip(pick(b_keep, not_y), 'tp', 1)
        tok = jnp.concatenate([near_tok, far_tok])

        a0, b0, sums = call_norm_bwd(pick(a_keep, z), pick(b_keep, y), a_grad, b_grad, own_quarter, inv_std, ln_gamma[None], loss)
        a1, b2 = flip(a0, 'tp', 1), flip(b0, 'tp', 2)
        a2, a3 = flip(a0, 'tp', 2), flip(a1, 'tp', 2)
        b1, b3 = flip(b0, 'tp', 1), flip(b2, 'tp', 1)
        d_hidden = call_round(picks, [a0, b0, a1, b1, a2, b2, a3, b3])

        for bits in (1, 2):
            got_sums = flip(sums, 'dp', bits)
            sums = sums + got_sums
        got_sums = [flip(sums, 'tp', k) for k in (1, 2, 3)]
        sums = sums + got_sums[0] + (got_sums[1] + got_sums[2])

        chunks = [(k * (rows // 6), rows // 6) for k in range(6)]
        d_embed, got = None, []
        for n, (offset, size) in enumerate(chunks):
            arrived = got[n - 2] if n >= 2 else None
            d_chunk, d_embed = call_de(idx, logits, z_pairs, tok, lab, d_embed, offset, size, arrived, chunks[n - 2][0] if n >= 2 else None)
            got.append(flip(d_chunk, 'dp', 1))
        for n in (4, 5):
            d_embed = call_place(idx, got[n], d_embed, chunks[n][0])

        return sums[2, 0], d_hidden, d_embed, sums[0], sums[1]


    return jax.shard_map(local_step, mesh=mesh, in_specs=(P('dp', None, None), P(None), P(None), P('tp', None), P('dp', None), P('dp', None)), out_specs=(P(), P('dp', None, None), P('tp', None), P(None), P(None)), check_vma=False)
```

```python
import functools

import jax
import jax.numpy as jnp
from jax import lax
from jax.experimental import pallas as pl
from jax.experimental.pallas import tpu as pltpu
from jax.sharding import PartitionSpec as P


LAYER_EPS = 1e-5
BLOCK = 256
PAIR = 2 * BLOCK
BIG = 1e30
VMEM_LIMIT = 62 * 1024 * 1024
DE_VMEM = 20 * 1024 * 1024
EARLY_OUT = True
DZ_CHUNK = 1024


CORE, NEAR_PAIRS, FAR_PAIRS, ALL_PAIRS, ROW_START = 0, 1, 2, 3, 4
NEAR_ORDER, NEAR_PIECES, FAR_PIECES, PAIR_IDS = 8, 16, 24, 32


def chunk_list(total, size):
    return [(start, min(size, total - start)) for start in range(0, total, size)]


def split_copy(source, target, sem, size):
    return [pltpu.make_async_copy(source.at[pl.ds(a, n), :], target.at[pl.ds(a, n), :], sem) for a, n in chunk_list(target.shape[0], size)]


def start(copies):
    for copy in copies:
        copy.start()


def last(i, count):
    return jnp.minimum(i, count - 1)


def logits_kernel(count, base, order, n_pieces, idx_ref, e_hbm, gamma_ref, beta_ref, *rest):
    pieces = rest[:n_pieces]
    l_hbm, zc_ref, st_ref, x_ref, e_ref, l_ref, sem, e_sem, l_sem = rest[-9:]
    i = pl.program_id(0)
    live = i < idx_ref[count]
    rows = e_ref.shape[0]
    slot = i % 2

    def copies(block, slot, h):
        target = x_ref.at[slot, pl.ds(h * BLOCK, BLOCK), :]
        if len(pieces[0].shape) == 3:
            return [(block >> 2 == k, pltpu.make_async_copy(ref.at[block & 3], target, sem.at[slot, h])) for k, ref in enumerate(pieces)]
        return [(block == k, pltpu.make_async_copy(ref, target, sem.at[slot, h])) for k, ref in enumerate(pieces)]

    def fetch(pair):
        for h in range(2):
            for chosen, copy in copies(idx_ref[order + 2 * pair + h], pair % 2, h):
                pl.when(chosen)(copy.start)

    def flush(k):
        pltpu.make_async_copy(l_ref.at[k], l_hbm.at[0], l_sem.at[k]).wait()

    @pl.when(i == 0)
    def _():
        fetch(0)
        table = e_hbm.at[pl.ds(pl.multiple_of(idx_ref[CORE] * rows, 16), rows), :]
        start(split_copy(table, e_ref, e_sem, 528))
        pltpu.make_async_copy(table, e_ref, e_sem).wait()

    pl.when(i + 1 < idx_ref[count])(lambda: fetch(i + 1))
    pl.when(live & (i >= 2))(lambda: flush(slot))

    @pl.when(live)
    def _():
        for h in range(2):
            copies(0, slot, h)[0][1].wait()
        zc_ref[0] = (x_ref[slot] * gamma_ref[...] + beta_ref[...]).astype(jnp.bfloat16)
        logits_step(e_ref, l_ref.at[slot], zc_ref, st_ref, split_copy(l_ref.at[slot], l_hbm.at[base + i], l_sem.at[slot], 528))

    @pl.when(i == idx_ref[count] - 1)
    def _():
        flush(slot)
        pl.when(i > 0)(lambda: flush(1 - slot))


def logits_step(e_ref, l_ref, zc_ref, st_ref, out):
    rows = e_ref.shape[0]
    size = 528
    top = jnp.full((1, PAIR), -BIG, jnp.float32)
    total = jnp.zeros((1, PAIR), jnp.float32)

    def add(start, n, old_top, top, total):
        return total * jnp.exp(old_top - top) + jnp.sum(jnp.exp(l_ref[start:start + n, :] - top), axis=0, keepdims=True)

    waiting = None
    for start, n in chunk_list(rows, size):
        tile = lax.dot_general(e_ref[start:start + n, :], zc_ref[0], (((1,), (1,)), ((), ())), preferred_element_type=jnp.float32)
        l_ref[start:start + n, :] = tile
        new_top = jnp.maximum(top, jnp.max(tile, axis=0, keepdims=True))
        if waiting is not None:
            total = add(*waiting, total)
            if EARLY_OUT:
                out[waiting[0] // size].start()
        waiting = (start, n, top, new_top)
        top = new_top
    total = add(*waiting, total)
    for copy in out[-1:] if EARLY_OUT else out:
        copy.start()
    st_ref[0, 0:1, :] = top
    st_ref[0, 1:2, :] = total


def grad_tile(tile, lse, weight, is_target):
    probs = jnp.exp(tile - lse)
    return (jnp.where(is_target, probs - 1.0, probs) * weight).astype(jnp.bfloat16)


def dz_kernel(idx_ref, e_hbm, l_hbm, tok_ref, lab_ref, own_ref, mate_ref, tl_ref, l_out_ref, acc_ref, out_ref, et_ref, e_ref, l_ref, sem, e_sem, l_sem):
    i = pl.program_id(0)
    rows = e_ref.shape[0]
    slot = i % 2
    live = i < idx_ref[NEAR_PAIRS]
    size = 512
    full = rows // size

    def fetch(pair):
        start(split_copy(l_hbm.at[pair], l_ref.at[pair % 2], l_sem.at[pair % 2], size))

    def table(k, n):
        at = pl.multiple_of(k * size, size)
        return pltpu.make_async_copy(e_hbm.at[pl.ds(pl.multiple_of(idx_ref[CORE] * rows + at, 16), n), :], e_ref.at[pl.ds(at, n), :], e_sem.at[k])

    @pl.when(i == 0)
    def _():
        for k, (_, n) in enumerate(chunk_list(rows, size)):
            table(k, n).start()
        fetch(0)

        def turn(k, carry):
            table(k, size).wait()
            at = pl.multiple_of(k * size, size)
            et_ref[:, pl.ds(at, size)] = e_ref[pl.ds(at, size), :].T
            return carry

        lax.fori_loop(0, full, turn, 0)
        if rows > full * size:
            table(full, rows - full * size).wait()
            et_ref[:, full * size:] = e_ref[full * size:, :].T

    pl.when(i + 1 < idx_ref[NEAR_PAIRS])(lambda: fetch(i + 1))

    @pl.when(live)
    def _():
        pltpu.make_async_copy(l_hbm.at[0], l_ref.at[slot], l_sem.at[slot]).wait()
        dz_step(idx_ref, et_ref, l_ref.at[slot], tok_ref, lab_ref, tl_ref, acc_ref)

    @pl.when(live)
    def _():
        out_ref[...] = acc_ref[...].T

    @pl.when(jnp.logical_not(live))
    def _():
        out_ref[...] = jnp.zeros_like(out_ref)

    for h in range(2):
        block = idx_ref[NEAR_ORDER + 2 * i + h]
        for seq in range(2):
            target = own_ref if seq == 0 else mate_ref
            copy = pltpu.make_async_copy(out_ref.at[pl.ds(h * BLOCK, BLOCK), :], target.at[block % 4], sem.at[h])
            pl.when(block // 4 == (idx_ref[CORE] + seq) % 2)(copy.start)
    for h in range(2):
        pltpu.make_async_copy(out_ref.at[pl.ds(h * BLOCK, BLOCK), :], own_ref.at[0], sem.at[h]).wait()


def dz_step(idx_ref, et_ref, l_ref, tok_ref, lab_ref, tl_ref, acc_ref):
    lse = tok_ref[0, 0:1, :]
    weight = tok_ref[0, 1:2, :]
    label = lab_ref[0] - idx_ref[ROW_START]
    target = jnp.zeros((1, PAIR), jnp.float32)
    for start, n in chunk_list(et_ref.shape[1], DZ_CHUNK):
        tile = l_ref[start:start + n, :]
        is_target = lax.broadcasted_iota(jnp.int32, (n, PAIR), 0) == label - start
        grad = grad_tile(tile, lse, weight, is_target)
        target = target + jnp.sum(jnp.where(is_target, tile, 0.0), axis=0, keepdims=True)
        part = jnp.dot(et_ref[:, start:start + n], grad, preferred_element_type=jnp.float32)
        if start == 0:
            acc_ref[...] = part
        else:
            acc_ref[...] += part
    tl_ref[0] = target


def de_kernel(offset, rows, got_offset, idx_ref, l_ref, z_ref, tok_ref, lab_ref, *rest):
    got_ref = None if got_offset is None else rest[0]
    part_ref, out_ref, buf_ref, sem = rest[-4:]
    core = idx_ref[CORE]
    half = out_ref.shape[0] // 2
    count = idx_ref[ALL_PAIRS]

    def rows_at(side, start, n):
        return out_ref.at[pl.ds(pl.multiple_of(side * half + start, 8), n), :]

    def source(i):
        return l_ref.at[idx_ref[PAIR_IDS + i], pl.ds(offset, rows), :]

    def fetch(i):
        start(split_copy(source(i), buf_ref.at[i % 3], sem.at[i % 3], 264))

    fetch(0)
    pl.when(count > 1)(lambda: fetch(1))
    got = None
    if got_ref is not None:
        target = rows_at(1 - core, got_offset, got_ref.shape[0])
        start(split_copy(got_ref, target, sem.at[3], 264))
        got = pltpu.make_async_copy(got_ref, target, sem.at[3])
    part_ref[...] = jnp.zeros_like(part_ref)

    def step(i, carry):
        pltpu.make_async_copy(source(i), buf_ref.at[i % 3], sem.at[i % 3]).wait()
        pl.when(i + 2 < count)(lambda: fetch(i + 2))
        pair = idx_ref[PAIR_IDS + i]
        lse = tok_ref[pair, 0:1, :]
        weight = tok_ref[pair, 1:2, :]
        label = lab_ref[pair] - idx_ref[ROW_START] - offset
        for at, n in chunk_list(rows, 528):
            is_target = lax.broadcasted_iota(jnp.int32, (n, PAIR), 0) == label - at
            grad = grad_tile(buf_ref[i % 3, at:at + n, :], lse, weight, is_target)
            part_ref[at:at + n, :] += jnp.dot(grad, z_ref[pair], preferred_element_type=jnp.float32)
        return carry

    lax.fori_loop(0, count, step, 0)
    target = rows_at(core, offset, rows)
    start(split_copy(part_ref, target, sem.at[4], 264))
    pltpu.make_async_copy(part_ref, target, sem.at[4]).wait()
    if got is not None:
        got.wait()


def place_kernel(got_offset, idx_ref, got_ref, de_ref, out_ref, sem):
    half = out_ref.shape[0] // 2
    at = pl.multiple_of((1 - idx_ref[CORE]) * half + got_offset, 8)
    target = out_ref.at[pl.ds(at, got_ref.shape[0]), :]
    start(split_copy(got_ref, target, sem, 264))
    pltpu.make_async_copy(got_ref, target, sem).wait()


def lse_kernel(st_ref, lab_ref, scale_ref, tok_ref, got_ref, send_sem, recv_sem):
    tp, dp = lax.axis_index('tp'), lax.axis_index('dp')
    peers = []
    for k in range(1, 8):
        z, y, c = k // 4, k // 2 % 2, k % 2
        peer_tp = (tp // 2 + z) % 2 * 2 + (tp % 2 + y) % 2
        peers.append({'tp': peer_tp, 'dp': dp // 2 * 2 + (dp % 2 + c) % 2})
    barrier = pltpu.get_barrier_semaphore()
    for peer in peers:
        pl.semaphore_signal(barrier, inc=1, device_id=peer, device_id_type=pl.DeviceIdType.MESH)
    pl.semaphore_wait(barrier, 7)
    copies = [
        pltpu.make_async_remote_copy(st_ref, got_ref.at[k], send_sem.at[k], recv_sem.at[k], device_id=peer, device_id_type=pl.DeviceIdType.MESH)
        for k, peer in enumerate(peers)
    ]
    for copy in copies:
        copy.start()
    for copy in copies:
        copy.wait()
    top = st_ref[:, 0, :]
    for k in range(7):
        top = jnp.maximum(top, got_ref[k, :, 0, :])
    total = st_ref[:, 1, :] * jnp.exp(st_ref[:, 0, :] - top)
    for k in range(7):
        total = total + got_ref[k, :, 1, :] * jnp.exp(got_ref[k, :, 0, :] - top)
    live = lab_ref[:, 0, :] >= 0
    tok_ref[:, 0, :] = jnp.where(live, top + jnp.log(total), BIG)
    tok_ref[:, 1, :] = jnp.where(live, scale_ref[...], 0.0)


def call_lse(stats, lab, scale, collective_id):
    vmem = pl.BlockSpec(memory_space=pltpu.VMEM)
    return pl.pallas_call(
        lse_kernel,
        in_specs=[vmem, vmem, vmem],
        out_specs=vmem,
        out_shape=jax.ShapeDtypeStruct(stats.shape, jnp.float32),
        scratch_shapes=[pltpu.VMEM((7,) + stats.shape, jnp.float32), pltpu.SemaphoreType.DMA((7,)), pltpu.SemaphoreType.DMA((7,))],
        compiler_params=pltpu.CompilerParams(collective_id=collective_id, has_side_effects=True, vmem_limit_bytes=4 * 1024 * 1024),
        cost_estimate=pl.CostEstimate(flops=10_000_000, bytes_accessed=1_000_000, transcendentals=20_000),
    )(stats, lab, scale)


def norm_kernel(pick_ref, h_ref, hat_ref, inv_ref, own_ref, far_ref):
    i = pl.program_id(0)
    x = h_ref[0].astype(jnp.float32)
    centered = x - jnp.mean(x, axis=-1, keepdims=True)
    inv = lax.rsqrt(jnp.mean(centered * centered, axis=-1, keepdims=True) + LAYER_EPS)
    hat = centered * inv
    hat_ref[0] = hat

    @pl.when(i == pick_ref[0])
    def _():
        own_ref[...] = hat
        inv_ref[...] = jnp.broadcast_to(inv, inv_ref.shape)

    @pl.when(i == pick_ref[1])
    def _():
        far_ref[...] = hat


def call_norm(picks, hidden):
    n, block, width = hidden.shape
    quarter = pl.BlockSpec((block, width), lambda i, s: (0, 0))
    each = pl.BlockSpec((1, block, width), lambda i, s: (i, 0, 0))
    one = jax.ShapeDtypeStruct((block, width), jnp.float32)
    return pl.pallas_call(
        norm_kernel,
        grid_spec=pltpu.PrefetchScalarGridSpec(
            num_scalar_prefetch=1, grid=(n,), in_specs=[each],
            out_specs=[each, pl.BlockSpec((block, 128), lambda i, s: (0, 0)), quarter, quarter],
        ),
        out_shape=[jax.ShapeDtypeStruct(hidden.shape, jnp.float32), jax.ShapeDtypeStruct((block, 128), jnp.float32), one, one],
        compiler_params=params(DE_VMEM),
        cost_estimate=pl.CostEstimate(flops=10_000_000, bytes_accessed=8_000_000, transcendentals=1024),
        name="norm",
    )(picks, hidden)


def norm_bwd_kernel(a_ref, b_ref, a_got_ref, b_got_ref, hat_ref, inv_ref, gamma_ref, loss_ref, a_out, b_out, sum_out):
    piece = a_ref.shape[0]
    grad = jnp.concatenate([a_ref[...] + a_got_ref[...], b_ref[...] + b_got_ref[...]])
    hat = hat_ref[...]
    scaled = grad * gamma_ref[...]
    inner = scaled - jnp.mean(scaled, axis=-1, keepdims=True) - hat * jnp.mean(scaled * hat, axis=-1, keepdims=True)
    inner = inner * inv_ref[:, 0:1]
    a_out[...] = inner[:piece]
    b_out[...] = inner[piece:]
    sum_out[...] = jnp.zeros_like(sum_out)
    sum_out[0:1, :] = jnp.sum(grad * hat, axis=0, keepdims=True)
    sum_out[1:2, :] = jnp.sum(grad, axis=0, keepdims=True)
    sum_out[2:3, 0:128] = loss_ref[...]


def call_norm_bwd(*args):
    piece, width = args[0].shape
    vmem = pl.BlockSpec(memory_space=pltpu.VMEM)
    half = jax.ShapeDtypeStruct((piece, width), jnp.float32)
    return pl.pallas_call(
        norm_bwd_kernel,
        in_specs=[vmem] * len(args),
        out_specs=[vmem] * 3,
        out_shape=[half, half, jax.ShapeDtypeStruct((8, width), jnp.float32)],
        compiler_params=pltpu.CompilerParams(vmem_limit_bytes=DE_VMEM),
        cost_estimate=pl.CostEstimate(flops=10_000_000, bytes_accessed=4_000_000, transcendentals=0),
        name="norm_bwd",
    )(*args)


def part_kernel(pick_ref, own_ref, got_ref, a_send, b_send, a_keep, b_keep):
    piece = a_send.shape[1]
    y, not_y, z, not_z = (pick_ref[6 + k] for k in range(4))
    for k in range(2):
        for out, block, at in ((a_send, 2 * k + not_y, 0), (a_keep, 2 * k + y, 0), (b_send, 2 * not_z + k, piece), (b_keep, 2 * z + k, piece)):
            out[k] = own_ref[block, at:at + piece, :] + got_ref[block, at:at + piece, :]


def call_part(picks, own, got):
    whole = pl.BlockSpec(own.shape, lambda i, s: (0, 0, 0), pipeline_mode=pl.Buffered(1))
    shape = (2, own.shape[1] // 2, own.shape[2])
    return pl.pallas_call(
        part_kernel,
        grid_spec=pltpu.PrefetchScalarGridSpec(
            num_scalar_prefetch=1, grid=(1,), in_specs=[whole, whole], out_specs=[pl.BlockSpec(shape, lambda i, s: (0, 0, 0), pipeline_mode=pl.Buffered(1))] * 4,
        ),
        out_shape=[jax.ShapeDtypeStruct(shape, jnp.float32)] * 4,
        compiler_params=params(DE_VMEM),
        cost_estimate=pl.CostEstimate(flops=1_000_000, bytes_accessed=9_000_000, transcendentals=0),
        name="part",
    )(picks, own, got)


def round_kernel(pick_ref, *refs):
    out_ref = refs[-1]
    piece = refs[0].shape[0]
    for p in range(4):
        start = pl.multiple_of(pick_ref[2 + p] * (2 * piece), 2 * piece)
        out_ref[0, pl.ds(start, piece), :] = refs[2 * p][...].astype(jnp.bfloat16)
        out_ref[0, pl.ds(start + piece, piece), :] = refs[2 * p + 1][...].astype(jnp.bfloat16)


def call_round(picks, pieces):
    piece, width = pieces[0].shape
    spec = pl.BlockSpec((piece, width), lambda i, s: (0, 0), pipeline_mode=pl.Buffered(1))
    out = (1, len(pieces) * piece, width)
    return pl.pallas_call(
        round_kernel,
        grid_spec=pltpu.PrefetchScalarGridSpec(
            num_scalar_prefetch=1, grid=(1,), in_specs=[spec] * len(pieces), out_specs=pl.BlockSpec(out, lambda i, s: (0, 0, 0)),
        ),
        out_shape=jax.ShapeDtypeStruct(out, jnp.bfloat16),
        compiler_params=params(DE_VMEM),
        cost_estimate=pl.CostEstimate(flops=1_000_000, bytes_accessed=5_000_000, transcendentals=0),
        name="round",
    )(picks, *pieces)


def params(limit=VMEM_LIMIT):
    return pltpu.CompilerParams(vmem_limit_bytes=limit, dimension_semantics=("arbitrary",))


def cost(pairs, rows, width):
    n = PAIR * pairs * rows
    return pl.CostEstimate(flops=2 * n * width, bytes_accessed=4 * n, transcendentals=n)


ANY = pl.BlockSpec(memory_space=pl.ANY)


def call_logits(idx, e, gamma, beta, pieces, previous, rows):
    pairs = 8
    base, count, order = (0, NEAR_PAIRS, NEAR_PIECES) if previous is None else (4, FAR_PAIRS, FAR_PIECES)
    width = e.shape[1]
    extra = [] if previous is None else list(previous)
    spec = pltpu.PrefetchScalarGridSpec(
        num_scalar_prefetch=1,
        grid=(4,),
        in_specs=[ANY]
        + [pl.BlockSpec((1, width), lambda i, s: (0, 0))] * 2 + [ANY] * (len(pieces) + len(extra)),
        out_specs=[
            ANY,
            pl.BlockSpec((1, PAIR, width), lambda i, s: (base + last(i, s[count]), 0, 0)),
            pl.BlockSpec((1, 2, PAIR), lambda i, s: (last(i, s[count]), 0, 0)),
        ],
        scratch_shapes=[
            pltpu.VMEM((2, PAIR, width), jnp.float32),
            pltpu.VMEM((rows, width), jnp.bfloat16),
            pltpu.VMEM((2, rows, PAIR), jnp.float32),
            pltpu.SemaphoreType.DMA((2, 2)),
            pltpu.SemaphoreType.DMA,
            pltpu.SemaphoreType.DMA((2,)),
        ],
    )
    first = 4 + len(pieces)
    return pl.pallas_call(
        functools.partial(logits_kernel, count, base, order, len(pieces)),
        grid_spec=spec,
        out_shape=[
            jax.ShapeDtypeStruct((pairs, rows, PAIR), jnp.float32),
            jax.ShapeDtypeStruct((pairs, PAIR, width), jnp.bfloat16),
            jax.ShapeDtypeStruct((4, 2, PAIR), jnp.float32),
        ],
        input_output_aliases={} if previous is None else {first: 0, first + 1: 1},
        compiler_params=params(),
        cost_estimate=cost(3, rows, width),
        name="logits_near" if previous is None else "logits_far",
    )(idx, e, gamma[None], beta[None], *pieces, *extra)


def call_dz(idx, e, l, tok, lab):
    width, rows = e.shape[1], l.shape[1]
    pick_row = lambda i, s: (last(i, s[NEAR_PAIRS]), 0, 0)
    spec = pltpu.PrefetchScalarGridSpec(
        num_scalar_prefetch=1,
        grid=(4,),
        in_specs=[
            ANY,
            ANY,
            pl.BlockSpec((1, 2, PAIR), pick_row),
            pl.BlockSpec((1, 1, PAIR), pick_row),
        ],
        out_specs=[ANY, ANY, pl.BlockSpec((1, 1, PAIR), pick_row), ANY],
        scratch_shapes=[
            pltpu.VMEM((width, PAIR), jnp.float32),
            pltpu.VMEM((PAIR, width), jnp.float32),
            pltpu.VMEM((width, rows), jnp.bfloat16),
            pltpu.VMEM((rows, width), jnp.bfloat16),
            pltpu.VMEM((2, rows, PAIR), jnp.float32),
            pltpu.SemaphoreType.DMA((2,)),
            pltpu.SemaphoreType.DMA((pl.cdiv(rows, 512),)),
            pltpu.SemaphoreType.DMA((2,)),
        ],
    )
    half = jax.ShapeDtypeStruct((4, BLOCK, width), jnp.float32)
    return pl.pallas_call(
        dz_kernel,
        grid_spec=spec,
        out_shape=[half, half, jax.ShapeDtypeStruct((4, 1, PAIR), jnp.float32), jax.ShapeDtypeStruct(l.shape, l.dtype)],
        input_output_aliases={2: 3},
        compiler_params=params(),
        cost_estimate=cost(3, rows, width),
        name="dz_part",
    )(idx, e, l, tok, lab)


def call_de(idx, l, zc, tok, lab, de, offset, rows, got, got_offset):
    total, width = l.shape[1], zc.shape[2]

    def whole(x):
        return pl.BlockSpec(x.shape, lambda i, s: (0,) * x.ndim, pipeline_mode=pl.Buffered(1))

    extra = [] if de is None else [de]
    extra_specs = [ANY] * len(extra)
    if got is not None:
        extra = [got] + extra
        extra_specs = [whole(got)] + extra_specs
    spec = pltpu.PrefetchScalarGridSpec(
        num_scalar_prefetch=1,
        grid=(1,),
        in_specs=[ANY, whole(zc), whole(tok), whole(lab)] + extra_specs,
        out_specs=[pl.BlockSpec((rows, width), lambda i, s: (0, 0), pipeline_mode=pl.Buffered(1)), ANY],
        scratch_shapes=[pltpu.VMEM((3, rows, PAIR), jnp.float32), pltpu.SemaphoreType.DMA((5,))],
    )
    return pl.pallas_call(
        functools.partial(de_kernel, offset, rows, got_offset if got is not None else None),
        grid_spec=spec,
        out_shape=[jax.ShapeDtypeStruct((rows, width), jnp.float32), jax.ShapeDtypeStruct((2 * total, width), jnp.float32)],
        input_output_aliases={} if de is None else {4 + len(extra): 1},
        compiler_params=params(DE_VMEM),
        cost_estimate=cost(5, rows, width),
    )(idx, l, zc, tok, lab, *extra)


def call_place(idx, got, de, got_offset):
    spec = pltpu.PrefetchScalarGridSpec(
        num_scalar_prefetch=1,
        grid=(1,),
        in_specs=[pl.BlockSpec(got.shape, lambda i, s: (0, 0), pipeline_mode=pl.Buffered(1)), ANY],
        out_specs=ANY,
        scratch_shapes=[pltpu.SemaphoreType.DMA],
    )
    return pl.pallas_call(
        functools.partial(place_kernel, got_offset),
        grid_spec=spec,
        out_shape=jax.ShapeDtypeStruct(de.shape, de.dtype),
        input_output_aliases={2: 0},
        compiler_params=params(DE_VMEM),
        name="place",
    )(idx, got, de)


def idx_of(scalars, order, pair_idx, core, tp):
    return jnp.concatenate([scalars, order[0], order[0] ^ (core * 4), order[1] ^ (core * 4 + tp), pair_idx])


def order_blocks(active):
    n = active.shape[1]
    act = active.astype(jnp.int32)
    ids = jnp.arange(n, dtype=jnp.int32)
    before = (ids[None, :] < ids[:, None]).astype(jnp.int32)
    ahead = jnp.sum(before[None] * act[:, None, :], axis=2)
    count = jnp.sum(act, axis=1, keepdims=True)
    place = jnp.where(act > 0, ahead, count + ids - ahead)
    hit = place[:, None, :] == ids[None, :, None]
    return jnp.sum(jnp.where(hit, ids, 0), axis=2), count[:, 0], hit


def solution(mesh):
    n_tp, n_dp = mesh.shape['tp'], mesh.shape['dp']

    def flip(x, axis, bits):
        n = n_tp if axis == 'tp' else n_dp
        return lax.ppermute(x, axis, [(k, k ^ bits) for k in range(n)])

    def pick(x, index):
        return lax.dynamic_index_in_dim(x, index, 0, keepdims=False)

    def local_step(hidden, ln_gamma, ln_beta, embed_shard, labels, loss_mask):
        tp, dp = lax.axis_index('tp'), lax.axis_index('dp')
        core = dp & 1
        y, z = (tp & 1).astype(jnp.uint32), (tp >> 1).astype(jnp.uint32)
        not_y, not_z = 1 - y, 1 - z
        seq, width = hidden.shape[1:]
        quarters = seq // BLOCK
        rows = embed_shard.shape[0] // 2
        row_start = tp * (2 * rows) + core * rows

        def by_core(mine, other):
            return jnp.stack([jnp.where(core == 0, mine, other), jnp.where(core == 0, other, mine)])

        marked = jnp.where(loss_mask[0] > 0, labels[0], -1)
        far_marks = [flip(marked, 'dp', 2), flip(marked, 'dp', 3)]
        mate_marks = flip(marked, 'dp', 1)

        picks = jnp.stack([tp, tp ^ 3] + [tp ^ p for p in range(4)] + [tp & 1, 1 - (tp & 1), tp >> 1, 1 - (tp >> 1)])
        x_hat, inv_std, own_quarter, far_quarter = call_norm(picks, hidden.reshape(quarters, BLOCK, width))
        mate = flip(x_hat, 'dp', 1)
        far0, far3 = flip(own_quarter, 'dp', 2), flip(far_quarter, 'dp', 2)

        marks = jnp.concatenate([by_core(marked, mate_marks), by_core(*far_marks)]).reshape(2, 8, BLOCK)
        token_count = jnp.sum((marks >= 0).astype(jnp.float32))
        order, active, hit = order_blocks(jnp.any(marks >= 0, axis=2))
        lab = jnp.sum(jnp.where(hit[..., None], marks[:, None], 0), axis=2).reshape(8, 1, PAIR)
        pairs = (active + 1) // 2
        pair_ids = jnp.arange(8, dtype=jnp.int32)
        pair_idx = jnp.where(pair_ids < pairs[0], pair_ids, jnp.minimum(4 + pair_ids - pairs[0], 7))
        zero = jnp.zeros((), jnp.int32)
        scalars = jnp.stack([core, pairs[0], pairs[1], pairs[0] + pairs[1], row_start, zero, zero, zero])
        idx, y, z, not_y, not_z = lax.optimization_barrier((idx_of(scalars, order, pair_idx, core, tp), y, z, not_y, not_z))

        logits, z_pairs, near_stats = call_logits(idx, embed_shard, ln_gamma, ln_beta, [x_hat, mate], None, rows)

        scale = jnp.broadcast_to(1.0 / token_count, (1, PAIR))
        near_tok = call_lse(near_stats, lab[:4], scale, 0)
        mate0, mate3 = flip(far0, 'dp', 1), flip(far3, 'dp', 1)
        far1, far2 = flip(far0, 'tp', 1), flip(far0, 'tp', 2)
        dz_own, dz_mate, target, logits = call_dz(idx, embed_shard, logits, near_tok, lab[:4])

        mate1, mate2 = flip(far1, 'dp', 1), flip(far2, 'dp', 1)
        lead = ((tp == 0) & (core == 0)).astype(jnp.float32)
        loss = jnp.sum(jnp.where(lab[:4, 0] >= 0, lead * near_tok[:, 0] - target[:, 0], 0.0)) / token_count
        loss, idx = lax.optimization_barrier((jnp.broadcast_to(loss, (1, 128)), idx))
        pieces = [far0, far1, far2, far3, mate0, mate1, mate2, mate3]
        logits, z_pairs, far_stats = call_logits(idx, embed_shard, ln_gamma, ln_beta, pieces, (logits, z_pairs), rows)
        far_tok = call_lse(far_stats, lab[4:], scale, 1)
        dz_got = flip(dz_mate, 'dp', 1)

        a_send, b_send, a_keep, b_keep = call_part(picks, dz_own, dz_got)
        a_got, b_got = flip(a_send, 'tp', 1), flip(b_send, 'tp', 2)
        a_keep, b_keep = a_keep + a_got, b_keep + b_got
        a_grad = flip(pick(a_keep, not_z), 'tp', 2)
        b_grad = flip(pick(b_keep, not_y), 'tp', 1)
        tok = jnp.concatenate([near_tok, far_tok])

        a0, b0, sums = call_norm_bwd(pick(a_keep, z), pick(b_keep, y), a_grad, b_grad, own_quarter, inv_std, ln_gamma[None], loss)
        a1, b2 = flip(a0, 'tp', 1), flip(b0, 'tp', 2)
        a2, a3 = flip(a0, 'tp', 2), flip(a1, 'tp', 2)
        b1, b3 = flip(b0, 'tp', 1), flip(b2, 'tp', 1)
        d_hidden = call_round(picks, [a0, b0, a1, b1, a2, b2, a3, b3])

        for axis in ('dp', 'tp'):
            got_sums = [flip(sums, axis, k) for k in (1, 2, 3)]
            sums = sums + got_sums[0] + (got_sums[1] + got_sums[2])

        chunks = [(0, rows // 3), (rows // 3, rows // 3), (4 * (rows // 6), rows // 6), (5 * (rows // 6), rows // 6)]
        d_embed, got = None, []
        for n, (offset, size) in enumerate(chunks):
            arrived = got[n - 2] if n >= 2 else None
            d_chunk, d_embed = call_de(idx, logits, z_pairs, tok, lab, d_embed, offset, size, arrived, chunks[n - 2][0] if n >= 2 else None)
            got.append(flip(d_chunk, 'dp', 1))
        for n in (2, 3):
            d_embed = call_place(idx, got[n], d_embed, chunks[n][0])

        return sums[2, 0], d_hidden, d_embed, sums[0], sums[1]


    return jax.shard_map(local_step, mesh=mesh, in_specs=(P('dp', None, None), P(None), P(None), P('tp', None), P('dp', None), P('dp', None)), out_specs=(P(), P('dp', None, None), P('tp', None), P(None), P(None)), check_vma=False)
```

```python
import functools

import jax
import jax.numpy as jnp
from jax import lax
from jax.experimental import pallas as pl
from jax.experimental.pallas import tpu as pltpu
from jax.sharding import PartitionSpec as P


LAYER_EPS = 1e-5
BLOCK = 256
PAIR = 2 * BLOCK
BIG = 1e30
VMEM_LIMIT = 62 * 1024 * 1024
DE_VMEM = 16 * 1024 * 1024
EARLY_OUT = True
DZ_CHUNK = 1024
LOGITS_CHUNK = 272


CORE, NEAR_PAIRS, FAR_PAIRS, ALL_PAIRS, ROW_START = 0, 1, 2, 3, 4
NEAR_ORDER, NEAR_PIECES, FAR_PIECES, PAIR_IDS = 8, 16, 24, 32


def chunk_list(total, size):
    return [(start, min(size, total - start)) for start in range(0, total, size)]


def split_copy(source, target, sem, size):
    return [pltpu.make_async_copy(source.at[pl.ds(a, n), :], target.at[pl.ds(a, n), :], sem) for a, n in chunk_list(target.shape[0], size)]


def start(copies):
    for copy in copies:
        copy.start()


def last(i, count):
    return jnp.minimum(i, count - 1)


def logits_kernel(count, base, order, n_pieces, idx_ref, e_hbm, gamma_ref, beta_ref, *rest):
    pieces = rest[:n_pieces]
    l_hbm, zc_ref, st_ref, x_ref, e_ref, l_ref, sem, e_sem, l_sem = rest[-9:]
    i = pl.program_id(0)
    live = i < idx_ref[count]
    rows = e_ref.shape[0]
    slot = i % 2

    def copies(block, slot, h):
        target = x_ref.at[slot, pl.ds(h * BLOCK, BLOCK), :]
        if len(pieces[0].shape) == 3:
            return [(block >> 2 == k, pltpu.make_async_copy(ref.at[block & 3], target, sem.at[slot, h])) for k, ref in enumerate(pieces)]
        return [(block == k, pltpu.make_async_copy(ref, target, sem.at[slot, h])) for k, ref in enumerate(pieces)]

    def fetch(pair):
        for h in range(2):
            for chosen, copy in copies(idx_ref[order + 2 * pair + h], pair % 2, h):
                pl.when(chosen)(copy.start)

    def flush(k):
        pltpu.make_async_copy(l_ref.at[k], l_hbm.at[0], l_sem.at[k]).wait()

    @pl.when(i == 0)
    def _():
        fetch(0)
        table = e_hbm.at[pl.ds(pl.multiple_of(idx_ref[CORE] * rows, 16), rows), :]
        start(split_copy(table, e_ref, e_sem, 528))
        pltpu.make_async_copy(table, e_ref, e_sem).wait()

    pl.when(i + 1 < idx_ref[count])(lambda: fetch(i + 1))
    pl.when(live & (i >= 2))(lambda: flush(slot))

    @pl.when(live)
    def _():
        for h in range(2):
            copies(0, slot, h)[0][1].wait()
        zc_ref[0] = (x_ref[slot] * gamma_ref[...][None, :] + beta_ref[...][None, :]).astype(jnp.bfloat16)
        logits_step(e_ref, l_ref.at[slot], zc_ref, st_ref, split_copy(l_ref.at[slot], l_hbm.at[base + i], l_sem.at[slot], LOGITS_CHUNK))

    @pl.when(i == idx_ref[count] - 1)
    def _():
        flush(slot)
        pl.when(i > 0)(lambda: flush(1 - slot))


def logits_step(e_ref, l_ref, zc_ref, st_ref, out):
    rows = e_ref.shape[0]
    size = LOGITS_CHUNK
    top = jnp.full((1, PAIR), -BIG, jnp.float32)
    total = jnp.zeros((1, PAIR), jnp.float32)

    def add(start, n, old_top, top, total):
        return total * jnp.exp(old_top - top) + jnp.sum(jnp.exp(l_ref[start:start + n, :] - top), axis=0, keepdims=True)

    waiting = None
    for start, n in chunk_list(rows, size):
        tile = lax.dot_general(e_ref[start:start + n, :], zc_ref[0], (((1,), (1,)), ((), ())), preferred_element_type=jnp.float32)
        l_ref[start:start + n, :] = tile
        new_top = jnp.maximum(top, jnp.max(tile, axis=0, keepdims=True))
        if waiting is not None:
            total = add(*waiting, total)
            if EARLY_OUT:
                out[waiting[0] // size].start()
        waiting = (start, n, top, new_top)
        top = new_top
    total = add(*waiting, total)
    for copy in out[-1:] if EARLY_OUT else out:
        copy.start()
    st_ref[0, 0:1, :] = top
    st_ref[0, 1:2, :] = total


def grad_tile(tile, lse, weight, is_target):
    probs = jnp.exp(tile - lse)
    return (jnp.where(is_target, probs - 1.0, probs) * weight).astype(jnp.bfloat16)


def dz_kernel(idx_ref, e_hbm, l_hbm, tok_ref, lab_ref, own_ref, mate_ref, tl_ref, l_out_ref, acc_ref, out_ref, et_ref, e_ref, l_ref, sem, e_sem, l_sem):
    i = pl.program_id(0)
    rows = e_ref.shape[0]
    slot = i % 2
    live = i < idx_ref[NEAR_PAIRS]
    size = 512
    full = rows // size

    def fetch(pair):
        start(split_copy(l_hbm.at[pair], l_ref.at[pair % 2], l_sem.at[pair % 2], size))

    def table(k, n):
        at = pl.multiple_of(k * size, size)
        return pltpu.make_async_copy(e_hbm.at[pl.ds(pl.multiple_of(idx_ref[CORE] * rows + at, 16), n), :], e_ref.at[pl.ds(at, n), :], e_sem.at[k])

    @pl.when(i == 0)
    def _():
        for k, (_, n) in enumerate(chunk_list(rows, size)):
            table(k, n).start()
        fetch(0)

        def turn(k, carry):
            table(k, size).wait()
            at = pl.multiple_of(k * size, size)
            et_ref[:, pl.ds(at, size)] = e_ref[pl.ds(at, size), :].T
            return carry

        lax.fori_loop(0, full, turn, 0)
        if rows > full * size:
            table(full, rows - full * size).wait()
            et_ref[:, full * size:] = e_ref[full * size:, :].T

    pl.when(i + 1 < idx_ref[NEAR_PAIRS])(lambda: fetch(i + 1))

    @pl.when(live)
    def _():
        pltpu.make_async_copy(l_hbm.at[0], l_ref.at[slot], l_sem.at[slot]).wait()
        dz_step(idx_ref, et_ref, l_ref.at[slot], tok_ref, lab_ref, tl_ref, acc_ref)

    def sent():
        for h in range(2):
            pltpu.make_async_copy(out_ref.at[pl.ds(h * BLOCK, BLOCK), :], own_ref.at[0], sem.at[h]).wait()

    pl.when(i > 0)(sent)

    @pl.when(live)
    def _():
        out_ref[...] = acc_ref[...].T

    @pl.when(jnp.logical_not(live))
    def _():
        out_ref[...] = jnp.zeros_like(out_ref)

    for h in range(2):
        block = idx_ref[NEAR_ORDER + 2 * i + h]
        for seq in range(2):
            target = own_ref if seq == 0 else mate_ref
            copy = pltpu.make_async_copy(out_ref.at[pl.ds(h * BLOCK, BLOCK), :], target.at[block % 4], sem.at[h])
            pl.when(block // 4 == (idx_ref[CORE] + seq) % 2)(copy.start)
    pl.when(i == pl.num_programs(0) - 1)(sent)


def dz_step(idx_ref, et_ref, l_ref, tok_ref, lab_ref, tl_ref, acc_ref):
    lse = tok_ref[0, 0:1, :]
    weight = tok_ref[0, 1:2, :]
    label = lab_ref[0] - idx_ref[ROW_START]
    target = jnp.zeros((1, PAIR), jnp.float32)
    for start, n in chunk_list(et_ref.shape[1], DZ_CHUNK):
        tile = l_ref[start:start + n, :]
        is_target = lax.broadcasted_iota(jnp.int32, (n, PAIR), 0) == label - start
        grad = grad_tile(tile, lse, weight, is_target)
        target = target + jnp.sum(jnp.where(is_target, tile, 0.0), axis=0, keepdims=True)
        part = jnp.dot(et_ref[:, start:start + n], grad, preferred_element_type=jnp.float32)
        if start == 0:
            acc_ref[...] = part
        else:
            acc_ref[...] += part
    tl_ref[0] = target


def de_kernel(offset, rows, got_offset, idx_ref, l_ref, z_ref, tok_ref, lab_ref, *rest):
    got_ref = None if got_offset is None else rest[0]
    part_ref, out_ref, buf_ref, sem = rest[-4:]
    core = idx_ref[CORE]
    half = out_ref.shape[0] // 2
    count = idx_ref[ALL_PAIRS]

    def rows_at(side, start, n):
        return out_ref.at[pl.ds(pl.multiple_of(side * half + start, 8), n), :]

    block = buf_ref.shape[1]
    steps = rows // block * count

    def source(i):
        at = pl.multiple_of(offset + i // count * block, 8)
        return l_ref.at[idx_ref[PAIR_IDS + i % count], pl.ds(at, block), :]

    def write(k):
        at = pl.multiple_of(k * block, 8)
        half_start = pl.multiple_of(core * half + offset + at, 8)
        return part_ref.at[pl.ds(at, block), :], out_ref.at[pl.ds(half_start, block), :]

    def fetch(i):
        start(split_copy(source(i), buf_ref.at[i % 3], sem.at[i % 3], 264))

    fetch(0)
    pl.when(steps > 1)(lambda: fetch(1))
    got = None
    if got_ref is not None:
        target = rows_at(1 - core, got_offset, got_ref.shape[0])
        start(split_copy(got_ref, target, sem.at[3], 264))
        got = pltpu.make_async_copy(got_ref, target, sem.at[3])
    part_ref[...] = jnp.zeros_like(part_ref)

    def step(i, carry):
        pltpu.make_async_copy(source(i), buf_ref.at[i % 3], sem.at[i % 3]).wait()
        pl.when(i + 2 < steps)(lambda: fetch(i + 2))
        k = i // count
        pair = idx_ref[PAIR_IDS + i % count]
        lse = tok_ref[pair, 0:1, :]
        weight = tok_ref[pair, 1:2, :]
        label = lab_ref[pair] - idx_ref[ROW_START] - offset - k * block
        for at, n in chunk_list(block, 528):
            is_target = lax.broadcasted_iota(jnp.int32, (n, PAIR), 0) == label - at
            grad = grad_tile(buf_ref[i % 3, at:at + n, :], lse, weight, is_target)
            part_ref[pl.ds(pl.multiple_of(k * block + at, 8), n), :] += jnp.dot(grad, z_ref[pair], preferred_element_type=jnp.float32)
        pl.when(i % count == count - 1)(lambda: start(split_copy(*write(k), sem.at[4], 264)))
        return carry

    lax.fori_loop(0, steps, step, 0)
    for k in range(rows // block):
        pltpu.make_async_copy(*write(k), sem.at[4]).wait()
    if got is not None:
        got.wait()


def place_kernel(got_offset, idx_ref, got_ref, de_ref, out_ref, sem):
    half = out_ref.shape[0] // 2
    at = pl.multiple_of((1 - idx_ref[CORE]) * half + got_offset, 8)
    target = out_ref.at[pl.ds(at, got_ref.shape[0]), :]
    start(split_copy(got_ref, target, sem, 264))
    pltpu.make_async_copy(got_ref, target, sem).wait()


def lse_kernel(st_ref, lab_ref, scale_ref, tok_ref, got_ref, send_sem, recv_sem):
    tp, dp = lax.axis_index('tp'), lax.axis_index('dp')
    peers = []
    for k in range(1, 8):
        z, y, c = k // 4, k // 2 % 2, k % 2
        peer_tp = (tp // 2 + z) % 2 * 2 + (tp % 2 + y) % 2
        peers.append({'tp': peer_tp, 'dp': dp // 2 * 2 + (dp % 2 + c) % 2})
    barrier = pltpu.get_barrier_semaphore()
    for peer in peers:
        pl.semaphore_signal(barrier, inc=1, device_id=peer, device_id_type=pl.DeviceIdType.MESH)
    pl.semaphore_wait(barrier, 7)
    copies = [
        pltpu.make_async_remote_copy(st_ref, got_ref.at[k], send_sem.at[k], recv_sem.at[k], device_id=peer, device_id_type=pl.DeviceIdType.MESH)
        for k, peer in enumerate(peers)
    ]
    for copy in copies:
        copy.start()
    for copy in copies:
        copy.wait()
    top = st_ref[:, 0, :]
    for k in range(7):
        top = jnp.maximum(top, got_ref[k, :, 0, :])
    total = st_ref[:, 1, :] * jnp.exp(st_ref[:, 0, :] - top)
    for k in range(7):
        total = total + got_ref[k, :, 1, :] * jnp.exp(got_ref[k, :, 0, :] - top)
    live = lab_ref[:, 0, :] >= 0
    tok_ref[:, 0, :] = jnp.where(live, top + jnp.log(total), BIG)
    tok_ref[:, 1, :] = jnp.where(live, scale_ref[...], 0.0)


def call_lse(stats, lab, scale, collective_id):
    vmem = pl.BlockSpec(memory_space=pltpu.VMEM)
    return pl.pallas_call(
        lse_kernel,
        in_specs=[vmem, vmem, vmem],
        out_specs=vmem,
        out_shape=jax.ShapeDtypeStruct(stats.shape, jnp.float32),
        scratch_shapes=[pltpu.VMEM((7,) + stats.shape, jnp.float32), pltpu.SemaphoreType.DMA((7,)), pltpu.SemaphoreType.DMA((7,))],
        compiler_params=pltpu.CompilerParams(collective_id=collective_id, has_side_effects=True, vmem_limit_bytes=4 * 1024 * 1024),
        cost_estimate=pl.CostEstimate(flops=10_000_000, bytes_accessed=1_000_000, transcendentals=20_000),
    )(stats, lab, scale)


def norm_kernel(pick_ref, h_ref, hat_ref, inv_ref, own_ref, far_ref):
    i = pl.program_id(0)
    x = h_ref[0].astype(jnp.float32)
    centered = x - jnp.mean(x, axis=-1, keepdims=True)
    inv = lax.rsqrt(jnp.mean(centered * centered, axis=-1, keepdims=True) + LAYER_EPS)
    hat = centered * inv
    hat_ref[0] = hat

    @pl.when(i == pick_ref[0])
    def _():
        own_ref[...] = hat
        inv_ref[...] = jnp.broadcast_to(inv, inv_ref.shape)

    @pl.when(i == pick_ref[1])
    def _():
        far_ref[...] = hat


def call_norm(picks, hidden):
    n, block, width = hidden.shape
    quarter = pl.BlockSpec((block, width), lambda i, s: (0, 0))
    each = pl.BlockSpec((1, block, width), lambda i, s: (i, 0, 0))
    one = jax.ShapeDtypeStruct((block, width), jnp.float32)
    return pl.pallas_call(
        norm_kernel,
        grid_spec=pltpu.PrefetchScalarGridSpec(
            num_scalar_prefetch=1, grid=(n,), in_specs=[each],
            out_specs=[each, pl.BlockSpec((block, 128), lambda i, s: (0, 0)), quarter, quarter],
        ),
        out_shape=[jax.ShapeDtypeStruct(hidden.shape, jnp.float32), jax.ShapeDtypeStruct((block, 128), jnp.float32), one, one],
        compiler_params=params(DE_VMEM),
        cost_estimate=pl.CostEstimate(flops=10_000_000, bytes_accessed=8_000_000, transcendentals=1024),
        name="norm",
    )(picks, hidden)


def norm_bwd_kernel(a_ref, b_ref, a_got_ref, b_got_ref, hat_ref, inv_ref, gamma_ref, loss_ref, a_out, b_out, sum_out):
    piece = a_ref.shape[0]
    grad = jnp.concatenate([a_ref[...] + a_got_ref[...], b_ref[...] + b_got_ref[...]])
    hat = hat_ref[...]
    scaled = grad * gamma_ref[...][None, :]
    inner = scaled - jnp.mean(scaled, axis=-1, keepdims=True) - hat * jnp.mean(scaled * hat, axis=-1, keepdims=True)
    inner = inner * inv_ref[:, 0:1]
    a_out[...] = inner[:piece]
    b_out[...] = inner[piece:]
    sum_out[...] = jnp.zeros_like(sum_out)
    sum_out[0:1, :] = jnp.sum(grad * hat, axis=0, keepdims=True)
    sum_out[1:2, :] = jnp.sum(grad, axis=0, keepdims=True)
    sum_out[2:3, 0:128] = loss_ref[...]


def call_norm_bwd(*args):
    piece, width = args[0].shape
    vmem = pl.BlockSpec(memory_space=pltpu.VMEM)
    half = jax.ShapeDtypeStruct((piece, width), jnp.float32)
    return pl.pallas_call(
        norm_bwd_kernel,
        in_specs=[vmem] * len(args),
        out_specs=[vmem] * 3,
        out_shape=[half, half, jax.ShapeDtypeStruct((8, width), jnp.float32)],
        compiler_params=pltpu.CompilerParams(vmem_limit_bytes=DE_VMEM),
        cost_estimate=pl.CostEstimate(flops=10_000_000, bytes_accessed=4_000_000, transcendentals=0),
        name="norm_bwd",
    )(*args)


def part_kernel(pick_ref, own_ref, got_ref, a_send, b_send, a_keep, b_keep):
    piece = a_send.shape[1]
    y, not_y, z, not_z = (pick_ref[6 + k] for k in range(4))
    for k in range(2):
        for out, block, at in ((a_send, 2 * k + not_y, 0), (a_keep, 2 * k + y, 0), (b_send, 2 * not_z + k, piece), (b_keep, 2 * z + k, piece)):
            out[k] = own_ref[block, at:at + piece, :] + got_ref[block, at:at + piece, :]


def call_part(picks, own, got):
    whole = pl.BlockSpec(own.shape, lambda i, s: (0, 0, 0), pipeline_mode=pl.Buffered(1))
    shape = (2, own.shape[1] // 2, own.shape[2])
    return pl.pallas_call(
        part_kernel,
        grid_spec=pltpu.PrefetchScalarGridSpec(
            num_scalar_prefetch=1, grid=(1,), in_specs=[whole, whole], out_specs=[pl.BlockSpec(shape, lambda i, s: (0, 0, 0), pipeline_mode=pl.Buffered(1))] * 4,
        ),
        out_shape=[jax.ShapeDtypeStruct(shape, jnp.float32)] * 4,
        compiler_params=params(DE_VMEM),
        cost_estimate=pl.CostEstimate(flops=1_000_000, bytes_accessed=9_000_000, transcendentals=0),
        name="part",
    )(picks, own, got)


def round_kernel(pick_ref, *refs):
    out_ref = refs[-1]
    piece = refs[0].shape[0]
    for p in range(4):
        start = pl.multiple_of(pick_ref[2 + p] * (2 * piece), 2 * piece)
        out_ref[0, pl.ds(start, piece), :] = refs[2 * p][...].astype(jnp.bfloat16)
        out_ref[0, pl.ds(start + piece, piece), :] = refs[2 * p + 1][...].astype(jnp.bfloat16)


def call_round(picks, pieces):
    piece, width = pieces[0].shape
    spec = pl.BlockSpec((piece, width), lambda i, s: (0, 0), pipeline_mode=pl.Buffered(1))
    out = (1, len(pieces) * piece, width)
    return pl.pallas_call(
        round_kernel,
        grid_spec=pltpu.PrefetchScalarGridSpec(
            num_scalar_prefetch=1, grid=(1,), in_specs=[spec] * len(pieces), out_specs=pl.BlockSpec(out, lambda i, s: (0, 0, 0)),
        ),
        out_shape=jax.ShapeDtypeStruct(out, jnp.bfloat16),
        compiler_params=params(DE_VMEM),
        cost_estimate=pl.CostEstimate(flops=1_000_000, bytes_accessed=5_000_000, transcendentals=0),
        name="round",
    )(picks, *pieces)


def params(limit=VMEM_LIMIT):
    return pltpu.CompilerParams(vmem_limit_bytes=limit, dimension_semantics=("arbitrary",))


def cost(pairs, rows, width):
    n = PAIR * pairs * rows
    return pl.CostEstimate(flops=2 * n * width, bytes_accessed=4 * n, transcendentals=n)


ANY = pl.BlockSpec(memory_space=pl.ANY)


def call_logits(idx, e, gamma, beta, pieces, previous, rows):
    pairs = 8
    base, count, order = (0, NEAR_PAIRS, NEAR_PIECES) if previous is None else (4, FAR_PAIRS, FAR_PIECES)
    width = e.shape[1]
    extra = [] if previous is None else list(previous)
    spec = pltpu.PrefetchScalarGridSpec(
        num_scalar_prefetch=1,
        grid=(4,),
        in_specs=[ANY]
        + [pl.BlockSpec((width,), lambda i, s: (0,))] * 2 + [ANY] * (len(pieces) + len(extra)),
        out_specs=[
            ANY,
            pl.BlockSpec((1, PAIR, width), lambda i, s: (base + last(i, s[count]), 0, 0)),
            pl.BlockSpec((1, 2, PAIR), lambda i, s: (last(i, s[count]), 0, 0)),
        ],
        scratch_shapes=[
            pltpu.VMEM((2, PAIR, width), jnp.float32),
            pltpu.VMEM((rows, width), jnp.bfloat16),
            pltpu.VMEM((2, rows, PAIR), jnp.float32),
            pltpu.SemaphoreType.DMA((2, 2)),
            pltpu.SemaphoreType.DMA,
            pltpu.SemaphoreType.DMA((2,)),
        ],
    )
    first = 4 + len(pieces)
    return pl.pallas_call(
        functools.partial(logits_kernel, count, base, order, len(pieces)),
        grid_spec=spec,
        out_shape=[
            jax.ShapeDtypeStruct((pairs, rows, PAIR), jnp.float32),
            jax.ShapeDtypeStruct((pairs, PAIR, width), jnp.bfloat16),
            jax.ShapeDtypeStruct((4, 2, PAIR), jnp.float32),
        ],
        input_output_aliases={} if previous is None else {first: 0, first + 1: 1},
        compiler_params=params(),
        cost_estimate=cost(3, rows, width),
        name="logits_near" if previous is None else "logits_far",
    )(idx, e, gamma, beta, *pieces, *extra)


def call_dz(idx, e, l, tok, lab):
    width, rows = e.shape[1], l.shape[1]
    pick_row = lambda i, s: (last(i, s[NEAR_PAIRS]), 0, 0)
    spec = pltpu.PrefetchScalarGridSpec(
        num_scalar_prefetch=1,
        grid=(4,),
        in_specs=[
            ANY,
            ANY,
            pl.BlockSpec((1, 2, PAIR), pick_row),
            pl.BlockSpec((1, 1, PAIR), pick_row),
        ],
        out_specs=[ANY, ANY, pl.BlockSpec((1, 1, PAIR), pick_row), ANY],
        scratch_shapes=[
            pltpu.VMEM((width, PAIR), jnp.float32),
            pltpu.VMEM((PAIR, width), jnp.float32),
            pltpu.VMEM((width, rows), jnp.bfloat16),
            pltpu.VMEM((rows, width), jnp.bfloat16),
            pltpu.VMEM((2, rows, PAIR), jnp.float32),
            pltpu.SemaphoreType.DMA((2,)),
            pltpu.SemaphoreType.DMA((pl.cdiv(rows, 512),)),
            pltpu.SemaphoreType.DMA((2,)),
        ],
    )
    half = jax.ShapeDtypeStruct((4, BLOCK, width), jnp.float32)
    return pl.pallas_call(
        dz_kernel,
        grid_spec=spec,
        out_shape=[half, half, jax.ShapeDtypeStruct((4, 1, PAIR), jnp.float32), jax.ShapeDtypeStruct(l.shape, l.dtype)],
        input_output_aliases={2: 3},
        compiler_params=params(),
        cost_estimate=cost(3, rows, width),
        name="dz_part",
    )(idx, e, l, tok, lab)


def call_de(idx, l, zc, tok, lab, de, offset, rows, got, got_offset):
    total, width = l.shape[1], zc.shape[2]

    def whole(x):
        return pl.BlockSpec(x.shape, lambda i, s: (0,) * x.ndim, pipeline_mode=pl.Buffered(1))

    extra = [] if de is None else [de]
    extra_specs = [ANY] * len(extra)
    if got is not None:
        extra = [got] + extra
        extra_specs = [whole(got)] + extra_specs
    spec = pltpu.PrefetchScalarGridSpec(
        num_scalar_prefetch=1,
        grid=(1,),
        in_specs=[ANY, whole(zc), whole(tok), whole(lab)] + extra_specs,
        out_specs=[pl.BlockSpec((rows, width), lambda i, s: (0, 0), pipeline_mode=pl.Buffered(1)), ANY],
        scratch_shapes=[pltpu.VMEM((3, total // 6, PAIR), jnp.float32), pltpu.SemaphoreType.DMA((5,))],
    )
    return pl.pallas_call(
        functools.partial(de_kernel, offset, rows, got_offset if got is not None else None),
        grid_spec=spec,
        out_shape=[jax.ShapeDtypeStruct((rows, width), jnp.float32), jax.ShapeDtypeStruct((2 * total, width), jnp.float32)],
        input_output_aliases={} if de is None else {4 + len(extra): 1},
        compiler_params=params(DE_VMEM),
        cost_estimate=cost(5, rows, width),
    )(idx, l, zc, tok, lab, *extra)


def call_place(idx, got, de, got_offset):
    spec = pltpu.PrefetchScalarGridSpec(
        num_scalar_prefetch=1,
        grid=(1,),
        in_specs=[pl.BlockSpec(got.shape, lambda i, s: (0, 0), pipeline_mode=pl.Buffered(1)), ANY],
        out_specs=ANY,
        scratch_shapes=[pltpu.SemaphoreType.DMA],
    )
    return pl.pallas_call(
        functools.partial(place_kernel, got_offset),
        grid_spec=spec,
        out_shape=jax.ShapeDtypeStruct(de.shape, de.dtype),
        input_output_aliases={2: 0},
        compiler_params=params(DE_VMEM),
        name="place",
    )(idx, got, de)


def idx_of(scalars, order, pair_idx, core, tp):
    return jnp.concatenate([scalars, order[0], order[0] ^ (core * 4), order[1] ^ (core * 4 + tp), pair_idx])


def order_blocks(active):
    n = active.shape[1]
    act = active.astype(jnp.int32)
    ids = jnp.arange(n, dtype=jnp.int32)
    before = (ids[None, :] < ids[:, None]).astype(jnp.int32)
    ahead = jnp.sum(before[None] * act[:, None, :], axis=2)
    count = jnp.sum(act, axis=1, keepdims=True)
    place = jnp.where(act > 0, ahead, count + ids - ahead)
    hit = place[:, None, :] == ids[None, :, None]
    return jnp.sum(jnp.where(hit, ids, 0), axis=2), count[:, 0], hit


def solution(mesh):
    n_tp, n_dp = mesh.shape['tp'], mesh.shape['dp']

    def flip(x, axis, bits):
        n = n_tp if axis == 'tp' else n_dp
        return lax.ppermute(x, axis, [(k, k ^ bits) for k in range(n)])

    def pick(x, index):
        return lax.dynamic_index_in_dim(x, index, 0, keepdims=False)

    def local_step(hidden, ln_gamma, ln_beta, embed_shard, labels, loss_mask):
        tp, dp = lax.axis_index('tp'), lax.axis_index('dp')
        core = dp & 1
        y, z = (tp & 1).astype(jnp.uint32), (tp >> 1).astype(jnp.uint32)
        not_y, not_z = 1 - y, 1 - z
        seq, width = hidden.shape[1:]
        quarters = seq // BLOCK
        rows = embed_shard.shape[0] // 2
        row_start = tp * (2 * rows) + core * rows

        def by_core(mine, other):
            return jnp.stack([jnp.where(core == 0, mine, other), jnp.where(core == 0, other, mine)])

        marked = jnp.where(loss_mask[0] > 0, labels[0], -1)
        far_marks = [flip(marked, 'dp', 2), flip(marked, 'dp', 3)]
        mate_marks = flip(marked, 'dp', 1)

        picks = jnp.stack([tp, tp ^ 3] + [tp ^ p for p in range(4)] + [tp & 1, 1 - (tp & 1), tp >> 1, 1 - (tp >> 1)])
        x_hat, inv_std, own_quarter, far_quarter = call_norm(picks, hidden.reshape(quarters, BLOCK, width))
        mate = flip(x_hat, 'dp', 1)
        far0, far3 = flip(own_quarter, 'dp', 2), flip(far_quarter, 'dp', 2)

        marks = jnp.concatenate([by_core(marked, mate_marks), by_core(*far_marks)]).reshape(2, 8, BLOCK)
        token_count = jnp.sum((marks >= 0).astype(jnp.float32))
        order, active, hit = order_blocks(jnp.any(marks >= 0, axis=2))
        lab = jnp.sum(jnp.where(hit[..., None], marks[:, None], 0), axis=2).reshape(8, 1, PAIR)
        pairs = (active + 1) // 2
        pair_ids = jnp.arange(8, dtype=jnp.int32)
        pair_idx = jnp.where(pair_ids < pairs[0], pair_ids, jnp.minimum(4 + pair_ids - pairs[0], 7))
        zero = jnp.zeros((), jnp.int32)
        scalars = jnp.stack([core, pairs[0], pairs[1], pairs[0] + pairs[1], row_start, zero, zero, zero])
        idx, y, z, not_y, not_z = lax.optimization_barrier((idx_of(scalars, order, pair_idx, core, tp), y, z, not_y, not_z))

        logits, z_pairs, near_stats = call_logits(idx, embed_shard, ln_gamma, ln_beta, [x_hat, mate], None, rows)

        scale = jnp.broadcast_to(1.0 / token_count, (1, PAIR))
        near_tok = call_lse(near_stats, lab[:4], scale, 0)
        mate0, mate3 = flip(far0, 'dp', 1), flip(far3, 'dp', 1)
        far1, far2 = flip(far0, 'tp', 1), flip(far0, 'tp', 2)
        dz_own, dz_mate, target, logits = call_dz(idx, embed_shard, logits, near_tok, lab[:4])

        mate1, mate2 = flip(far1, 'dp', 1), flip(far2, 'dp', 1)
        lead = ((tp == 0) & (core == 0)).astype(jnp.float32)
        loss = jnp.sum(jnp.where(lab[:4, 0] >= 0, lead * near_tok[:, 0] - target[:, 0], 0.0)) / token_count
        loss, idx = lax.optimization_barrier((jnp.broadcast_to(loss, (1, 128)), idx))
        pieces = [far0, far1, far2, far3, mate0, mate1, mate2, mate3]
        logits, z_pairs, far_stats = call_logits(idx, embed_shard, ln_gamma, ln_beta, pieces, (logits, z_pairs), rows)
        far_tok = call_lse(far_stats, lab[4:], scale, 1)
        dz_got = flip(dz_mate, 'dp', 1)

        a_send, b_send, a_keep, b_keep = call_part(picks, dz_own, dz_got)
        a_got, b_got = flip(a_send, 'tp', 1), flip(b_send, 'tp', 2)
        a_keep, b_keep = a_keep + a_got, b_keep + b_got
        a_grad = flip(pick(a_keep, not_z), 'tp', 2)
        b_grad = flip(pick(b_keep, not_y), 'tp', 1)
        tok = jnp.concatenate([near_tok, far_tok])

        a0, b0, sums = call_norm_bwd(pick(a_keep, z), pick(b_keep, y), a_grad, b_grad, own_quarter, inv_std, ln_gamma, loss)
        a1, b2 = flip(a0, 'tp', 1), flip(b0, 'tp', 2)
        a2, a3 = flip(a0, 'tp', 2), flip(a1, 'tp', 2)
        b1, b3 = flip(b0, 'tp', 1), flip(b2, 'tp', 1)
        d_hidden = call_round(picks, [a0, b0, a1, b1, a2, b2, a3, b3])

        for axis in ('dp', 'tp'):
            got_sums = [flip(sums, axis, k) for k in (1, 2, 3)]
            sums = sums + got_sums[0] + (got_sums[1] + got_sums[2])

        chunks = [(0, rows // 3), (rows // 3, rows // 3), (4 * (rows // 6), rows // 6), (5 * (rows // 6), rows // 6)]
        d_embed, got = None, []
        for n, (offset, size) in enumerate(chunks):
            arrived = got[n - 2] if n >= 2 else None
            d_chunk, d_embed = call_de(idx, logits, z_pairs, tok, lab, d_embed, offset, size, arrived, chunks[n - 2][0] if n >= 2 else None)
            got.append(flip(d_chunk, 'dp', 1))
        for n in (2, 3):
            d_embed = call_place(idx, got[n], d_embed, chunks[n][0])

        return sums[2, 0], d_hidden, d_embed, sums[0], sums[1]


    return jax.shard_map(local_step, mesh=mesh, in_specs=(P('dp', None, None), P(None), P(None), P('tp', None), P('dp', None), P('dp', None)), out_specs=(P(), P('dp', None, None), P('tp', None), P(None), P(None)), check_vma=False)
```

```python
import functools

import jax
import jax.numpy as jnp
from jax import lax
from jax.experimental import pallas as pl
from jax.experimental.pallas import tpu as pltpu
from jax.sharding import PartitionSpec as P


LAYER_EPS = 1e-5
BLOCK = 256
PAIR = 2 * BLOCK
BIG = 1e30
VMEM_LIMIT = 62 * 1024 * 1024
DE_VMEM = 16 * 1024 * 1024
EARLY_OUT = True
DZ_CHUNK = 1024
LOGITS_CHUNK = 272


CORE, NEAR_PAIRS, FAR_PAIRS, ALL_PAIRS, ROW_START = 0, 1, 2, 3, 4
NEAR_ORDER, NEAR_PIECES, FAR_PIECES, PAIR_IDS = 8, 16, 24, 32


def chunk_list(total, size):
    return [(start, min(size, total - start)) for start in range(0, total, size)]


def split_copy(source, target, sem, size):
    return [pltpu.make_async_copy(source.at[pl.ds(a, n), :], target.at[pl.ds(a, n), :], sem) for a, n in chunk_list(target.shape[0], size)]


def start(copies):
    for copy in copies:
        copy.start()


def last(i, count):
    return jnp.minimum(i, count - 1)


def logits_kernel(count, base, order, n_pieces, idx_ref, e_hbm, gamma_ref, beta_ref, *rest):
    pieces = rest[:n_pieces]
    l_hbm, zc_ref, st_ref, x_ref, e_ref, l_ref, sem, e_sem, l_sem = rest[-9:]
    i = pl.program_id(0)
    live = i < idx_ref[count]
    rows = e_ref.shape[0]
    slot = i % 2

    def copies(block, slot, h):
        target = x_ref.at[slot, pl.ds(h * BLOCK, BLOCK), :]
        if len(pieces[0].shape) == 3:
            return [(block >> 2 == k, pltpu.make_async_copy(ref.at[block & 3], target, sem.at[slot, h])) for k, ref in enumerate(pieces)]
        return [(block == k, pltpu.make_async_copy(ref, target, sem.at[slot, h])) for k, ref in enumerate(pieces)]

    def fetch(pair):
        for h in range(2):
            for chosen, copy in copies(idx_ref[order + 2 * pair + h], pair % 2, h):
                pl.when(chosen)(copy.start)

    def flush(k):
        pltpu.make_async_copy(l_ref.at[k], l_hbm.at[0], l_sem.at[k]).wait()

    @pl.when(i == 0)
    def _():
        fetch(0)
        table = e_hbm.at[pl.ds(pl.multiple_of(idx_ref[CORE] * rows, 16), rows), :]
        start(split_copy(table, e_ref, e_sem, 528))
        pltpu.make_async_copy(table, e_ref, e_sem).wait()

    pl.when(i + 1 < idx_ref[count])(lambda: fetch(i + 1))
    pl.when(live & (i >= 2))(lambda: flush(slot))

    @pl.when(live)
    def _():
        for h in range(2):
            copies(0, slot, h)[0][1].wait()
        zc_ref[0] = (x_ref[slot] * gamma_ref[...][None, :] + beta_ref[...][None, :]).astype(jnp.bfloat16)
        logits_step(e_ref, l_ref.at[slot], zc_ref, st_ref, split_copy(l_ref.at[slot], l_hbm.at[base + i], l_sem.at[slot], LOGITS_CHUNK))

    @pl.when(i == idx_ref[count] - 1)
    def _():
        flush(slot)
        pl.when(i > 0)(lambda: flush(1 - slot))


def logits_step(e_ref, l_ref, zc_ref, st_ref, out):
    rows = e_ref.shape[0]
    size = LOGITS_CHUNK
    top = jnp.full((1, PAIR), -BIG, jnp.float32)
    total = jnp.zeros((1, PAIR), jnp.float32)

    def add(start, n, old_top, top, total):
        return total * jnp.exp(old_top - top) + jnp.sum(jnp.exp(l_ref[start:start + n, :] - top), axis=0, keepdims=True)

    waiting = None
    for start, n in chunk_list(rows, size):
        tile = lax.dot_general(e_ref[start:start + n, :], zc_ref[0], (((1,), (1,)), ((), ())), preferred_element_type=jnp.float32)
        l_ref[start:start + n, :] = tile
        new_top = jnp.maximum(top, jnp.max(tile, axis=0, keepdims=True))
        if waiting is not None:
            total = add(*waiting, total)
            if EARLY_OUT:
                out[waiting[0] // size].start()
        waiting = (start, n, top, new_top)
        top = new_top
    total = add(*waiting, total)
    for copy in out[-1:] if EARLY_OUT else out:
        copy.start()
    st_ref[0, 0:1, :] = top
    st_ref[0, 1:2, :] = total


def grad_tile(tile, lse, weight, is_target):
    probs = jnp.exp(tile - lse)
    return (jnp.where(is_target, probs - 1.0, probs) * weight).astype(jnp.bfloat16)


def dz_kernel(idx_ref, e_hbm, l_hbm, tok_ref, lab_ref, own_ref, mate_ref, tl_ref, l_out_ref, acc_ref, out_ref, et_ref, e_ref, l_ref, sem, e_sem, l_sem, first_sem):
    i = pl.program_id(0)
    rows = e_ref.shape[0]
    slot = i % 2
    live = i < idx_ref[NEAR_PAIRS]
    table = e_hbm.at[pl.ds(pl.multiple_of(idx_ref[CORE] * rows, 16), rows), :]
    chunks = chunk_list(rows, DZ_CHUNK)

    def first(k):
        at = pl.ds(*chunks[k])
        return (
            pltpu.make_async_copy(table.at[at, :], e_ref.at[at, :], e_sem.at[k]),
            pltpu.make_async_copy(l_hbm.at[0, at, :], l_ref.at[0, at, :], first_sem.at[k]),
        )

    def fetch(pair):
        start(split_copy(l_hbm.at[pair], l_ref.at[pair % 2], l_sem.at[pair % 2], 512))

    @pl.when(i == 0)
    def _():
        for k in range(len(chunks)):
            start(first(k))

    pl.when(i + 1 < idx_ref[NEAR_PAIRS])(lambda: fetch(i + 1))

    @pl.when(i == 0)
    def _():
        def turn(k):
            at, n = chunks[k]
            et_ref[:, at:at + n] = e_ref[at:at + n, :].T

        def ready(k):
            if k == 0:
                first(0)[0].wait()
                turn(0)
            if k + 1 < len(chunks):
                first(k + 1)[0].wait()
            first(k)[1].wait()
            if k + 1 < len(chunks):
                turn(k + 1)

        dz_step(idx_ref, et_ref, l_ref.at[0], tok_ref, lab_ref, tl_ref, acc_ref, ready)

    @pl.when(live & (i > 0))
    def _():
        pltpu.make_async_copy(l_hbm.at[0], l_ref.at[slot], l_sem.at[slot]).wait()
        dz_step(idx_ref, et_ref, l_ref.at[slot], tok_ref, lab_ref, tl_ref, acc_ref, None)

    def sent():
        for h in range(2):
            pltpu.make_async_copy(out_ref.at[pl.ds(h * BLOCK, BLOCK), :], own_ref.at[0], sem.at[h]).wait()

    pl.when(i > 0)(sent)

    @pl.when(live)
    def _():
        out_ref[...] = acc_ref[...].T

    @pl.when(jnp.logical_not(live))
    def _():
        out_ref[...] = jnp.zeros_like(out_ref)

    for h in range(2):
        block = idx_ref[NEAR_ORDER + 2 * i + h]
        for seq in range(2):
            target = own_ref if seq == 0 else mate_ref
            copy = pltpu.make_async_copy(out_ref.at[pl.ds(h * BLOCK, BLOCK), :], target.at[block % 4], sem.at[h])
            pl.when(block // 4 == (idx_ref[CORE] + seq) % 2)(copy.start)
    pl.when(i == pl.num_programs(0) - 1)(sent)


def dz_step(idx_ref, et_ref, l_ref, tok_ref, lab_ref, tl_ref, acc_ref, ready):
    lse = tok_ref[0, 0:1, :]
    weight = tok_ref[0, 1:2, :]
    label = lab_ref[0] - idx_ref[ROW_START]
    target = jnp.zeros((1, PAIR), jnp.float32)
    for k, (start, n) in enumerate(chunk_list(et_ref.shape[1], DZ_CHUNK)):
        if ready is not None:
            ready(k)
        tile = l_ref[start:start + n, :]
        is_target = lax.broadcasted_iota(jnp.int32, (n, PAIR), 0) == label - start
        grad = grad_tile(tile, lse, weight, is_target)
        target = target + jnp.sum(jnp.where(is_target, tile, 0.0), axis=0, keepdims=True)
        part = jnp.dot(et_ref[:, start:start + n], grad, preferred_element_type=jnp.float32)
        if start == 0:
            acc_ref[...] = part
        else:
            acc_ref[...] += part
    tl_ref[0] = target


def de_kernel(offset, rows, got_offset, idx_ref, l_ref, z_ref, tok_ref, lab_ref, *rest):
    got_ref = None if got_offset is None else rest[0]
    part_ref, out_ref, buf_ref, sem = rest[-4:]
    core = idx_ref[CORE]
    half = out_ref.shape[0] // 2
    count = idx_ref[ALL_PAIRS]

    def rows_at(side, start, n):
        return out_ref.at[pl.ds(pl.multiple_of(side * half + start, 8), n), :]

    block = buf_ref.shape[1]
    steps = rows // block * count

    def source(i):
        at = pl.multiple_of(offset + i // count * block, 8)
        return l_ref.at[idx_ref[PAIR_IDS + i % count], pl.ds(at, block), :]

    def write(k):
        at = pl.multiple_of(k * block, 8)
        half_start = pl.multiple_of(core * half + offset + at, 8)
        return part_ref.at[pl.ds(at, block), :], out_ref.at[pl.ds(half_start, block), :]

    def fetch(i):
        start(split_copy(source(i), buf_ref.at[i % 2], sem.at[i % 2], 264))

    fetch(0)
    got = None
    if got_ref is not None:
        target = rows_at(1 - core, got_offset, got_ref.shape[0])
        start(split_copy(got_ref, target, sem.at[3], 264))
        got = pltpu.make_async_copy(got_ref, target, sem.at[3])
    part_ref[...] = jnp.zeros_like(part_ref)

    def step(i, carry):
        pltpu.make_async_copy(source(i), buf_ref.at[i % 2], sem.at[i % 2]).wait()
        pl.when(i + 1 < steps)(lambda: fetch(i + 1))
        k = i // count
        pair = idx_ref[PAIR_IDS + i % count]
        lse = tok_ref[pair, 0:1, :]
        weight = tok_ref[pair, 1:2, :]
        label = lab_ref[pair] - idx_ref[ROW_START] - offset - k * block
        for at, n in chunk_list(block, 528):
            is_target = lax.broadcasted_iota(jnp.int32, (n, PAIR), 0) == label - at
            grad = grad_tile(buf_ref[i % 2, at:at + n, :], lse, weight, is_target)
            part_ref[pl.ds(pl.multiple_of(k * block + at, 8), n), :] += jnp.dot(grad, z_ref[pair], preferred_element_type=jnp.float32)
        pl.when(i % count == count - 1)(lambda: start(split_copy(*write(k), sem.at[4], 264)))
        return carry

    lax.fori_loop(0, steps, step, 0)
    for k in range(rows // block):
        pltpu.make_async_copy(*write(k), sem.at[4]).wait()
    if got is not None:
        got.wait()


def place_kernel(got_offset, idx_ref, got_ref, de_ref, out_ref, sem):
    half = out_ref.shape[0] // 2
    at = pl.multiple_of((1 - idx_ref[CORE]) * half + got_offset, 8)
    target = out_ref.at[pl.ds(at, got_ref.shape[0]), :]
    start(split_copy(got_ref, target, sem, 264))
    pltpu.make_async_copy(got_ref, target, sem).wait()


def lse_kernel(st_ref, lab_ref, scale_ref, tok_ref, got_ref, send_sem, recv_sem):
    tp, dp = lax.axis_index('tp'), lax.axis_index('dp')
    peers = []
    for k in range(1, 8):
        z, y, c = k // 4, k // 2 % 2, k % 2
        peer_tp = (tp // 2 + z) % 2 * 2 + (tp % 2 + y) % 2
        peers.append({'tp': peer_tp, 'dp': dp // 2 * 2 + (dp % 2 + c) % 2})
    barrier = pltpu.get_barrier_semaphore()
    for peer in peers:
        pl.semaphore_signal(barrier, inc=1, device_id=peer, device_id_type=pl.DeviceIdType.MESH)
    pl.semaphore_wait(barrier, 7)
    copies = [
        pltpu.make_async_remote_copy(st_ref, got_ref.at[k], send_sem.at[k], recv_sem.at[k], device_id=peer, device_id_type=pl.DeviceIdType.MESH)
        for k, peer in enumerate(peers)
    ]
    for copy in copies:
        copy.start()
    for copy in copies:
        copy.wait()
    top = st_ref[:, 0, :]
    for k in range(7):
        top = jnp.maximum(top, got_ref[k, :, 0, :])
    total = st_ref[:, 1, :] * jnp.exp(st_ref[:, 0, :] - top)
    for k in range(7):
        total = total + got_ref[k, :, 1, :] * jnp.exp(got_ref[k, :, 0, :] - top)
    live = lab_ref[:, 0, :] >= 0
    tok_ref[:, 0, :] = jnp.where(live, top + jnp.log(total), BIG)
    tok_ref[:, 1, :] = jnp.where(live, scale_ref[...], 0.0)


def call_lse(stats, lab, scale, collective_id):
    vmem = pl.BlockSpec(memory_space=pltpu.VMEM)
    return pl.pallas_call(
        lse_kernel,
        in_specs=[vmem, vmem, vmem],
        out_specs=vmem,
        out_shape=jax.ShapeDtypeStruct(stats.shape, jnp.float32),
        scratch_shapes=[pltpu.VMEM((7,) + stats.shape, jnp.float32), pltpu.SemaphoreType.DMA((7,)), pltpu.SemaphoreType.DMA((7,))],
        compiler_params=pltpu.CompilerParams(collective_id=collective_id, has_side_effects=True, vmem_limit_bytes=4 * 1024 * 1024),
        cost_estimate=pl.CostEstimate(flops=10_000_000, bytes_accessed=1_000_000, transcendentals=20_000),
    )(stats, lab, scale)


def norm_kernel(pick_ref, h_ref, hat_ref, inv_ref, own_ref, far_ref):
    i = pl.program_id(0)
    x = h_ref[0].astype(jnp.float32)
    centered = x - jnp.mean(x, axis=-1, keepdims=True)
    inv = lax.rsqrt(jnp.mean(centered * centered, axis=-1, keepdims=True) + LAYER_EPS)
    hat = centered * inv
    hat_ref[0] = hat

    @pl.when(i == pick_ref[0])
    def _():
        own_ref[...] = hat
        inv_ref[...] = jnp.broadcast_to(inv, inv_ref.shape)

    @pl.when(i == pick_ref[1])
    def _():
        far_ref[...] = hat


def call_norm(picks, hidden):
    n, block, width = hidden.shape
    quarter = pl.BlockSpec((block, width), lambda i, s: (0, 0))
    each = pl.BlockSpec((1, block, width), lambda i, s: (i, 0, 0))
    one = jax.ShapeDtypeStruct((block, width), jnp.float32)
    return pl.pallas_call(
        norm_kernel,
        grid_spec=pltpu.PrefetchScalarGridSpec(
            num_scalar_prefetch=1, grid=(n,), in_specs=[each],
            out_specs=[each, pl.BlockSpec((block, 128), lambda i, s: (0, 0)), quarter, quarter],
        ),
        out_shape=[jax.ShapeDtypeStruct(hidden.shape, jnp.float32), jax.ShapeDtypeStruct((block, 128), jnp.float32), one, one],
        compiler_params=params(DE_VMEM),
        cost_estimate=pl.CostEstimate(flops=10_000_000, bytes_accessed=8_000_000, transcendentals=1024),
        name="norm",
    )(picks, hidden)


def norm_bwd_kernel(a_ref, b_ref, a_got_ref, b_got_ref, hat_ref, inv_ref, gamma_ref, loss_ref, a_out, b_out, sum_out):
    piece = a_ref.shape[0]
    grad = jnp.concatenate([a_ref[...] + a_got_ref[...], b_ref[...] + b_got_ref[...]])
    hat = hat_ref[...]
    scaled = grad * gamma_ref[...][None, :]
    inner = scaled - jnp.mean(scaled, axis=-1, keepdims=True) - hat * jnp.mean(scaled * hat, axis=-1, keepdims=True)
    inner = inner * inv_ref[:, 0:1]
    a_out[...] = inner[:piece]
    b_out[...] = inner[piece:]
    sum_out[...] = jnp.zeros_like(sum_out)
    sum_out[0:1, :] = jnp.sum(grad * hat, axis=0, keepdims=True)
    sum_out[1:2, :] = jnp.sum(grad, axis=0, keepdims=True)
    sum_out[2:3, 0:128] = loss_ref[...]


def call_norm_bwd(*args):
    piece, width = args[0].shape
    vmem = pl.BlockSpec(memory_space=pltpu.VMEM)
    half = jax.ShapeDtypeStruct((piece, width), jnp.float32)
    return pl.pallas_call(
        norm_bwd_kernel,
        in_specs=[vmem] * len(args),
        out_specs=[vmem] * 3,
        out_shape=[half, half, jax.ShapeDtypeStruct((8, width), jnp.float32)],
        compiler_params=pltpu.CompilerParams(vmem_limit_bytes=DE_VMEM),
        cost_estimate=pl.CostEstimate(flops=10_000_000, bytes_accessed=4_000_000, transcendentals=0),
        name="norm_bwd",
    )(*args)


def part_kernel(pick_ref, own_ref, got_ref, a_send, b_send, a_keep, b_keep):
    piece = a_send.shape[1]
    y, not_y, z, not_z = (pick_ref[6 + k] for k in range(4))
    for k in range(2):
        for out, block, at in ((a_send, 2 * k + not_y, 0), (a_keep, 2 * k + y, 0), (b_send, 2 * not_z + k, piece), (b_keep, 2 * z + k, piece)):
            out[k] = own_ref[block, at:at + piece, :] + got_ref[block, at:at + piece, :]


def call_part(picks, own, got):
    whole = pl.BlockSpec(own.shape, lambda i, s: (0, 0, 0), pipeline_mode=pl.Buffered(1))
    shape = (2, own.shape[1] // 2, own.shape[2])
    return pl.pallas_call(
        part_kernel,
        grid_spec=pltpu.PrefetchScalarGridSpec(
            num_scalar_prefetch=1, grid=(1,), in_specs=[whole, whole], out_specs=[pl.BlockSpec(shape, lambda i, s: (0, 0, 0), pipeline_mode=pl.Buffered(1))] * 4,
        ),
        out_shape=[jax.ShapeDtypeStruct(shape, jnp.float32)] * 4,
        compiler_params=params(DE_VMEM),
        cost_estimate=pl.CostEstimate(flops=1_000_000, bytes_accessed=9_000_000, transcendentals=0),
        name="part",
    )(picks, own, got)


def round_kernel(pick_ref, *refs):
    out_ref = refs[-1]
    piece = refs[0].shape[0]
    for p in range(4):
        start = pl.multiple_of(pick_ref[2 + p] * (2 * piece), 2 * piece)
        out_ref[0, pl.ds(start, piece), :] = refs[2 * p][...].astype(jnp.bfloat16)
        out_ref[0, pl.ds(start + piece, piece), :] = refs[2 * p + 1][...].astype(jnp.bfloat16)


def call_round(picks, pieces):
    piece, width = pieces[0].shape
    spec = pl.BlockSpec((piece, width), lambda i, s: (0, 0), pipeline_mode=pl.Buffered(1))
    out = (1, len(pieces) * piece, width)
    return pl.pallas_call(
        round_kernel,
        grid_spec=pltpu.PrefetchScalarGridSpec(
            num_scalar_prefetch=1, grid=(1,), in_specs=[spec] * len(pieces), out_specs=pl.BlockSpec(out, lambda i, s: (0, 0, 0)),
        ),
        out_shape=jax.ShapeDtypeStruct(out, jnp.bfloat16),
        compiler_params=params(DE_VMEM),
        cost_estimate=pl.CostEstimate(flops=1_000_000, bytes_accessed=5_000_000, transcendentals=0),
        name="round",
    )(picks, *pieces)


def params(limit=VMEM_LIMIT):
    return pltpu.CompilerParams(vmem_limit_bytes=limit, dimension_semantics=("arbitrary",))


def cost(pairs, rows, width):
    n = PAIR * pairs * rows
    return pl.CostEstimate(flops=2 * n * width, bytes_accessed=4 * n, transcendentals=n)


ANY = pl.BlockSpec(memory_space=pl.ANY)


def call_logits(idx, e, gamma, beta, pieces, previous, rows):
    pairs = 8
    base, count, order = (0, NEAR_PAIRS, NEAR_PIECES) if previous is None else (4, FAR_PAIRS, FAR_PIECES)
    width = e.shape[1]
    extra = [] if previous is None else list(previous)
    spec = pltpu.PrefetchScalarGridSpec(
        num_scalar_prefetch=1,
        grid=(4,),
        in_specs=[ANY]
        + [pl.BlockSpec((width,), lambda i, s: (0,))] * 2 + [ANY] * (len(pieces) + len(extra)),
        out_specs=[
            ANY,
            pl.BlockSpec((1, PAIR, width), lambda i, s: (base + last(i, s[count]), 0, 0)),
            pl.BlockSpec((1, 2, PAIR), lambda i, s: (last(i, s[count]), 0, 0)),
        ],
        scratch_shapes=[
            pltpu.VMEM((2, PAIR, width), jnp.float32),
            pltpu.VMEM((rows, width), jnp.bfloat16),
            pltpu.VMEM((2, rows, PAIR), jnp.float32),
            pltpu.SemaphoreType.DMA((2, 2)),
            pltpu.SemaphoreType.DMA,
            pltpu.SemaphoreType.DMA((2,)),
        ],
    )
    first = 4 + len(pieces)
    return pl.pallas_call(
        functools.partial(logits_kernel, count, base, order, len(pieces)),
        grid_spec=spec,
        out_shape=[
            jax.ShapeDtypeStruct((pairs, rows, PAIR), jnp.float32),
            jax.ShapeDtypeStruct((pairs, PAIR, width), jnp.bfloat16),
            jax.ShapeDtypeStruct((4, 2, PAIR), jnp.float32),
        ],
        input_output_aliases={} if previous is None else {first: 0, first + 1: 1},
        compiler_params=params(),
        cost_estimate=cost(3, rows, width),
        name="logits_near" if previous is None else "logits_far",
    )(idx, e, gamma, beta, *pieces, *extra)


def call_dz(idx, e, l, tok, lab):
    width, rows = e.shape[1], l.shape[1]
    pick_row = lambda i, s: (last(i, s[NEAR_PAIRS]), 0, 0)
    spec = pltpu.PrefetchScalarGridSpec(
        num_scalar_prefetch=1,
        grid=(4,),
        in_specs=[
            ANY,
            ANY,
            pl.BlockSpec((1, 2, PAIR), pick_row),
            pl.BlockSpec((1, 1, PAIR), pick_row),
        ],
        out_specs=[ANY, ANY, pl.BlockSpec((1, 1, PAIR), pick_row), ANY],
        scratch_shapes=[
            pltpu.VMEM((width, PAIR), jnp.float32),
            pltpu.VMEM((PAIR, width), jnp.float32),
            pltpu.VMEM((width, rows), jnp.bfloat16),
            pltpu.VMEM((rows, width), jnp.bfloat16),
            pltpu.VMEM((2, rows, PAIR), jnp.float32),
            pltpu.SemaphoreType.DMA((2,)),
            pltpu.SemaphoreType.DMA((pl.cdiv(rows, DZ_CHUNK),)),
            pltpu.SemaphoreType.DMA((2,)),
            pltpu.SemaphoreType.DMA((pl.cdiv(rows, DZ_CHUNK),)),
        ],
    )
    half = jax.ShapeDtypeStruct((4, BLOCK, width), jnp.float32)
    return pl.pallas_call(
        dz_kernel,
        grid_spec=spec,
        out_shape=[half, half, jax.ShapeDtypeStruct((4, 1, PAIR), jnp.float32), jax.ShapeDtypeStruct(l.shape, l.dtype)],
        input_output_aliases={2: 3},
        compiler_params=params(),
        cost_estimate=cost(3, rows, width),
        name="dz_part",
    )(idx, e, l, tok, lab)


def call_de(idx, l, zc, tok, lab, de, offset, rows, got, got_offset):
    total, width = l.shape[1], zc.shape[2]

    def whole(x):
        return pl.BlockSpec(x.shape, lambda i, s: (0,) * x.ndim, pipeline_mode=pl.Buffered(1))

    extra = [] if de is None else [de]
    extra_specs = [ANY] * len(extra)
    if got is not None:
        extra = [got] + extra
        extra_specs = [whole(got)] + extra_specs
    spec = pltpu.PrefetchScalarGridSpec(
        num_scalar_prefetch=1,
        grid=(1,),
        in_specs=[ANY, whole(zc), whole(tok), whole(lab)] + extra_specs,
        out_specs=[pl.BlockSpec((rows, width), lambda i, s: (0, 0), pipeline_mode=pl.Buffered(1)), ANY],
        scratch_shapes=[pltpu.VMEM((2, rows, PAIR), jnp.float32), pltpu.SemaphoreType.DMA((5,))],
    )
    return pl.pallas_call(
        functools.partial(de_kernel, offset, rows, got_offset if got is not None else None),
        grid_spec=spec,
        out_shape=[jax.ShapeDtypeStruct((rows, width), jnp.float32), jax.ShapeDtypeStruct((2 * total, width), jnp.float32)],
        input_output_aliases={} if de is None else {4 + len(extra): 1},
        compiler_params=params(DE_VMEM),
        cost_estimate=cost(5, rows, width),
    )(idx, l, zc, tok, lab, *extra)


def call_place(idx, got, de, got_offset):
    spec = pltpu.PrefetchScalarGridSpec(
        num_scalar_prefetch=1,
        grid=(1,),
        in_specs=[pl.BlockSpec(got.shape, lambda i, s: (0, 0), pipeline_mode=pl.Buffered(1)), ANY],
        out_specs=ANY,
        scratch_shapes=[pltpu.SemaphoreType.DMA],
    )
    return pl.pallas_call(
        functools.partial(place_kernel, got_offset),
        grid_spec=spec,
        out_shape=jax.ShapeDtypeStruct(de.shape, de.dtype),
        input_output_aliases={2: 0},
        compiler_params=params(DE_VMEM),
        name="place",
    )(idx, got, de)


def idx_of(scalars, order, pair_idx, core, tp):
    return jnp.concatenate([scalars, order[0], order[0] ^ (core * 4), order[1] ^ (core * 4 + tp), pair_idx])


def order_blocks(active):
    n = active.shape[1]
    act = active.astype(jnp.int32)
    ids = jnp.arange(n, dtype=jnp.int32)
    before = (ids[None, :] < ids[:, None]).astype(jnp.int32)
    ahead = jnp.sum(before[None] * act[:, None, :], axis=2)
    count = jnp.sum(act, axis=1, keepdims=True)
    place = jnp.where(act > 0, ahead, count + ids - ahead)
    hit = place[:, None, :] == ids[None, :, None]
    return jnp.sum(jnp.where(hit, ids, 0), axis=2), count[:, 0], hit


def solution(mesh):
    n_tp, n_dp = mesh.shape['tp'], mesh.shape['dp']

    def flip(x, axis, bits):
        n = n_tp if axis == 'tp' else n_dp
        return lax.ppermute(x, axis, [(k, k ^ bits) for k in range(n)])

    def pick(x, index):
        return lax.dynamic_index_in_dim(x, index, 0, keepdims=False)

    def local_step(hidden, ln_gamma, ln_beta, embed_shard, labels, loss_mask):
        tp, dp = lax.axis_index('tp'), lax.axis_index('dp')
        core = dp & 1
        y, z = (tp & 1).astype(jnp.uint32), (tp >> 1).astype(jnp.uint32)
        not_y, not_z = 1 - y, 1 - z
        seq, width = hidden.shape[1:]
        quarters = seq // BLOCK
        rows = embed_shard.shape[0] // 2
        row_start = tp * (2 * rows) + core * rows

        def by_core(mine, other):
            return jnp.stack([jnp.where(core == 0, mine, other), jnp.where(core == 0, other, mine)])

        marked = jnp.where(loss_mask[0] > 0, labels[0], -1)
        far_marks = [flip(marked, 'dp', 2), flip(marked, 'dp', 3)]
        mate_marks = flip(marked, 'dp', 1)

        picks = jnp.stack([tp, tp ^ 3] + [tp ^ p for p in range(4)] + [tp & 1, 1 - (tp & 1), tp >> 1, 1 - (tp >> 1)])
        x_hat, inv_std, own_quarter, far_quarter = call_norm(picks, hidden.reshape(quarters, BLOCK, width))
        mate = flip(x_hat, 'dp', 1)
        far0, far3 = flip(own_quarter, 'dp', 2), flip(far_quarter, 'dp', 2)

        marks = jnp.concatenate([by_core(marked, mate_marks), by_core(*far_marks)]).reshape(2, 8, BLOCK)
        token_count = jnp.sum((marks >= 0).astype(jnp.float32))
        order, active, hit = order_blocks(jnp.any(marks >= 0, axis=2))
        lab = jnp.sum(jnp.where(hit[..., None], marks[:, None], 0), axis=2).reshape(8, 1, PAIR)
        pairs = (active + 1) // 2
        pair_ids = jnp.arange(8, dtype=jnp.int32)
        pair_idx = jnp.where(pair_ids < pairs[0], pair_ids, jnp.minimum(4 + pair_ids - pairs[0], 7))
        zero = jnp.zeros((), jnp.int32)
        scalars = jnp.stack([core, pairs[0], pairs[1], pairs[0] + pairs[1], row_start, zero, zero, zero])
        idx, y, z, not_y, not_z = lax.optimization_barrier((idx_of(scalars, order, pair_idx, core, tp), y, z, not_y, not_z))

        logits, z_pairs, near_stats = call_logits(idx, embed_shard, ln_gamma, ln_beta, [x_hat, mate], None, rows)

        scale = jnp.broadcast_to(1.0 / token_count, (1, PAIR))
        near_tok = call_lse(near_stats, lab[:4], scale, 0)
        mate0, mate3 = flip(far0, 'dp', 1), flip(far3, 'dp', 1)
        far1, far2 = flip(far0, 'tp', 1), flip(far0, 'tp', 2)
        dz_own, dz_mate, target, logits = call_dz(idx, embed_shard, logits, near_tok, lab[:4])

        mate1, mate2 = flip(far1, 'dp', 1), flip(far2, 'dp', 1)
        lead = ((tp == 0) & (core == 0)).astype(jnp.float32)
        loss = jnp.sum(jnp.where(lab[:4, 0] >= 0, lead * near_tok[:, 0] - target[:, 0], 0.0)) / token_count
        loss, idx = lax.optimization_barrier((jnp.broadcast_to(loss, (1, 128)), idx))
        pieces = [far0, far1, far2, far3, mate0, mate1, mate2, mate3]
        logits, z_pairs, far_stats = call_logits(idx, embed_shard, ln_gamma, ln_beta, pieces, (logits, z_pairs), rows)
        far_tok = call_lse(far_stats, lab[4:], scale, 1)
        dz_got = flip(dz_mate, 'dp', 1)

        a_send, b_send, a_keep, b_keep = call_part(picks, dz_own, dz_got)
        a_got, b_got = flip(a_send, 'tp', 1), flip(b_send, 'tp', 2)
        a_keep, b_keep = a_keep + a_got, b_keep + b_got
        a_grad = flip(pick(a_keep, not_z), 'tp', 2)
        b_grad = flip(pick(b_keep, not_y), 'tp', 1)
        tok = jnp.concatenate([near_tok, far_tok])

        a0, b0, sums = call_norm_bwd(pick(a_keep, z), pick(b_keep, y), a_grad, b_grad, own_quarter, inv_std, ln_gamma, loss)
        a1, b2 = flip(a0, 'tp', 1), flip(b0, 'tp', 2)
        a2, a3 = flip(a0, 'tp', 2), flip(a1, 'tp', 2)
        b1, b3 = flip(b0, 'tp', 1), flip(b2, 'tp', 1)
        d_hidden = call_round(picks, [a0, b0, a1, b1, a2, b2, a3, b3])

        for axis in ('dp', 'tp'):
            got_sums = [flip(sums, axis, k) for k in (1, 2, 3)]
            sums = sums + got_sums[0] + (got_sums[1] + got_sums[2])

        chunks = [(0, rows // 3), (rows // 3, rows // 3), (4 * (rows // 6), rows // 6), (5 * (rows // 6), rows // 6)]
        d_embed, got = None, []
        for n, (offset, size) in enumerate(chunks):
            arrived = got[n - 2] if n >= 2 else None
            d_chunk, d_embed = call_de(idx, logits, z_pairs, tok, lab, d_embed, offset, size, arrived, chunks[n - 2][0] if n >= 2 else None)
            got.append(flip(d_chunk, 'dp', 1))
        for n in (2, 3):
            d_embed = call_place(idx, got[n], d_embed, chunks[n][0])

        return sums[2, 0], d_hidden, d_embed, sums[0], sums[1]


    return jax.shard_map(local_step, mesh=mesh, in_specs=(P('dp', None, None), P(None), P(None), P('tp', None), P('dp', None), P('dp', None)), out_specs=(P(), P('dp', None, None), P('tp', None), P(None), P(None)), check_vma=False)
```

```python
import functools

import jax
import jax.numpy as jnp
from jax import lax
from jax.experimental import pallas as pl
from jax.experimental.pallas import tpu as pltpu
from jax.sharding import PartitionSpec as P


LAYER_EPS = 1e-5
BLOCK = 256
PAIR = 2 * BLOCK
BIG = 1e30
VMEM_LIMIT = 62 * 1024 * 1024
DE_VMEM = 16 * 1024 * 1024
EARLY_OUT = True
DZ_CHUNK = 1024
LOGITS_CHUNK = 272


CORE, NEAR_PAIRS, FAR_PAIRS, ALL_PAIRS, ROW_START = 0, 1, 2, 3, 4
NEAR_ORDER, NEAR_PIECES, FAR_PIECES, PAIR_IDS = 8, 16, 24, 32


def chunk_list(total, size):
    return [(start, min(size, total - start)) for start in range(0, total, size)]


def split_copy(source, target, sem, size):
    return [pltpu.make_async_copy(source.at[pl.ds(a, n), :], target.at[pl.ds(a, n), :], sem) for a, n in chunk_list(target.shape[0], size)]


def start(copies):
    for copy in copies:
        copy.start()


def last(i, count):
    return jnp.minimum(i, count - 1)


def logits_kernel(count, base, order, n_pieces, idx_ref, e_hbm, gamma_ref, beta_ref, *rest):
    pieces = rest[:n_pieces]
    l_hbm, zc_ref, st_ref, x_ref, e_ref, l_ref, sem, e_sem, l_sem = rest[-9:]
    i = pl.program_id(0)
    live = i < idx_ref[count]
    rows = e_ref.shape[0]
    slot = i % 2

    def copies(block, slot, h):
        target = x_ref.at[slot, pl.ds(h * BLOCK, BLOCK), :]
        if len(pieces[0].shape) == 3:
            return [(block >> 2 == k, pltpu.make_async_copy(ref.at[block & 3], target, sem.at[slot, h])) for k, ref in enumerate(pieces)]
        return [(block == k, pltpu.make_async_copy(ref, target, sem.at[slot, h])) for k, ref in enumerate(pieces)]

    def fetch(pair):
        for h in range(2):
            for chosen, copy in copies(idx_ref[order + 2 * pair + h], pair % 2, h):
                pl.when(chosen)(copy.start)

    def flush(k):
        pltpu.make_async_copy(l_ref.at[k], l_hbm.at[0], l_sem.at[k]).wait()

    @pl.when(i == 0)
    def _():
        fetch(0)
        table = e_hbm.at[pl.ds(pl.multiple_of(idx_ref[CORE] * rows, 16), rows), :]
        start(split_copy(table, e_ref, e_sem, 528))
        pltpu.make_async_copy(table, e_ref, e_sem).wait()

    pl.when(i + 1 < idx_ref[count])(lambda: fetch(i + 1))
    pl.when(live & (i >= 2))(lambda: flush(slot))

    @pl.when(live)
    def _():
        for h in range(2):
            copies(0, slot, h)[0][1].wait()
        zc_ref[0] = (x_ref[slot] * gamma_ref[...][None, :] + beta_ref[...][None, :]).astype(jnp.bfloat16)
        logits_step(e_ref, l_ref.at[slot], zc_ref, st_ref, split_copy(l_ref.at[slot], l_hbm.at[base + i], l_sem.at[slot], LOGITS_CHUNK))

    @pl.when(i == idx_ref[count] - 1)
    def _():
        flush(slot)
        pl.when(i > 0)(lambda: flush(1 - slot))


def logits_step(e_ref, l_ref, zc_ref, st_ref, out):
    rows = e_ref.shape[0]
    size = LOGITS_CHUNK
    top = jnp.full((1, PAIR), -BIG, jnp.float32)
    total = jnp.zeros((1, PAIR), jnp.float32)

    def add(start, n, old_top, top, total):
        return total * jnp.exp(old_top - top) + jnp.sum(jnp.exp(l_ref[start:start + n, :] - top), axis=0, keepdims=True)

    waiting = None
    for start, n in chunk_list(rows, size):
        tile = lax.dot_general(e_ref[start:start + n, :], zc_ref[0], (((1,), (1,)), ((), ())), preferred_element_type=jnp.float32)
        l_ref[start:start + n, :] = tile
        new_top = jnp.maximum(top, jnp.max(tile, axis=0, keepdims=True))
        if waiting is not None:
            total = add(*waiting, total)
            if EARLY_OUT:
                out[waiting[0] // size].start()
        waiting = (start, n, top, new_top)
        top = new_top
    total = add(*waiting, total)
    for copy in out[-1:] if EARLY_OUT else out:
        copy.start()
    st_ref[0, 0:1, :] = top
    st_ref[0, 1:2, :] = total


def grad_tile(tile, lse, weight, is_target):
    probs = jnp.exp(tile - lse)
    return (jnp.where(is_target, probs - 1.0, probs) * weight).astype(jnp.bfloat16)


def dz_kernel(idx_ref, e_hbm, l_hbm, tok_ref, lab_ref, own_ref, mate_ref, tl_ref, l_out_ref, acc_ref, out_ref, et_ref, e_ref, l_ref, sem, e_sem, l_sem, first_sem):
    i = pl.program_id(0)
    rows = e_ref.shape[0]
    slot = i % 2
    live = i < idx_ref[NEAR_PAIRS]
    table = e_hbm.at[pl.ds(pl.multiple_of(idx_ref[CORE] * rows, 16), rows), :]
    chunks = chunk_list(rows, DZ_CHUNK)

    def first(k):
        at = pl.ds(*chunks[k])
        return (
            pltpu.make_async_copy(table.at[at, :], e_ref.at[at, :], e_sem.at[k]),
            pltpu.make_async_copy(l_hbm.at[0, at, :], l_ref.at[0, at, :], first_sem.at[k]),
        )

    def fetch(pair):
        start(split_copy(l_hbm.at[pair], l_ref.at[pair % 2], l_sem.at[pair % 2], 512))

    @pl.when(i == 0)
    def _():
        for k in range(min(3, len(chunks))):
            start(first(k))

    pl.when((i > 0) & (i + 1 < idx_ref[NEAR_PAIRS]))(lambda: fetch(i + 1))

    @pl.when(i == 0)
    def _():
        def turn(k):
            at, n = chunks[k]
            et_ref[:, at:at + n] = e_ref[at:at + n, :].T

        def ready(k):
            if k + 3 < len(chunks):
                start(first(k + 3))
            elif k + 3 == len(chunks):
                pl.when(idx_ref[NEAR_PAIRS] > 1)(lambda: fetch(1))
            if k == 0:
                first(0)[0].wait()
                turn(0)
            if k + 1 < len(chunks):
                first(k + 1)[0].wait()
            first(k)[1].wait()
            if k + 1 < len(chunks):
                turn(k + 1)

        dz_step(idx_ref, et_ref, l_ref.at[0], tok_ref, lab_ref, tl_ref, acc_ref, ready)

    @pl.when(live & (i > 0))
    def _():
        pltpu.make_async_copy(l_hbm.at[0], l_ref.at[slot], l_sem.at[slot]).wait()
        dz_step(idx_ref, et_ref, l_ref.at[slot], tok_ref, lab_ref, tl_ref, acc_ref, None)

    def sent():
        for h in range(2):
            pltpu.make_async_copy(out_ref.at[pl.ds(h * BLOCK, BLOCK), :], own_ref.at[0], sem.at[h]).wait()

    pl.when(i > 0)(sent)

    @pl.when(live)
    def _():
        out_ref[...] = acc_ref[...].T

    @pl.when(jnp.logical_not(live))
    def _():
        out_ref[...] = jnp.zeros_like(out_ref)

    for h in range(2):
        block = idx_ref[NEAR_ORDER + 2 * i + h]
        for seq in range(2):
            target = own_ref if seq == 0 else mate_ref
            copy = pltpu.make_async_copy(out_ref.at[pl.ds(h * BLOCK, BLOCK), :], target.at[block % 4], sem.at[h])
            pl.when(block // 4 == (idx_ref[CORE] + seq) % 2)(copy.start)
    pl.when(i == pl.num_programs(0) - 1)(sent)


def dz_step(idx_ref, et_ref, l_ref, tok_ref, lab_ref, tl_ref, acc_ref, ready):
    lse = tok_ref[0, 0:1, :]
    weight = tok_ref[0, 1:2, :]
    label = lab_ref[0] - idx_ref[ROW_START]
    target = jnp.zeros((1, PAIR), jnp.float32)
    for k, (start, n) in enumerate(chunk_list(et_ref.shape[1], DZ_CHUNK)):
        if ready is not None:
            ready(k)
        tile = l_ref[start:start + n, :]
        is_target = lax.broadcasted_iota(jnp.int32, (n, PAIR), 0) == label - start
        grad = grad_tile(tile, lse, weight, is_target)
        target = target + jnp.sum(jnp.where(is_target, tile, 0.0), axis=0, keepdims=True)
        part = jnp.dot(et_ref[:, start:start + n], grad, preferred_element_type=jnp.float32)
        if start == 0:
            acc_ref[...] = part
        else:
            acc_ref[...] += part
    tl_ref[0] = target


def de_kernel(offset, rows, got_offset, idx_ref, l_ref, z_ref, tok_ref, lab_ref, *rest):
    got_ref = None if got_offset is None else rest[0]
    part_ref, out_ref, buf_ref, sem = rest[-4:]
    core = idx_ref[CORE]
    half = out_ref.shape[0] // 2
    count = idx_ref[ALL_PAIRS]

    def rows_at(side, start, n):
        return out_ref.at[pl.ds(pl.multiple_of(side * half + start, 8), n), :]

    block = buf_ref.shape[1]
    steps = rows // block * count

    def source(i):
        at = pl.multiple_of(offset + i // count * block, 8)
        return l_ref.at[idx_ref[PAIR_IDS + i % count], pl.ds(at, block), :]

    def write(k):
        at = pl.multiple_of(k * block, 8)
        half_start = pl.multiple_of(core * half + offset + at, 8)
        return part_ref.at[pl.ds(at, block), :], out_ref.at[pl.ds(half_start, block), :]

    def fetch(i):
        start(split_copy(source(i), buf_ref.at[i % 3], sem.at[i % 3], 264))

    fetch(0)
    pl.when(steps > 1)(lambda: fetch(1))
    got = None
    if got_ref is not None:
        target = rows_at(1 - core, got_offset, got_ref.shape[0])
        start(split_copy(got_ref, target, sem.at[3], 264))
        got = pltpu.make_async_copy(got_ref, target, sem.at[3])
    part_ref[...] = jnp.zeros_like(part_ref)

    def step(i, carry):
        pltpu.make_async_copy(source(i), buf_ref.at[i % 3], sem.at[i % 3]).wait()
        pl.when(i + 2 < steps)(lambda: fetch(i + 2))
        k = i // count
        pair = idx_ref[PAIR_IDS + i % count]
        lse = tok_ref[pair, 0:1, :]
        weight = tok_ref[pair, 1:2, :]
        label = lab_ref[pair] - idx_ref[ROW_START] - offset - k * block
        for at, n in chunk_list(block, 528):
            is_target = lax.broadcasted_iota(jnp.int32, (n, PAIR), 0) == label - at
            grad = grad_tile(buf_ref[i % 3, at:at + n, :], lse, weight, is_target)
            part_ref[pl.ds(pl.multiple_of(k * block + at, 8), n), :] += jnp.dot(grad, z_ref[pair], preferred_element_type=jnp.float32)
        pl.when(i % count == count - 1)(lambda: start(split_copy(*write(k), sem.at[4], 264)))
        return carry

    lax.fori_loop(0, steps, step, 0)
    for k in range(rows // block):
        pltpu.make_async_copy(*write(k), sem.at[4]).wait()
    if got is not None:
        got.wait()


def place_kernel(got_offset, idx_ref, got_ref, de_ref, out_ref, sem):
    half = out_ref.shape[0] // 2
    at = pl.multiple_of((1 - idx_ref[CORE]) * half + got_offset, 8)
    target = out_ref.at[pl.ds(at, got_ref.shape[0]), :]
    start(split_copy(got_ref, target, sem, 264))
    pltpu.make_async_copy(got_ref, target, sem).wait()


def lse_kernel(st_ref, lab_ref, scale_ref, tok_ref, got_ref, send_sem, recv_sem):
    tp, dp = lax.axis_index('tp'), lax.axis_index('dp')
    peers = []
    for k in range(1, 8):
        z, y, c = k // 4, k // 2 % 2, k % 2
        peer_tp = (tp // 2 + z) % 2 * 2 + (tp % 2 + y) % 2
        peers.append({'tp': peer_tp, 'dp': dp // 2 * 2 + (dp % 2 + c) % 2})
    barrier = pltpu.get_barrier_semaphore()
    for peer in peers:
        pl.semaphore_signal(barrier, inc=1, device_id=peer, device_id_type=pl.DeviceIdType.MESH)
    pl.semaphore_wait(barrier, 7)
    copies = [
        pltpu.make_async_remote_copy(st_ref, got_ref.at[k], send_sem.at[k], recv_sem.at[k], device_id=peer, device_id_type=pl.DeviceIdType.MESH)
        for k, peer in enumerate(peers)
    ]
    for copy in copies:
        copy.start()
    for copy in copies:
        copy.wait()
    top = st_ref[:, 0, :]
    for k in range(7):
        top = jnp.maximum(top, got_ref[k, :, 0, :])
    total = st_ref[:, 1, :] * jnp.exp(st_ref[:, 0, :] - top)
    for k in range(7):
        total = total + got_ref[k, :, 1, :] * jnp.exp(got_ref[k, :, 0, :] - top)
    live = lab_ref[:, 0, :] >= 0
    tok_ref[:, 0, :] = jnp.where(live, top + jnp.log(total), BIG)
    tok_ref[:, 1, :] = jnp.where(live, scale_ref[...], 0.0)


def call_lse(stats, lab, scale, collective_id):
    vmem = pl.BlockSpec(memory_space=pltpu.VMEM)
    return pl.pallas_call(
        lse_kernel,
        in_specs=[vmem, vmem, vmem],
        out_specs=vmem,
        out_shape=jax.ShapeDtypeStruct(stats.shape, jnp.float32),
        scratch_shapes=[pltpu.VMEM((7,) + stats.shape, jnp.float32), pltpu.SemaphoreType.DMA((7,)), pltpu.SemaphoreType.DMA((7,))],
        compiler_params=pltpu.CompilerParams(collective_id=collective_id, has_side_effects=True, vmem_limit_bytes=4 * 1024 * 1024),
        cost_estimate=pl.CostEstimate(flops=10_000_000, bytes_accessed=1_000_000, transcendentals=20_000),
    )(stats, lab, scale)


def norm_kernel(pick_ref, h_ref, hat_ref, inv_ref, own_ref, far_ref):
    i = pl.program_id(0)
    x = h_ref[0].astype(jnp.float32)
    centered = x - jnp.mean(x, axis=-1, keepdims=True)
    inv = lax.rsqrt(jnp.mean(centered * centered, axis=-1, keepdims=True) + LAYER_EPS)
    hat = centered * inv
    hat_ref[0] = hat

    @pl.when(i == pick_ref[0])
    def _():
        own_ref[...] = hat
        inv_ref[...] = jnp.broadcast_to(inv, inv_ref.shape)

    @pl.when(i == pick_ref[1])
    def _():
        far_ref[...] = hat


def call_norm(picks, hidden):
    n, block, width = hidden.shape
    quarter = pl.BlockSpec((block, width), lambda i, s: (0, 0))
    each = pl.BlockSpec((1, block, width), lambda i, s: (i, 0, 0))
    one = jax.ShapeDtypeStruct((block, width), jnp.float32)
    return pl.pallas_call(
        norm_kernel,
        grid_spec=pltpu.PrefetchScalarGridSpec(
            num_scalar_prefetch=1, grid=(n,), in_specs=[each],
            out_specs=[each, pl.BlockSpec((block, 128), lambda i, s: (0, 0)), quarter, quarter],
        ),
        out_shape=[jax.ShapeDtypeStruct(hidden.shape, jnp.float32), jax.ShapeDtypeStruct((block, 128), jnp.float32), one, one],
        compiler_params=params(DE_VMEM),
        cost_estimate=pl.CostEstimate(flops=10_000_000, bytes_accessed=8_000_000, transcendentals=1024),
        name="norm",
    )(picks, hidden)


def norm_bwd_kernel(a_ref, b_ref, a_got_ref, b_got_ref, hat_ref, inv_ref, gamma_ref, loss_ref, a_out, b_out, sum_out):
    piece = a_ref.shape[0]
    grad = jnp.concatenate([a_ref[...] + a_got_ref[...], b_ref[...] + b_got_ref[...]])
    hat = hat_ref[...]
    scaled = grad * gamma_ref[...][None, :]
    inner = scaled - jnp.mean(scaled, axis=-1, keepdims=True) - hat * jnp.mean(scaled * hat, axis=-1, keepdims=True)
    inner = inner * inv_ref[:, 0:1]
    a_out[...] = inner[:piece]
    b_out[...] = inner[piece:]
    sum_out[...] = jnp.zeros_like(sum_out)
    sum_out[0:1, :] = jnp.sum(grad * hat, axis=0, keepdims=True)
    sum_out[1:2, :] = jnp.sum(grad, axis=0, keepdims=True)
    sum_out[2:3, 0:128] = loss_ref[...]


def call_norm_bwd(*args):
    piece, width = args[0].shape
    vmem = pl.BlockSpec(memory_space=pltpu.VMEM)
    half = jax.ShapeDtypeStruct((piece, width), jnp.float32)
    return pl.pallas_call(
        norm_bwd_kernel,
        in_specs=[vmem] * len(args),
        out_specs=[vmem] * 3,
        out_shape=[half, half, jax.ShapeDtypeStruct((8, width), jnp.float32)],
        compiler_params=pltpu.CompilerParams(vmem_limit_bytes=DE_VMEM),
        cost_estimate=pl.CostEstimate(flops=10_000_000, bytes_accessed=4_000_000, transcendentals=0),
        name="norm_bwd",
    )(*args)


def part_kernel(pick_ref, own_ref, got_ref, a_send, b_send, a_keep, b_keep):
    piece = a_send.shape[1]
    y, not_y, z, not_z = (pick_ref[6 + k] for k in range(4))
    for k in range(2):
        for out, block, at in ((a_send, 2 * k + not_y, 0), (a_keep, 2 * k + y, 0), (b_send, 2 * not_z + k, piece), (b_keep, 2 * z + k, piece)):
            out[k] = own_ref[block, at:at + piece, :] + got_ref[block, at:at + piece, :]


def call_part(picks, own, got):
    whole = pl.BlockSpec(own.shape, lambda i, s: (0, 0, 0), pipeline_mode=pl.Buffered(1))
    shape = (2, own.shape[1] // 2, own.shape[2])
    return pl.pallas_call(
        part_kernel,
        grid_spec=pltpu.PrefetchScalarGridSpec(
            num_scalar_prefetch=1, grid=(1,), in_specs=[whole, whole], out_specs=[pl.BlockSpec(shape, lambda i, s: (0, 0, 0), pipeline_mode=pl.Buffered(1))] * 4,
        ),
        out_shape=[jax.ShapeDtypeStruct(shape, jnp.float32)] * 4,
        compiler_params=params(DE_VMEM),
        cost_estimate=pl.CostEstimate(flops=1_000_000, bytes_accessed=9_000_000, transcendentals=0),
        name="part",
    )(picks, own, got)


def round_kernel(pick_ref, *refs):
    out_ref = refs[-1]
    piece = refs[0].shape[0]
    for p in range(4):
        start = pl.multiple_of(pick_ref[2 + p] * (2 * piece), 2 * piece)
        out_ref[0, pl.ds(start, piece), :] = refs[2 * p][...].astype(jnp.bfloat16)
        out_ref[0, pl.ds(start + piece, piece), :] = refs[2 * p + 1][...].astype(jnp.bfloat16)


def call_round(picks, pieces):
    piece, width = pieces[0].shape
    spec = pl.BlockSpec((piece, width), lambda i, s: (0, 0), pipeline_mode=pl.Buffered(1))
    out = (1, len(pieces) * piece, width)
    return pl.pallas_call(
        round_kernel,
        grid_spec=pltpu.PrefetchScalarGridSpec(
            num_scalar_prefetch=1, grid=(1,), in_specs=[spec] * len(pieces), out_specs=pl.BlockSpec(out, lambda i, s: (0, 0, 0)),
        ),
        out_shape=jax.ShapeDtypeStruct(out, jnp.bfloat16),
        compiler_params=params(DE_VMEM),
        cost_estimate=pl.CostEstimate(flops=1_000_000, bytes_accessed=5_000_000, transcendentals=0),
        name="round",
    )(picks, *pieces)


def params(limit=VMEM_LIMIT):
    return pltpu.CompilerParams(vmem_limit_bytes=limit, dimension_semantics=("arbitrary",))


def cost(pairs, rows, width):
    n = PAIR * pairs * rows
    return pl.CostEstimate(flops=2 * n * width, bytes_accessed=4 * n, transcendentals=n)


ANY = pl.BlockSpec(memory_space=pl.ANY)


def call_logits(idx, e, gamma, beta, pieces, previous, rows):
    pairs = 8
    base, count, order = (0, NEAR_PAIRS, NEAR_PIECES) if previous is None else (4, FAR_PAIRS, FAR_PIECES)
    width = e.shape[1]
    extra = [] if previous is None else list(previous)
    spec = pltpu.PrefetchScalarGridSpec(
        num_scalar_prefetch=1,
        grid=(4,),
        in_specs=[ANY]
        + [pl.BlockSpec((width,), lambda i, s: (0,))] * 2 + [ANY] * (len(pieces) + len(extra)),
        out_specs=[
            ANY,
            pl.BlockSpec((1, PAIR, width), lambda i, s: (base + last(i, s[count]), 0, 0)),
            pl.BlockSpec((1, 2, PAIR), lambda i, s: (last(i, s[count]), 0, 0)),
        ],
        scratch_shapes=[
            pltpu.VMEM((2, PAIR, width), jnp.float32),
            pltpu.VMEM((rows, width), jnp.bfloat16),
            pltpu.VMEM((2, rows, PAIR), jnp.float32),
            pltpu.SemaphoreType.DMA((2, 2)),
            pltpu.SemaphoreType.DMA,
            pltpu.SemaphoreType.DMA((2,)),
        ],
    )
    first = 4 + len(pieces)
    return pl.pallas_call(
        functools.partial(logits_kernel, count, base, order, len(pieces)),
        grid_spec=spec,
        out_shape=[
            jax.ShapeDtypeStruct((pairs, rows, PAIR), jnp.float32),
            jax.ShapeDtypeStruct((pairs, PAIR, width), jnp.bfloat16),
            jax.ShapeDtypeStruct((4, 2, PAIR), jnp.float32),
        ],
        input_output_aliases={} if previous is None else {first: 0, first + 1: 1},
        compiler_params=params(),
        cost_estimate=cost(3, rows, width),
        name="logits_near" if previous is None else "logits_far",
    )(idx, e, gamma, beta, *pieces, *extra)


def call_dz(idx, e, l, tok, lab):
    width, rows = e.shape[1], l.shape[1]
    pick_row = lambda i, s: (last(i, s[NEAR_PAIRS]), 0, 0)
    spec = pltpu.PrefetchScalarGridSpec(
        num_scalar_prefetch=1,
        grid=(4,),
        in_specs=[
            ANY,
            ANY,
            pl.BlockSpec((1, 2, PAIR), pick_row),
            pl.BlockSpec((1, 1, PAIR), pick_row),
        ],
        out_specs=[ANY, ANY, pl.BlockSpec((1, 1, PAIR), pick_row), ANY],
        scratch_shapes=[
            pltpu.VMEM((width, PAIR), jnp.float32),
            pltpu.VMEM((PAIR, width), jnp.float32),
            pltpu.VMEM((width, rows), jnp.bfloat16),
            pltpu.VMEM((rows, width), jnp.bfloat16),
            pltpu.VMEM((2, rows, PAIR), jnp.float32),
            pltpu.SemaphoreType.DMA((2,)),
            pltpu.SemaphoreType.DMA((pl.cdiv(rows, DZ_CHUNK),)),
            pltpu.SemaphoreType.DMA((2,)),
            pltpu.SemaphoreType.DMA((pl.cdiv(rows, DZ_CHUNK),)),
        ],
    )
    half = jax.ShapeDtypeStruct((4, BLOCK, width), jnp.float32)
    return pl.pallas_call(
        dz_kernel,
        grid_spec=spec,
        out_shape=[half, half, jax.ShapeDtypeStruct((4, 1, PAIR), jnp.float32), jax.ShapeDtypeStruct(l.shape, l.dtype)],
        input_output_aliases={2: 3},
        compiler_params=params(),
        cost_estimate=cost(3, rows, width),
        name="dz_part",
    )(idx, e, l, tok, lab)


def call_de(idx, l, zc, tok, lab, de, offset, rows, got, got_offset):
    total, width = l.shape[1], zc.shape[2]

    def whole(x):
        return pl.BlockSpec(x.shape, lambda i, s: (0,) * x.ndim, pipeline_mode=pl.Buffered(1))

    extra = [] if de is None else [de]
    extra_specs = [ANY] * len(extra)
    if got is not None:
        extra = [got] + extra
        extra_specs = [whole(got)] + extra_specs
    spec = pltpu.PrefetchScalarGridSpec(
        num_scalar_prefetch=1,
        grid=(1,),
        in_specs=[ANY, whole(zc), whole(tok), whole(lab)] + extra_specs,
        out_specs=[pl.BlockSpec((rows, width), lambda i, s: (0, 0), pipeline_mode=pl.Buffered(1)), ANY],
        scratch_shapes=[pltpu.VMEM((3, total // 6, PAIR), jnp.float32), pltpu.SemaphoreType.DMA((5,))],
    )
    return pl.pallas_call(
        functools.partial(de_kernel, offset, rows, got_offset if got is not None else None),
        grid_spec=spec,
        out_shape=[jax.ShapeDtypeStruct((rows, width), jnp.float32), jax.ShapeDtypeStruct((2 * total, width), jnp.float32)],
        input_output_aliases={} if de is None else {4 + len(extra): 1},
        compiler_params=params(DE_VMEM),
        cost_estimate=cost(5, rows, width),
    )(idx, l, zc, tok, lab, *extra)


def call_place(idx, got, de, got_offset):
    spec = pltpu.PrefetchScalarGridSpec(
        num_scalar_prefetch=1,
        grid=(1,),
        in_specs=[pl.BlockSpec(got.shape, lambda i, s: (0, 0), pipeline_mode=pl.Buffered(1)), ANY],
        out_specs=ANY,
        scratch_shapes=[pltpu.SemaphoreType.DMA],
    )
    return pl.pallas_call(
        functools.partial(place_kernel, got_offset),
        grid_spec=spec,
        out_shape=jax.ShapeDtypeStruct(de.shape, de.dtype),
        input_output_aliases={2: 0},
        compiler_params=params(DE_VMEM),
        name="place",
    )(idx, got, de)


def idx_of(scalars, order, pair_idx, core, tp):
    return jnp.concatenate([scalars, order[0], order[0] ^ (core * 4), order[1] ^ (core * 4 + tp), pair_idx])


def order_blocks(active):
    n = active.shape[1]
    act = active.astype(jnp.int32)
    ids = jnp.arange(n, dtype=jnp.int32)
    before = (ids[None, :] < ids[:, None]).astype(jnp.int32)
    ahead = jnp.sum(before[None] * act[:, None, :], axis=2)
    count = jnp.sum(act, axis=1, keepdims=True)
    place = jnp.where(act > 0, ahead, count + ids - ahead)
    hit = place[:, None, :] == ids[None, :, None]
    return jnp.sum(jnp.where(hit, ids, 0), axis=2), count[:, 0], hit


def solution(mesh):
    n_tp, n_dp = mesh.shape['tp'], mesh.shape['dp']

    def flip(x, axis, bits):
        n = n_tp if axis == 'tp' else n_dp
        return lax.ppermute(x, axis, [(k, k ^ bits) for k in range(n)])

    def pick(x, index):
        return lax.dynamic_index_in_dim(x, index, 0, keepdims=False)

    def local_step(hidden, ln_gamma, ln_beta, embed_shard, labels, loss_mask):
        tp, dp = lax.axis_index('tp'), lax.axis_index('dp')
        core = dp & 1
        y, z = (tp & 1).astype(jnp.uint32), (tp >> 1).astype(jnp.uint32)
        not_y, not_z = 1 - y, 1 - z
        seq, width = hidden.shape[1:]
        quarters = seq // BLOCK
        rows = embed_shard.shape[0] // 2
        row_start = tp * (2 * rows) + core * rows

        def by_core(mine, other):
            return jnp.stack([jnp.where(core == 0, mine, other), jnp.where(core == 0, other, mine)])

        marked = jnp.where(loss_mask[0] > 0, labels[0], -1)
        far_marks = [flip(marked, 'dp', 2), flip(marked, 'dp', 3)]
        mate_marks = flip(marked, 'dp', 1)

        picks = jnp.stack([tp, tp ^ 3] + [tp ^ p for p in range(4)] + [tp & 1, 1 - (tp & 1), tp >> 1, 1 - (tp >> 1)])
        x_hat, inv_std, own_quarter, far_quarter = call_norm(picks, hidden.reshape(quarters, BLOCK, width))
        mate = flip(x_hat, 'dp', 1)
        far0, far3 = flip(own_quarter, 'dp', 2), flip(far_quarter, 'dp', 2)

        marks = jnp.concatenate([by_core(marked, mate_marks), by_core(*far_marks)]).reshape(2, 8, BLOCK)
        token_count = jnp.sum((marks >= 0).astype(jnp.float32))
        order, active, hit = order_blocks(jnp.any(marks >= 0, axis=2))
        lab = jnp.sum(jnp.where(hit[..., None], marks[:, None], 0), axis=2).reshape(8, 1, PAIR)
        pairs = (active + 1) // 2
        pair_ids = jnp.arange(8, dtype=jnp.int32)
        pair_idx = jnp.where(pair_ids < pairs[0], pair_ids, jnp.minimum(4 + pair_ids - pairs[0], 7))
        zero = jnp.zeros((), jnp.int32)
        scalars = jnp.stack([core, pairs[0], pairs[1], pairs[0] + pairs[1], row_start, zero, zero, zero])
        idx, y, z, not_y, not_z = lax.optimization_barrier((idx_of(scalars, order, pair_idx, core, tp), y, z, not_y, not_z))

        logits, z_pairs, near_stats = call_logits(idx, embed_shard, ln_gamma, ln_beta, [x_hat, mate], None, rows)

        scale = jnp.broadcast_to(1.0 / token_count, (1, PAIR))
        near_tok = call_lse(near_stats, lab[:4], scale, 0)
        mate0, mate3 = flip(far0, 'dp', 1), flip(far3, 'dp', 1)
        far1, far2 = flip(far0, 'tp', 1), flip(far0, 'tp', 2)
        dz_own, dz_mate, target, logits = call_dz(idx, embed_shard, logits, near_tok, lab[:4])

        mate1, mate2 = flip(far1, 'dp', 1), flip(far2, 'dp', 1)
        lead = ((tp == 0) & (core == 0)).astype(jnp.float32)
        loss = jnp.sum(jnp.where(lab[:4, 0] >= 0, lead * near_tok[:, 0] - target[:, 0], 0.0)) / token_count
        loss, idx = lax.optimization_barrier((jnp.broadcast_to(loss, (1, 128)), idx))
        pieces = [far0, far1, far2, far3, mate0, mate1, mate2, mate3]
        logits, z_pairs, far_stats = call_logits(idx, embed_shard, ln_gamma, ln_beta, pieces, (logits, z_pairs), rows)
        far_tok = call_lse(far_stats, lab[4:], scale, 1)
        dz_got = flip(dz_mate, 'dp', 1)

        a_send, b_send, a_keep, b_keep = call_part(picks, dz_own, dz_got)
        a_got, b_got = flip(a_send, 'tp', 1), flip(b_send, 'tp', 2)
        a_keep, b_keep = a_keep + a_got, b_keep + b_got
        a_grad = flip(pick(a_keep, not_z), 'tp', 2)
        b_grad = flip(pick(b_keep, not_y), 'tp', 1)
        tok = jnp.concatenate([near_tok, far_tok])

        a0, b0, sums = call_norm_bwd(pick(a_keep, z), pick(b_keep, y), a_grad, b_grad, own_quarter, inv_std, ln_gamma, loss)
        a1, b2 = flip(a0, 'tp', 1), flip(b0, 'tp', 2)
        a2, a3 = flip(a0, 'tp', 2), flip(a1, 'tp', 2)
        b1, b3 = flip(b0, 'tp', 1), flip(b2, 'tp', 1)
        d_hidden = call_round(picks, [a0, b0, a1, b1, a2, b2, a3, b3])

        for axis in ('dp', 'tp'):
            got_sums = [flip(sums, axis, k) for k in (1, 2, 3)]
            sums = sums + got_sums[0] + (got_sums[1] + got_sums[2])

        chunks = [(0, rows // 3), (rows // 3, rows // 3), (4 * (rows // 6), rows // 6), (5 * (rows // 6), rows // 6)]
        d_embed, got = None, []
        for n, (offset, size) in enumerate(chunks):
            arrived = got[n - 2] if n >= 2 else None
            d_chunk, d_embed = call_de(idx, logits, z_pairs, tok, lab, d_embed, offset, size, arrived, chunks[n - 2][0] if n >= 2 else None)
            got.append(flip(d_chunk, 'dp', 1))
        for n in (2, 3):
            d_embed = call_place(idx, got[n], d_embed, chunks[n][0])

        return sums[2, 0], d_hidden, d_embed, sums[0], sums[1]


    return jax.shard_map(local_step, mesh=mesh, in_specs=(P('dp', None, None), P(None), P(None), P('tp', None), P('dp', None), P('dp', None)), out_specs=(P(), P('dp', None, None), P('tp', None), P(None), P(None)), check_vma=False)
```
